32 devices in a mesh: ty: 2 (over x), tx: 4 (over y, core), pat: 4 (over z).
Axes of the slice: x: 2, y: 2, z: 4, core: 2. Of those that a mesh axis runs over, the one named last changes fastest.
Arguments:
- estimate: float32 [32, 32, 1024], P(None, 'ty', 'tx'), may hold values from 0.5 to 1.5, as said below
- data: float32 [8, 32, 32, 1024], P('pat', None, 'ty', 'tx'), may hold values from 0.1 to 6, as said below
- axial: float32 [32, 32], replicated, may hold values from 0 to 0.6, as said below
- lateral_kernel: float32 [9, 9], replicated, may hold values from 0.01 to 0.04
- psf_radius: int32 [9], replicated, may hold values from 0 to 4
- pattern_codes: int32 [2, 8], replicated, may hold values from 0 to 4, as said below
Outputs:
- object_out: float32 [32, 32, 1024], P(None, 'ty', 'tx')
- residual_rms: float32 [4], replicated
The draws below stay inside these ranges and needn't reach their ends.
Inputs may be any that keep to these rules, and one draw needn't show every extreme that they name: `estimate`: positive values. `data`: positive photon counts. `axial`: nonnegative entries. `pattern_codes`: angle indices are 0 to 2, phase indices 0 to 4.
All inputs are finite; a program needn't handle non-finite values.
Results may differ from the reference program's by a relative error of at most 0.0003.
The reference program's roundings to bfloat16 on the way (of `kernel` and `backward`) count: a program that leaves them out, or rounds other values in their place, can miss the bound.
Values may be sent and summed in bfloat16 or wider, within the bound.
No kernel may reach another device: no remote copies, remote signals or barrier semaphores. Data moves between devices by JAX's collectives and lax.ppermute only.
A program may use at most 128 MiB of HBM per device.

```python
import math
import jax
import jax.numpy as jnp
from jax import lax

Z = 32
ROWS_DEV = 16
COLS_DEV = 256
RADIUS = 4
ITERS = 4
PATTERNS = 8
NY = 32
NX = 1024


def tile_table(key):
    row_tile = (jnp.arange(NY).astype(jnp.int32) // ROWS_DEV).astype(jnp.int32)
    col_tile = (jnp.arange(NX).astype(jnp.int32) // COLS_DEV).astype(jnp.int32)
    parity = ((row_tile[:, None] + col_tile[None, :]) % 2).astype(jnp.float32)
    jitter = jax.random.uniform(key, (NY // ROWS_DEV, NX // COLS_DEV), jnp.float32, 0.0, 1.0)
    return (parity, jitter[row_tile[:, None], col_tile[None, :]])


def draw_estimate(key, part):
    parity, jitter = tile_table(jax.random.fold_in(key, 41))
    level = jnp.where(parity > 0.5, 0.6 + 0.2 * jitter, 1.15 + 0.15 * jitter)
    noise = jax.random.uniform(jax.random.fold_in(key, 42), (Z, NY, NX), jnp.float32, 0.85, 1.15)
    return level[None] * noise


def draw_data(key, part):
    parity, jitter = tile_table(jax.random.fold_in(key, 31))
    tile_level = jnp.where(parity > 0.5, 1.6 + 0.8 * jitter, 0.4 + 0.2 * jitter)
    pattern_index = jnp.arange(PATTERNS).astype(jnp.float32)
    pattern_level = 0.5 * jnp.exp(math.log(4.0) * pattern_index / (PATTERNS - 1))
    noise = jax.random.uniform(jax.random.fold_in(key, 32), (PATTERNS, Z, NY, NX), jnp.float32, 0.55, 1.2)
    return pattern_level[:, None, None, None] * tile_level[None, None] * noise


def draw_axial(key, part):
    plane_index = jnp.arange(Z).astype(jnp.float32)
    distance = jnp.abs(plane_index[:, None] - plane_index[None, :])
    spread = jax.random.uniform(jax.random.fold_in(key, 11), (Z, Z), jnp.float32, 0.0, 1.0)
    diagonal = jax.random.uniform(jax.random.fold_in(key, 12), (Z, Z), jnp.float32, 0.4, 0.6)
    offside = spread * 0.05 * jnp.exp(-distance / 8.0)
    return jnp.where(distance == 0.0, diagonal, offside)


def draw_pattern_codes(key, part):
    angle_order = jax.random.permutation(jax.random.fold_in(key, 21), PATTERNS).astype(jnp.int32)
    phase_order = jax.random.permutation(jax.random.fold_in(key, 22), PATTERNS).astype(jnp.int32)
    offset = jax.random.randint(jax.random.fold_in(key, 23), (), 0, 5).astype(jnp.int32)
    angles = angle_order % 3
    phases = (phase_order + offset) % 5
    return jnp.stack([angles, phases]).astype(jnp.int32)


def with_ends(values, own_key, low, largest):
    place = [jax.random.randint(jax.random.fold_in(own_key, axis), (), 0, length) for axis, length in enumerate(values.shape)]
    longest = values.shape.index(max(values.shape))
    neighbour = place[:longest] + [(place[longest] + 1) % values.shape[longest]] + place[longest + 1:]
    return values.at[tuple(place)].set(low).at[tuple(neighbour)].set(largest)


def setup_inputs(seed: int = 0) -> dict:
    arg_keys = jax.random.split(jax.random.key(seed), 7)
    estimate = draw_estimate(jax.random.fold_in(arg_keys[6], 71), 0)
    data = draw_data(jax.random.fold_in(arg_keys[6], 71), 0)
    axial = draw_axial(jax.random.fold_in(arg_keys[6], 71), 0)
    lateral_kernel = jnp.clip(jax.random.uniform(arg_keys[3], (2 * RADIUS + 1, 2 * RADIUS + 1), jnp.float32, 0.01, 0.04), 0.01, 0.04)
    psf_radius = with_ends(jax.random.randint(arg_keys[4], (2 * RADIUS + 1,), 0, RADIUS + 1), jax.random.fold_in(arg_keys[4], 1), 0, RADIUS).astype(jnp.int32)
    pattern_codes = draw_pattern_codes(jax.random.fold_in(arg_keys[6], 71), 0)
    return {"estimate": estimate, "data": data, "axial": axial, "lateral_kernel": lateral_kernel, "psf_radius": psf_radius, "pattern_codes": pattern_codes}


TWO_PI = 2.0 * math.pi

def wave_table(angle_code, phase_code, row_coord, col_coord, planes):
    step_col = jnp.where(angle_code == 0, 2, -1).astype(jnp.int32)
    step_row = jnp.where(angle_code == 0, 0, jnp.where(angle_code == 1, 2, -2)).astype(jnp.int32)
    argument = (step_col[:, None, None] * col_coord[None, None, :] + step_row[:, None, None] * row_coord[None, :, None] + phase_code[:, None, None]) % 5
    lateral_wave = jnp.cos(argument.astype(jnp.float32) * (TWO_PI / 5.0))
    plane_index = jnp.arange(planes).astype(jnp.float32)
    axial_wave = jnp.cos(plane_index * (TWO_PI * 3.0 / planes))
    return 1.0 + 0.7 * lateral_wave[:, None, :, :] * axial_wave[None, :, None, None]

def masked_kernel(lateral_kernel, psf_radius):
    offsets = jnp.arange(2 * RADIUS + 1).astype(jnp.int32) - RADIUS
    within = jnp.abs(offsets)[None, :] <= psf_radius.astype(jnp.int32)[:, None]
    return jnp.where(within, lateral_kernel, jnp.zeros_like(lateral_kernel)).astype(jnp.bfloat16)

def widen(values):
    return lax.optimization_barrier(values).astype(jnp.float32)

def lateral_pass(values, kernel):
    dims = values.shape
    flattened = widen(values).reshape((-1, 1, dims[-2], dims[-1]))
    result = lax.conv_general_dilated(flattened, widen(kernel)[None, None], (1, 1), ((RADIUS, RADIUS), (RADIUS, RADIUS)), precision=lax.Precision.HIGHEST)
    return result.reshape(dims)

def reference(estimate, data, axial, lateral_kernel, psf_radius, pattern_codes):
    kernel = masked_kernel(lateral_kernel, psf_radius)
    flipped = kernel[::-1, ::-1]
    axial_f = widen(axial.astype(jnp.bfloat16))
    row_coord = jnp.arange(NY).astype(jnp.int32)
    col_coord = jnp.arange(NX).astype(jnp.int32)
    lighting = wave_table(pattern_codes[0], pattern_codes[1], row_coord, col_coord, Z)
    inside = jnp.ones((1, NY, NX), jnp.bfloat16)
    coverage = widen(lateral_pass(inside, flipped).astype(jnp.bfloat16))
    spread = jnp.einsum('ba,byx->ayx', axial_f, jnp.broadcast_to(coverage, (Z, NY, NX)), precision=lax.Precision.HIGHEST)
    normalizer = lax.optimization_barrier(jnp.sum(lighting * spread[None], axis=0))
    cell_count = float(PATTERNS * Z * NY * NX)
    current = estimate
    squares_list = []
    for iteration in range(ITERS):
        lighted = widen((lighting * current[None]).astype(jnp.bfloat16))
        blurred = jnp.einsum('ab,pbyx->payx', axial_f, lighted, precision=lax.Precision.HIGHEST).astype(jnp.bfloat16)
        predicted = lateral_pass(blurred, kernel)
        misfit = data - predicted
        squares_list.append(jnp.sum(misfit * misfit))
        quotient = (data / predicted).astype(jnp.bfloat16)
        backward = widen(lateral_pass(quotient, flipped).astype(jnp.bfloat16))
        gathered = jnp.einsum('ba,pbyx->payx', axial_f, backward, precision=lax.Precision.HIGHEST)
        summed = lax.optimization_barrier(jnp.sum(lighting * gathered, axis=0))
        current = current * summed / normalizer
    squares = jnp.stack(squares_list)
    return (current, jnp.sqrt(squares / cell_count))
```

```python
import functools
import math

import jax
import jax.numpy as jnp
from jax import lax
from jax.experimental import pallas as pl
from jax.experimental.pallas import tpu as pltpu
from jax.sharding import PartitionSpec as P

RADIUS = 4
TAPS = 2 * RADIUS + 1
ITERS = 4
TWO_PI = 2.0 * math.pi

TILE = 32
HALO = 16
GROUP = TILE + 2 * HALO
ROWS_BLOCK = RADIUS
BLOCK = ROWS_BLOCK * GROUP
LANES = 128
SUB = 8
QUAD_ROWS = (0, 2, 1, 3)
F32 = jnp.float32
BF16 = jnp.bfloat16


def lane_iota(shape):
    return lax.broadcasted_iota(jnp.int32, shape, len(shape) - 1)


def column_of(lane):
    inner = lane % GROUP
    return jnp.where(inner < TILE + HALO, inner, inner - GROUP)


def roll(x, shift):
    shift = shift % LANES
    return x if shift == 0 else pltpu.roll(x, shift, 1)


def quad_transpose(v, lane):
    low = lane < 64
    even = (lane // TILE) % 2 == 0
    a0 = jnp.where(low, v[0], roll(v[2], 64))
    a2 = jnp.where(low, roll(v[0], 64), v[2])
    a1 = jnp.where(low, v[1], roll(v[3], 64))
    a3 = jnp.where(low, roll(v[1], 64), v[3])
    return (
        jnp.where(even, a0, roll(a1, 32)),
        jnp.where(even, roll(a0, -32), a1),
        jnp.where(even, a2, roll(a3, 32)),
        jnp.where(even, roll(a2, -32), a3),
    )


def pack_kernel(dest_of_tile, rows, where_ref, data_ref, est_ref, out_ref):
    lane = lane_iota((SUB, LANES))
    groups = data_ref.shape[0] // (rows * SUB)
    tiles_half = LANES // TILE

    def piece(half, src_ref, start, out_row):
        for quad in range(rows // 4):
            v = [src_ref[pl.ds(start + 4 * quad + r, SUB, stride=rows), :] for r in QUAD_ROWS]
            for t, piece_t in enumerate(quad_transpose(v, lane)):
                dest = dest_of_tile[half * tiles_half + t]
                out_ref[dest, pl.ds(out_row, SUB), quad * LANES : (quad + 1) * LANES] = piece_t

    for half in range(len(dest_of_tile) // tiles_half):

        @pl.when(pl.program_id(0) == half)
        def _(half=half):
            def step(i, carry):
                piece(half, data_ref, i * rows * SUB, pl.multiple_of(i * SUB, SUB))
                return carry

            lax.fori_loop(0, groups, step, 0)
            piece(half, est_ref, where_ref[1] * rows * SUB, groups * SUB)


def edge_messages(own, lane):
    left = right = None
    for u in range(4):
        slot = (lane // HALO) % 4 == u
        l_u, r_u = roll(own[u], HALO * u), roll(own[u], HALO * (u - 1))
        left = l_u if left is None else jnp.where(slot, l_u, left)
        right = r_u if right is None else jnp.where(slot, r_u, right)
    return left, right


def own_pair(v):
    return v, roll(v, -TILE)


def halo_kernel(src_of, in_ref, left_ref, right_ref):
    lane = lane_iota((SUB, LANES))
    ty, pat, planes_part = src_of["ty"], src_of["pat"], in_ref.shape[1] // SUB
    data_groups = planes_part - 1
    per_ty = in_ref.shape[2] // LANES // 2

    def emit(k, group, out_row):
        for i in range(ty):
            for pair in range(per_ty):
                own = []
                for q in (2 * pair, 2 * pair + 1):
                    own += own_pair(
                        in_ref[i * pat + k, pl.ds(group * SUB, SUB), q * LANES : (q + 1) * LANES]
                    )
                left, right = edge_messages(own, lane)
                vreg = i * per_ty + pair
                left_ref[pl.ds(out_row, SUB), vreg * LANES : (vreg + 1) * LANES] = left
                right_ref[pl.ds(out_row, SUB), vreg * LANES : (vreg + 1) * LANES] = right

    for k in range(pat):

        def step(g, carry, k=k):
            emit(k, g, pl.multiple_of((k * data_groups + g) * SUB, SUB))
            return carry

        lax.fori_loop(0, data_groups, step, 0)
        emit(k, data_groups, (pat * data_groups + k) * SUB)


def with_halo(own, u, from_right, from_left, lane):
    inner = lane % GROUP
    value = jnp.where(inner < TILE, own, roll(from_right, HALO * (2 - u)))
    return jnp.where(inner < TILE + HALO, value, roll(from_left, HALO * (3 - u)))


def taps_kernel(k_ref, w_ref):
    lane = lane_iota((GROUP, LANES))
    row = lax.broadcasted_iota(jnp.int32, (GROUP, LANES), 0)
    tap = column_of(row) - column_of(lane) + RADIUS
    first = lane < GROUP
    w_ref[...] = jnp.zeros_like(w_ref)
    hit = [tap == j for j in range(TAPS)]
    for flip in range(2):
        for i0 in range(TAPS + 1):
            value = jnp.zeros((GROUP, LANES), F32)
            for j in range(TAPS):
                def scalar(i):
                    if i < 0 or i >= TAPS:
                        return jnp.float32(0.0)
                    return k_ref[TAPS - 1 - i, TAPS - 1 - j] if flip else k_ref[i, j]
                value = jnp.where(hit[j], jnp.where(first, scalar(i0), scalar(i0 - 1)), value)
            value = value.astype(BF16)
            for k in range(3):
                for r in range(ROWS_BLOCK):
                    for q in range(ROWS_BLOCK // 2):
                        if ROWS_BLOCK * (k - 1) + r - 2 * q + RADIUS == i0:
                            w_ref[
                                3 * flip + k,
                                r * GROUP : (r + 1) * GROUP,
                                q * LANES : (q + 1) * LANES,
                            ] = value


def lateral(src_ref, w_ref, flip, b):
    total = None
    for k in range(3):
        part = jnp.dot(src_ref[b + k], w_ref[3 * flip + k], preferred_element_type=F32)
        total = part if total is None else total + part
    return total


def iterate(where_ref, w_ref, ax_fwd, ax_bwd, light_ref, wave_ref, colsum_ref, data_ref, obj_ref,
            norm_ref, stage_ref, quot_ref, sq_ref, nx, patterns):
    planes = obj_ref.shape[1]
    rows = patterns * planes
    blocks = obj_ref.shape[0]
    col = column_of(lane_iota((1, BLOCK)))
    place = where_ref[0] * TILE + col
    inside = (place >= 0) & (place < nx)
    own = (col >= 0) & (col < TILE)
    stage_ref[0] = jnp.zeros(stage_ref.shape[1:], BF16)
    stage_ref[blocks + 1] = jnp.zeros(stage_ref.shape[1:], BF16)
    quot_ref[0] = jnp.zeros(quot_ref.shape[1:], BF16)
    quot_ref[blocks + 1] = jnp.zeros(quot_ref.shape[1:], BF16)

    ones = jnp.broadcast_to(jnp.where(inside, 1.0, 0.0), (2 * SUB, BLOCK)).astype(BF16)
    zeros = jnp.zeros((2 * SUB, BLOCK), BF16)
    for b in range(blocks):
        total = None
        for k in range(3):
            if 0 <= b + k - 1 < blocks:
                part = jnp.dot(ones, w_ref[3 + k], preferred_element_type=F32)
                total = part if total is None else total + part
        cover = total.astype(BF16).astype(F32)[0:1]
        lat_sum = jnp.sum(light_ref[b], axis=0, keepdims=True)
        norm_ref[b] = colsum_ref[...] * cover * (float(patterns) + lat_sum * wave_ref[...])

    def lighting(b):
        lat = light_ref[b][:, None, :]
        return (1.0 + lat * wave_ref[...][None, :, :])

    for it, (quot_reach, obj_reach) in enumerate(((12, 8), (4, 0))):
        quot_ok = inside & (col >= -quot_reach) & (col < TILE + quot_reach)
        obj_ok = inside & (col >= -obj_reach) & (col < TILE + obj_reach)

        def light_step(b, carry):
            lit = (lighting(b) * obj_ref[b][None]).astype(BF16).reshape(rows, BLOCK)
            stage_ref[b + 1] = jnp.dot(ax_fwd[...], lit, preferred_element_type=F32).astype(BF16)
            return carry

        lax.fori_loop(0, blocks, light_step, 0)

        def quot_step(b, acc):
            predicted = lateral(stage_ref, w_ref, 0, b)
            data = data_ref[b]
            miss = data - predicted
            acc = acc + jnp.sum((miss * miss).reshape(rows // SUB, SUB, BLOCK), axis=0)
            quot = jnp.where(quot_ok, data / jnp.where(quot_ok, predicted, 1.0), 0.0)
            quot_ref[b + 1] = quot.astype(BF16)
            return acc

        acc = lax.fori_loop(0, blocks, quot_step, jnp.zeros((SUB, BLOCK), F32))
        sq_ref[it] = jnp.where(own, acc, 0.0)

        def back_step(b, carry):
            back = lateral(quot_ref, w_ref, 1, b).astype(BF16)
            gathered = jnp.dot(ax_bwd[...], back, preferred_element_type=F32)
            summed = jnp.sum(lighting(b) * gathered.reshape(patterns, planes, BLOCK), axis=0)
            obj_ref[b] = jnp.where(obj_ok, obj_ref[b] * summed / norm_ref[b], 0.0)
            return carry

        lax.fori_loop(0, blocks, back_step, 0)


def first_kernel(nx, patterns, src_of, where_ref, w_ref, ax_fwd, ax_bwd, light_ref, wave_ref, colsum_ref, in_ref,
                 from_left_ref, from_right_ref, data_ref, obj_out_ref, left_ref, right_ref, sq_ref,
                 obj_ref, norm_ref, stage_ref, quot_ref):
    lane = lane_iota((SUB, LANES))
    ty, pat = src_of["ty"], src_of["pat"]
    data_groups = in_ref.shape[1] // SUB - 1
    per_ty = in_ref.shape[2] // LANES // 2

    def unpack(k, group, src_row, out_ref, out_row):
        for i in range(ty):
            for pair in range(per_ty):
                vreg = i * per_ty + pair
                from_left = from_left_ref[pl.ds(src_row, SUB), vreg * LANES : (vreg + 1) * LANES]
                from_right = from_right_ref[pl.ds(src_row, SUB), vreg * LANES : (vreg + 1) * LANES]
                own = []
                for q in (2 * pair, 2 * pair + 1):
                    own += own_pair(
                        in_ref[i * pat + k, pl.ds(group * SUB, SUB), q * LANES : (q + 1) * LANES]
                    )
                for u in range(4):
                    m = 4 * vreg + u
                    out_ref[m // 2, pl.ds(out_row, SUB), (m % 2) * LANES : (m % 2 + 1) * LANES] = (
                        with_halo(own[u], u, from_right, from_left, lane)
                    )

    for k in range(pat):

        def step(g, carry, k=k):
            row = pl.multiple_of((k * data_groups + g) * SUB, SUB)
            unpack(k, g, row, data_ref, row)
            return carry

        lax.fori_loop(0, data_groups, step, 0)
        unpack(k, data_groups, (pat * data_groups + k) * SUB, obj_ref, k * SUB)

    iterate(where_ref, w_ref, ax_fwd, ax_bwd, light_ref, wave_ref, colsum_ref, data_ref, obj_ref,
            norm_ref, stage_ref, quot_ref, sq_ref, nx, patterns)

    for z in range(0, obj_ref.shape[1], SUB):
        for vreg in range(obj_ref.shape[0] // 2):
            own = []
            for u in range(4):
                m = 4 * vreg + u
                v = obj_ref[m // 2, z : z + SUB, (m % 2) * LANES : (m % 2 + 1) * LANES]
                own.append(v)
                obj_out_ref[m // 2, z : z + SUB, (m % 2) * LANES : (m % 2 + 1) * LANES] = v
            left, right = edge_messages(own, lane)
            left_ref[z : z + SUB, vreg * LANES : (vreg + 1) * LANES] = left
            right_ref[z : z + SUB, vreg * LANES : (vreg + 1) * LANES] = right


def second_kernel(nx, patterns, where_ref, w_ref, ax_fwd, ax_bwd, light_ref, wave_ref, colsum_ref, data_ref,
                  obj_in_ref, from_left_ref, from_right_ref, out_ref, sq_ref,
                  obj_ref, norm_ref, stage_ref, quot_ref):
    lane = lane_iota((SUB, LANES))
    for z in range(0, obj_ref.shape[1], SUB):
        for vreg in range(obj_ref.shape[0] // 2):
            from_left = from_left_ref[z : z + SUB, vreg * LANES : (vreg + 1) * LANES]
            from_right = from_right_ref[z : z + SUB, vreg * LANES : (vreg + 1) * LANES]
            for u in range(4):
                m = 4 * vreg + u
                at = (m // 2, slice(z, z + SUB), slice((m % 2) * LANES, (m % 2 + 1) * LANES))
                obj_ref[at] = with_halo(obj_in_ref[at], u, from_right, from_left, lane)

    iterate(where_ref, w_ref, ax_fwd, ax_bwd, light_ref, wave_ref, colsum_ref, data_ref, obj_ref,
            norm_ref, stage_ref, quot_ref, sq_ref, nx, patterns)

    ty = out_ref.shape[0]
    quads = out_ref.shape[2] // LANES
    own = (lane // TILE) % 2 == 0
    for z in range(0, obj_ref.shape[1], SUB):
        for i in range(ty):
            for q in range(quads):
                m = i * quads + q
                v0 = obj_ref[m, z : z + SUB, 0:LANES]
                v1 = obj_ref[m, z : z + SUB, LANES : 2 * LANES]
                out_ref[i, z : z + SUB, q * LANES : (q + 1) * LANES] = jnp.where(own, v0, roll(v1, TILE))


def final_kernel(dest_of_tile, rows, in_ref, out_ref):
    lane = lane_iota((SUB, LANES))
    planes = out_ref.shape[0] // rows
    tiles_half = LANES // TILE
    for half in range(len(dest_of_tile) // tiles_half):

        @pl.when(pl.program_id(0) == half)
        def _(half=half):
            for z in range(0, planes, SUB):
                for quad in range(rows // 4):
                    v = [
                        in_ref[dest_of_tile[half * tiles_half + t], z : z + SUB, quad * LANES : (quad + 1) * LANES]
                        for t in range(tiles_half)
                    ]
                    for g, row in enumerate(quad_transpose(v, lane)):
                        out_ref[pl.ds(z * rows + 4 * quad + QUAD_ROWS[g], SUB, stride=rows), :] = row


def masked_kernel(lateral_kernel, psf_radius):
    offsets = jnp.arange(TAPS) - RADIUS
    within = jnp.abs(offsets)[None, :] <= psf_radius[:, None]
    return jnp.where(within, lateral_kernel, jnp.zeros_like(lateral_kernel)).astype(BF16)


def shape(dims, dtype=F32):
    return jax.ShapeDtypeStruct(dims, dtype)


VMEM = pl.BlockSpec(memory_space=pltpu.VMEM)
SMEM = pl.BlockSpec(memory_space=pltpu.SMEM)


def tiled_device(sizes, estimate, data, axial, lateral_kernel, psf_radius, pattern_codes):
    ty, tx, pat = sizes["ty"], sizes["tx"], sizes["pat"]
    planes, rows, cols = estimate.shape
    pat_local = data.shape[0]
    patterns = pat_local * pat
    ny, nx = rows * ty, cols * tx
    members = ty * pat
    blocks = ny // ROWS_BLOCK
    axes = ("ty", "tx", "pat")

    owner = [(i, k if i % 2 == 0 else pat - 1 - k) for i in range(ty) for k in range(pat)]
    dest_of_tile = [i * pat + k for i, k in owner]
    order = [(i * tx + j) * pat + k for j in range(tx) for i, k in owner]
    to_right = [(a, b) for a, b in zip(order[:-1], order[1:])]
    to_left = [(b, a) for a, b in to_right]
    src_of = {"ty": ty, "pat": pat}

    ti, tj, tk = (lax.axis_index(a) for a in axes)
    tile = tj * members + ti * pat + jnp.where(ti % 2 == 0, tk, pat - 1 - tk)
    where = jnp.stack([tile, tk]).astype(jnp.int32)

    packed_rows = pat_local * planes + planes // pat
    message = pl.pallas_call(
        functools.partial(pack_kernel, dest_of_tile, rows),
        out_shape=shape((members, packed_rows, rows * TILE)),
        grid=(cols // LANES,),
        in_specs=[
            SMEM,
            pl.BlockSpec((data.size // cols, LANES), lambda h: (0, h)),
            pl.BlockSpec((planes * rows, LANES), lambda h: (0, h)),
        ],
        out_specs=pl.BlockSpec((members, packed_rows, rows * TILE), lambda h: (0, 0, 0)),
        name="pack",
    )(where, data.reshape(-1, cols), estimate.reshape(-1, cols))
    mine = lax.all_to_all(message, ("ty", "pat"), 0, 0, tiled=True)

    kernel = masked_kernel(lax.reduce_precision(lateral_kernel, 8, 7), psf_radius).astype(F32)
    weights = pl.pallas_call(
        taps_kernel,
        out_shape=shape((6, BLOCK, BLOCK), BF16),
        in_specs=[SMEM],
        out_specs=VMEM,
        name="taps",
    )(kernel)
    axial_b = axial.astype(BF16)
    same = (jnp.arange(patterns * planes)[:, None] // planes) == (jnp.arange(patterns * planes)[None, :] // planes)
    ax_fwd = jnp.where(same, jnp.tile(axial_b, (patterns, patterns)), jnp.zeros((), BF16))
    ax_bwd = jnp.where(same, jnp.tile(axial_b.T, (patterns, patterns)), jnp.zeros((), BF16))
    colsum = jnp.broadcast_to(jnp.sum(lax.reduce_precision(axial, 8, 7), axis=0)[:, None], (planes, BLOCK))
    wave = jnp.cos(jnp.arange(planes).astype(F32) * (TWO_PI * 3.0 / planes))
    wave = jnp.broadcast_to(wave[:, None], (planes, BLOCK))
    lane = jnp.arange(BLOCK)
    y = jnp.arange(blocks)[:, None] * ROWS_BLOCK + lane[None, :] // GROUP
    x = tile * TILE + column_of(lane)[None, :]
    angle, phase = pattern_codes[0], pattern_codes[1]
    step_col = jnp.where(angle == 0, 2, -1).astype(jnp.int32)
    step_row = jnp.where(angle == 0, 0, jnp.where(angle == 1, 2, -2)).astype(jnp.int32)
    argument = (
        step_col[None, :, None] * x[:, None, :] + step_row[None, :, None] * y[:, None, :] + phase[None, :, None]
    ) % 5
    light = 0.7 * jnp.cos(argument.astype(F32) * (TWO_PI / 5.0))

    halo_lanes = ny * HALO
    total_rows = packed_rows * pat
    left, right = pl.pallas_call(
        functools.partial(halo_kernel, src_of),
        out_shape=(shape((total_rows, halo_lanes)), shape((total_rows, halo_lanes))),
        in_specs=[VMEM],
        out_specs=(VMEM, VMEM),
        name="edges",
    )(mine)
    from_left = lax.ppermute(right, axes, to_right)
    from_right = lax.ppermute(left, axes, to_left)

    scratch = [
        pltpu.VMEM((blocks, planes, BLOCK), F32),
        pltpu.VMEM((blocks, planes, BLOCK), F32),
        pltpu.VMEM((blocks + 2, patterns * planes, BLOCK), BF16),
        pltpu.VMEM((blocks + 2, patterns * planes, BLOCK), BF16),
    ]
    tables = (where, weights, ax_fwd, ax_bwd, light, wave, colsum)
    table_specs = [SMEM] + [VMEM] * 6
    data_all, current, left, right, sq_first = pl.pallas_call(
        functools.partial(first_kernel, nx, patterns, src_of),
        out_shape=(
            shape((blocks, patterns * planes, BLOCK)),
            shape((blocks, planes, BLOCK)),
            shape((planes, halo_lanes)),
            shape((planes, halo_lanes)),
            shape((2, SUB, BLOCK)),
        ),
        in_specs=table_specs + [VMEM] * 3,
        out_specs=(VMEM,) * 5,
        scratch_shapes=scratch,
        name="first",
    )(*tables, mine, from_left, from_right)
    from_left = lax.ppermute(right, axes, to_right)
    from_right = lax.ppermute(left, axes, to_left)
    pieces, sq_second = pl.pallas_call(
        functools.partial(second_kernel, nx, patterns),
        out_shape=(shape((ty, planes, rows * TILE)), shape((2, SUB, BLOCK))),
        in_specs=table_specs + [VMEM] * 4,
        out_specs=(VMEM,) * 2,
        scratch_shapes=scratch,
        name="second",
    )(*tables, data_all, current, from_left, from_right)

    squares = jnp.sum(jnp.concatenate([sq_first, sq_second]), axis=(1, 2))
    squares = jnp.sum(lax.all_gather(squares, "tx"), axis=0)
    extra = jnp.pad(squares[None, :], ((0, SUB - 1), (0, rows * TILE - ITERS)))
    outgoing = jnp.concatenate([pieces, jnp.broadcast_to(extra, (ty,) + extra.shape)], axis=1)
    outgoing = jnp.broadcast_to(outgoing[:, None], (ty, pat) + outgoing.shape[1:])
    outgoing = outgoing.reshape((members,) + outgoing.shape[2:])
    incoming = lax.all_to_all(outgoing, ("ty", "pat"), 0, 0, tiled=True)
    result = pl.pallas_call(
        functools.partial(final_kernel, dest_of_tile, rows),
        out_shape=shape((planes * rows, cols)),
        grid=(cols // LANES,),
        in_specs=[pl.BlockSpec(incoming.shape, lambda h: (0, 0, 0))],
        out_specs=pl.BlockSpec((planes * rows, LANES), lambda h: (0, h)),
        name="unpack",
    )(incoming)
    squares = jnp.sum(incoming[:, planes, :ITERS], axis=0)
    cell_count = float(patterns * planes * ny * nx)
    return result.reshape(estimate.shape), jnp.sqrt(squares / cell_count)


def extended(block, sides, width):
    for axis, dim in sides:
        count = lax.axis_size(axis)
        forward = [(i, i + 1) for i in range(count - 1)]
        backward = [(target, source) for source, target in forward]
        low = lax.ppermute(
            lax.slice_in_dim(block, block.shape[dim] - width, None, axis=dim), axis, forward
        )
        high = lax.ppermute(lax.slice_in_dim(block, 0, width, axis=dim), axis, backward)
        block = jnp.concatenate([low, block, high], axis=dim)
    return block


def wave_table(angle_code, phase_code, row_coord, col_coord, planes):
    step_col = jnp.where(angle_code == 0, 2, -1).astype(jnp.int32)
    step_row = jnp.where(angle_code == 0, 0, jnp.where(angle_code == 1, 2, -2)).astype(jnp.int32)
    argument = (
        step_col[:, None, None] * col_coord[None, None, :]
        + step_row[:, None, None] * row_coord[None, :, None]
        + phase_code[:, None, None]
    ) % 5
    lateral_wave = jnp.cos(argument.astype(jnp.float32) * (TWO_PI / 5.0))
    plane_index = jnp.arange(planes).astype(jnp.float32)
    axial_wave = jnp.cos(plane_index * (TWO_PI * 3.0 / planes))
    return 1.0 + 0.7 * lateral_wave[:, None, :, :] * axial_wave[None, :, None, None]


def tap_matrices(kernel, width_in, width_out):
    tap_count = 2 * RADIUS + 1
    offset = jnp.arange(width_in)[:, None] - jnp.arange(width_out)[None, :]
    onehot = (offset[None, :, :] == jnp.arange(tap_count)[:, None, None]).astype(jnp.float32)
    return jnp.einsum(
        "ij,jab->iab", kernel.astype(jnp.float32), onehot, precision=lax.Precision.HIGHEST
    ).astype(jnp.bfloat16)


def lateral_pass(padded, matrices, height):
    summed = None
    for tap_row in range(2 * RADIUS + 1):
        window = padded[..., tap_row : tap_row + height, :]
        product = jnp.dot(window, matrices[tap_row], preferred_element_type=jnp.float32)
        summed = product if summed is None else summed + product
    return summed


def general_device(estimate, data, axial, lateral_kernel, psf_radius, pattern_codes):
    planes, height, width = estimate.shape
    pat_local = data.shape[0]
    full_rows = height * lax.axis_size("ty")
    full_cols = width * lax.axis_size("tx")
    depth = 2 * RADIUS
    margin = depth - RADIUS
    row_coord = lax.axis_index("ty") * height - depth + jnp.arange(height + 2 * depth)
    col_coord = lax.axis_index("tx") * width - depth + jnp.arange(width + 2 * depth)
    codes_here = lax.dynamic_slice_in_dim(
        pattern_codes, lax.axis_index("pat") * pat_local, pat_local, 1
    )
    lighting = wave_table(codes_here[0], codes_here[1], row_coord, col_coord, planes)
    lighting_inner = lighting[:, :, depth : depth + height, depth : depth + width]
    kernel = masked_kernel(lateral_kernel, psf_radius)
    forward_taps = tap_matrices(kernel, width + 2 * depth, width + 2 * margin)
    adjoint_taps = tap_matrices(kernel[::-1, ::-1], width + 2 * RADIUS, width)
    axial_b = axial.astype(jnp.bfloat16)
    row_inside = (row_coord >= 0) & (row_coord < full_rows)
    col_inside = (col_coord >= 0) & (col_coord < full_cols)
    inside_all = row_inside[:, None] & col_inside[None, :]
    inside = inside_all[
        margin : margin + height + 2 * RADIUS, margin : margin + width + 2 * RADIUS
    ].astype(jnp.bfloat16)
    inside_mid = inside_all[
        RADIUS : RADIUS + height + 2 * margin, RADIUS : RADIUS + width + 2 * margin
    ]
    coverage = lateral_pass(inside[None], adjoint_taps, height).astype(jnp.bfloat16)
    spread = jnp.einsum(
        "ba,byx->ayx",
        axial_b,
        jnp.broadcast_to(coverage, (planes, height, width)),
        preferred_element_type=jnp.float32,
    )
    normalizer = lax.psum(jnp.sum(lighting_inner * spread[None], axis=0), "pat")
    cell_count = float(pat_local * lax.axis_size("pat") * planes * full_rows * full_cols)
    data_wide = extended(data, (("ty", 2), ("tx", 3)), RADIUS)
    current = estimate
    squares_list = []
    for iteration in range(ITERS):
        padded = extended(current, (("ty", 1), ("tx", 2)), depth)
        lighted = (lighting * padded[None]).astype(jnp.bfloat16)
        blurred = jnp.einsum(
            "ab,pbyx->payx", axial_b, lighted, preferred_element_type=jnp.float32
        ).astype(jnp.bfloat16)
        predicted = lateral_pass(blurred, forward_taps, height + 2 * margin)
        predicted_inner = predicted[:, :, margin : margin + height, margin : margin + width]
        misfit = data - predicted_inner
        local_square = jnp.sum(misfit * misfit)
        safe = jnp.where(inside_mid[None, None], predicted, 1.0)
        quotient_padded = jnp.where(inside_mid[None, None], data_wide / safe, 0.0).astype(
            jnp.bfloat16
        )
        backward = lateral_pass(quotient_padded, adjoint_taps, height).astype(jnp.bfloat16)
        gathered = jnp.einsum(
            "ba,pbyx->payx", axial_b, backward, preferred_element_type=jnp.float32
        )
        contribution = jnp.sum(lighting_inner * gathered, axis=0)
        summed = lax.psum(contribution, "pat")
        current = current * summed / normalizer
        squares_list.append(lax.psum(local_square, ("ty", "tx", "pat")))
    squares = jnp.stack(squares_list)
    return (current, jnp.sqrt(squares / cell_count))


def solution(mesh):
    sizes = dict(mesh.shape)
    in_specs = (P(None, "ty", "tx"), P("pat", None, "ty", "tx"), P(), P(), P(), P())
    out_specs = (P(None, "ty", "tx"), P())

    def per_device(estimate, data, *rest):
        planes, rows, cols = estimate.shape
        members = sizes["ty"] * sizes["pat"]
        fits = (
            cols == members * TILE
            and cols % LANES == 0
            and rows % 8 == 0
            and rows * sizes["ty"] <= 2 * TILE
            and planes == sizes["pat"] * SUB
        )
        if fits:
            return tiled_device(sizes, estimate, data, *rest)
        return general_device(estimate, data, *rest)

    return jax.shard_map(
        per_device, mesh=mesh, in_specs=in_specs, out_specs=out_specs, check_vma=False
    )
```

```python
import functools
import math

import jax
import jax.numpy as jnp
import numpy as np
from jax import lax
from jax.experimental import pallas as pl
from jax.experimental.pallas import tpu as pltpu
from jax.sharding import PartitionSpec as P

RADIUS = 4
TAPS = 2 * RADIUS + 1
ITERS = 4
TWO_PI = 2.0 * math.pi

TILE = 32
HALO = 16
GROUP = TILE + 2 * HALO
ROWS_BLOCK = RADIUS
BLOCK = ROWS_BLOCK * GROUP
LANES = 128
SUB = 8
QUAD_ROWS = (0, 2, 1, 3)
CHUNK = 4
OFFSET = 1 << 20
F32 = jnp.float32
BF16 = jnp.bfloat16


def lane_iota(shape):
    return lax.broadcasted_iota(jnp.int32, shape, len(shape) - 1)


def column_of(lane):
    inner = lane % GROUP
    return jnp.where(inner < TILE + HALO, inner, inner - GROUP)


def roll(x, shift):
    shift = shift % LANES
    return x if shift == 0 else pltpu.roll(x, shift, 1)


def quad_transpose(v, lane):
    group = lane // TILE
    out = []
    for t in range(4):
        value = roll(v[0], -TILE * t)
        for g in range(1, 4):
            value = jnp.where(group == g, roll(v[g], TILE * (g - t)), value)
        out.append(value)
    return out


def pack_half(dest_of_tile, rows, half, groups, src_ref, out_ref):
    lane = lane_iota((SUB, LANES))
    tiles_half = LANES // TILE
    for i in range(groups):
        for quad in range(rows // 4):
            v = [src_ref[pl.ds(i * rows * SUB + 4 * quad + r, SUB, stride=rows), :] for r in QUAD_ROWS]
            for t, piece in enumerate(quad_transpose(v, lane)):
                dest = dest_of_tile[half * tiles_half + t]
                out_ref[dest, i * SUB : (i + 1) * SUB, quad * LANES : (quad + 1) * LANES] = piece


def pack_kernel(dest_of_tile, rows, data_ref, out_ref):
    for half in range(len(dest_of_tile) * TILE // LANES):

        @pl.when(pl.program_id(0) == half)
        def _(half=half):
            pack_half(dest_of_tile, rows, half, data_ref.shape[0] // (rows * SUB), data_ref, out_ref)


def estimate_kernel(dest_of_tile, rows, pat, est_ref, out_ref, all_ref):
    halves = len(dest_of_tile) * TILE // LANES
    for half in range(halves):

        @pl.when(pl.program_id(0) == half)
        def _(half=half):
            pack_half(dest_of_tile, rows, half, est_ref.shape[0] // (rows * SUB), est_ref, all_ref)
            if half == halves - 1:
                for i in range(out_ref.shape[0]):
                    out_ref[i] = all_ref[i * pat + lax.axis_index("pat")]


def edge_messages(pieces, lane):
    left = right = None
    for u, (v, offset) in enumerate(pieces):
        slot = (lane // HALO) % 4 == u
        l_u, r_u = roll(v, HALO * u - offset), roll(v, HALO * (u - 1) - offset)
        left = l_u if left is None else jnp.where(slot, l_u, left)
        right = r_u if right is None else jnp.where(slot, r_u, right)
    return left, right


def edges_kernel(src_of, in_ref, left_ref, right_ref):
    lane = lane_iota((SUB, LANES))
    ty, pat = src_of
    groups = in_ref.shape[1] // SUB
    per_ty = in_ref.shape[2] // LANES // 2
    for k in range(pat):
        for g in range(groups):
            row = slice((k * groups + g) * SUB, (k * groups + g + 1) * SUB)
            for i in range(ty):
                for pair in range(per_ty):
                    pieces = []
                    for q in (2 * pair, 2 * pair + 1):
                        v = in_ref[i * pat + k, g * SUB : (g + 1) * SUB, q * LANES : (q + 1) * LANES]
                        pieces += [(v, 0), (v, TILE)]
                    left, right = edge_messages(pieces, lane)
                    vreg = i * per_ty + pair
                    left_ref[row, vreg * LANES : (vreg + 1) * LANES] = left
                    right_ref[row, vreg * LANES : (vreg + 1) * LANES] = right


def unpack_wide(src_of, in_ref, from_left_ref, from_right_ref, out_ref):
    lane = lane_iota((SUB, LANES))
    ty, pat = src_of
    groups = in_ref.shape[1] // SUB
    per_ty = in_ref.shape[2] // LANES // 2
    for k in range(pat):
        for g in range(groups):
            row = slice((k * groups + g) * SUB, (k * groups + g + 1) * SUB)
            for i in range(ty):
                for pair in range(per_ty):
                    vreg = i * per_ty + pair
                    from_left = from_left_ref[row, vreg * LANES : (vreg + 1) * LANES]
                    from_right = from_right_ref[row, vreg * LANES : (vreg + 1) * LANES]
                    own = []
                    for q in (2 * pair, 2 * pair + 1):
                        v = in_ref[i * pat + k, g * SUB : (g + 1) * SUB, q * LANES : (q + 1) * LANES]
                        own += [v, roll(v, -TILE)]
                    for u in range(4):
                        m = 4 * vreg + u
                        out_ref[m // 2, row, (m % 2) * LANES : (m % 2 + 1) * LANES] = with_halo(
                            own[u], u, from_right, from_left, lane
                        )


def with_halo(own, u, from_right, from_left, lane):
    inner = lane % GROUP
    value = jnp.where(inner < TILE, own, roll(from_right, HALO * (2 - u)))
    return jnp.where(inner < TILE + HALO, value, roll(from_left, HALO * (3 - u)))


def tables_kernel(tile_of, k_ref, radius_ref, codes_ref, axial_ref, w_ref, fwd_ref, bwd_ref, light_ref):
    lane = lane_iota((GROUP, LANES))
    row = lax.broadcasted_iota(jnp.int32, (GROUP, LANES), 0)
    tap = column_of(row) - column_of(lane) + RADIUS
    first = lane < GROUP
    hit = [tap == j for j in range(TAPS)]
    nothing = jnp.zeros((GROUP, LANES), BF16)

    def scalar(flip, i, j):
        if i < 0 or i >= TAPS:
            return jnp.float32(0.0)
        if flip:
            i, j = TAPS - 1 - i, TAPS - 1 - j
        return jnp.where(abs(j - RADIUS) <= radius_ref[i], k_ref[i, j], 0.0)

    for flip in range(2):
        for i0 in range(-2, TAPS + 3):
            value = jnp.zeros((GROUP, LANES), F32)
            if 0 <= i0 <= TAPS:
                for j in range(TAPS):
                    both = jnp.where(first, scalar(flip, i0, j), scalar(flip, i0 - 1, j))
                    value = jnp.where(hit[j], both, value)
            value = value.astype(BF16)
            for k in range(3):
                for r in range(ROWS_BLOCK):
                    for q in range(ROWS_BLOCK // 2):
                        if ROWS_BLOCK * (k - 1) + r - 2 * q + RADIUS == i0:
                            w_ref[
                                3 * flip + k,
                                r * GROUP : (r + 1) * GROUP,
                                q * LANES : (q + 1) * LANES,
                            ] = value

    planes, rows = axial_ref.shape[0], fwd_ref.shape[0]
    axial = axial_ref[...].astype(BF16)
    pick = lax.broadcasted_iota(jnp.int32, (planes, rows), 1) % planes
    pick = (pick == lax.broadcasted_iota(jnp.int32, (planes, rows), 0)).astype(F32).astype(BF16)
    plain = jnp.dot(axial, pick, preferred_element_type=F32)
    turned = lax.dot_general(axial, pick, (((0,), (0,)), ((), ())), preferred_element_type=F32)
    column = lax.broadcasted_iota(jnp.int32, (planes, rows), 1)
    for p in range(rows // planes):
        here = column // planes == p
        fwd_ref[p * planes : (p + 1) * planes] = jnp.where(here, plain, 0.0).astype(BF16)
    span = 3 * planes
    for h in range(2):
        here = (column >= h * span) & (column < (h + 1) * span)
        bwd_ref[h * planes : (h + 1) * planes] = jnp.where(here, turned, 0.0).astype(BF16)[:, : 2 * span]

    col = column_of(lane_iota((1, BLOCK)))
    within = lane_iota((1, BLOCK)) // GROUP
    x = tile_of() * TILE + col
    cosines = [0.7 * math.cos(TWO_PI * m / 5.0) for m in range(5)]
    patterns = light_ref.shape[1]
    for p in range(patterns):
        angle, phase = codes_ref[0, p], codes_ref[1, p]
        step_col = jnp.where(angle == 0, 2, -1)
        step_row = jnp.where(angle == 0, 0, jnp.where(angle == 1, 2, -2))
        for b in range(light_ref.shape[0]):
            y = within + b * ROWS_BLOCK
            turn = lax.rem(step_col * x + step_row * y + phase + 5 * OFFSET, 5)
            value = jnp.full((1, BLOCK), cosines[0], F32)
            for m in range(1, 5):
                value = jnp.where(turn == m, cosines[m], value)
            light_ref[b, p : p + 1] = value


def lateral(src_ref, w_ref, flip, b, count):
    total = None
    for k in range(3):
        v = src_ref[b + k : b + k + count]
        part = jnp.dot(v.reshape(-1, BLOCK), w_ref[3 * flip + k], preferred_element_type=F32)
        total = part if total is None else total + part
    return total.reshape(count, -1, BLOCK)


def split3(v):
    high = v.astype(BF16)
    rest = v - high.astype(F32)
    mid = rest.astype(BF16)
    return high, mid, (rest - mid.astype(F32)).astype(BF16)


class Step:
    def __init__(self, nx, tile_of, w_ref, ax_fwd, ax_bwd, light_ref, wave_ref):
        self.w, self.ax_fwd, self.ax_bwd, self.light, self.wave = w_ref, ax_fwd, ax_bwd, light_ref, wave_ref
        self.blocks, self.patterns = light_ref.shape[0], light_ref.shape[1]
        self.planes = wave_ref.shape[0]
        self.col = column_of(lane_iota((1, BLOCK)))
        place = tile_of() * TILE + self.col
        self.inside = (place >= 0) & (place < nx)

    def reach(self, width):
        return self.inside & (self.col >= -width) & (self.col < TILE + width)

    def clear_ends(self, ref):
        ref[0] = jnp.zeros(ref.shape[1:], BF16)
        ref[self.blocks + 1] = jnp.zeros(ref.shape[1:], BF16)

    def normalizer(self, norm_ref):
        depth = self.ax_bwd.shape[1]
        ones = lax.broadcasted_iota(jnp.int32, (depth, BLOCK), 0) < self.planes
        ones = jnp.where(ones, 1.0, 0.0).astype(BF16)
        colsum = jnp.dot(self.ax_bwd[...], ones, preferred_element_type=F32)[: self.planes]
        ones = jnp.broadcast_to(jnp.where(self.inside, 1.0, 0.0), (2 * SUB, BLOCK)).astype(BF16)
        parts = [jnp.dot(ones, self.w[3 + k], preferred_element_type=F32) for k in range(3)]
        for b in range(self.blocks):
            total = sum(parts[k] for k in range(3) if 0 <= b + k - 1 < self.blocks)
            cover = total.astype(BF16).astype(F32)[0:1]
            lat_sum = jnp.sum(self.light[b], axis=0, keepdims=True)
            norm_ref[b] = colsum * cover * (float(self.patterns) + lat_sum * self.wave[...])

    def blur(self, obj_ref, stage_ref):
        for b in range(self.blocks):
            lighting = 1.0 + self.light[b][:, None, :] * self.wave[...][None]
            lit = (lighting * obj_ref[b][None]).astype(BF16).reshape(-1, BLOCK)
            stage_ref[b + 1] = jnp.dot(self.ax_fwd[...], lit, preferred_element_type=F32).astype(BF16)

    def compare(self, stage_ref, data_ref, quot_ref, width, predicted_ref=None):
        ok = self.reach(width)[None]
        acc = jnp.zeros((SUB, BLOCK), F32)
        for b in range(0, self.blocks, CHUNK):
            if predicted_ref is None:
                predicted = lateral(stage_ref, self.w, 0, b, CHUNK)
            else:
                predicted = predicted_ref[b : b + CHUNK]
            data = data_ref[b : b + CHUNK]
            miss = data - predicted
            acc = acc + jnp.sum((miss * miss).reshape(-1, SUB, BLOCK), axis=0)
            quot_ref[b + 1 : b + 1 + CHUNK] = jnp.where(ok, data / predicted, 0.0).astype(BF16)
        row = jnp.sum(jnp.where((self.col >= 0) & (self.col < TILE), acc, 0.0), axis=0, keepdims=True)
        return sum(row[:, h * LANES : (h + 1) * LANES] for h in range(BLOCK // LANES))

    def update(self, quot_ref, obj_ref, norm_ref, width):
        ok = self.reach(width)
        for b0 in range(0, self.blocks, CHUNK):
            back = lateral(quot_ref, self.w, 1, b0, CHUNK).astype(BF16)
            for b in range(b0, b0 + CHUNK):
                part = back[b - b0].astype(F32).reshape(self.patterns, self.planes, BLOCK)
                plain = jnp.sum(part, axis=0)
                waved = jnp.sum(self.light[b][:, None, :] * part, axis=0)
                stack = jnp.concatenate(split3(plain) + split3(waved), axis=0)
                both = jnp.dot(self.ax_bwd[...], stack, preferred_element_type=F32)
                summed = both[: self.planes] + self.wave[...] * both[self.planes :]
                obj_ref[b] = jnp.where(ok, obj_ref[b] * summed / norm_ref[b], 0.0)


def put_halo(own_ref, from_left_ref, from_right_ref, out_ref):
    lane = lane_iota((SUB, LANES))
    for z in range(0, out_ref.shape[1], SUB):
        for vreg in range(out_ref.shape[0] // 2):
            from_left = from_left_ref[z : z + SUB, vreg * LANES : (vreg + 1) * LANES]
            from_right = from_right_ref[z : z + SUB, vreg * LANES : (vreg + 1) * LANES]
            for u in range(4):
                m = 4 * vreg + u
                at = (m // 2, slice(z, z + SUB), slice((m % 2) * LANES, (m % 2 + 1) * LANES))
                out_ref[at] = with_halo(own_ref[at], u, from_right, from_left, lane)


def forward_kernel(nx, tile_of, src_of, w_ref, ax_fwd, ax_bwd, light_ref, wave_ref,
                   est_ref, from_left_ref, from_right_ref, obj_ref, norm_ref, predicted_ref, stage_ref):
    unpack_wide(src_of, est_ref, from_left_ref, from_right_ref, obj_ref)
    step = Step(nx, tile_of, w_ref, ax_fwd, ax_bwd, light_ref, wave_ref)
    step.normalizer(norm_ref)
    step.clear_ends(stage_ref)
    step.blur(obj_ref, stage_ref)
    for b in range(0, step.blocks, CHUNK):
        predicted_ref[b : b + CHUNK] = lateral(stage_ref, w_ref, 0, b, CHUNK)


def first_kernel(nx, tile_of, src_of, w_ref, ax_fwd, ax_bwd, light_ref, wave_ref, norm_ref, obj_in_ref,
                 predicted_ref, in_ref, from_left_ref, from_right_ref, data_ref, obj_ref, left_ref, right_ref,
                 sq_ref, stage_ref, quot_ref):
    unpack_wide(src_of, in_ref, from_left_ref, from_right_ref, data_ref)
    step = Step(nx, tile_of, w_ref, ax_fwd, ax_bwd, light_ref, wave_ref)
    step.clear_ends(stage_ref)
    step.clear_ends(quot_ref)
    obj_ref[...] = obj_in_ref[...]
    sq_ref[...] = jnp.zeros(sq_ref.shape, F32)
    sq_ref[0:1] = step.compare(None, data_ref, quot_ref, 12, predicted_ref)
    step.update(quot_ref, obj_ref, norm_ref, 8)
    step.blur(obj_ref, stage_ref)
    sq_ref[1:2] = step.compare(stage_ref, data_ref, quot_ref, 4)
    step.update(quot_ref, obj_ref, norm_ref, 0)

    lane = lane_iota((SUB, LANES))
    for z in range(0, step.planes, SUB):
        for vreg in range(step.blocks // 2):
            pieces = []
            for u in range(4):
                m = 4 * vreg + u
                pieces.append((obj_ref[m // 2, z : z + SUB, (m % 2) * LANES : (m % 2 + 1) * LANES], 0))
            left, right = edge_messages(pieces, lane)
            left_ref[z : z + SUB, vreg * LANES : (vreg + 1) * LANES] = left
            right_ref[z : z + SUB, vreg * LANES : (vreg + 1) * LANES] = right


def second_kernel(nx, tile_of, src_of, w_ref, ax_fwd, ax_bwd, light_ref, wave_ref, norm_ref, data_ref,
                  obj_in_ref, from_left_ref, from_right_ref, sq_in_ref, out_ref, obj_ref, stage_ref, quot_ref):
    put_halo(obj_in_ref, from_left_ref, from_right_ref, obj_ref)
    step = Step(nx, tile_of, w_ref, ax_fwd, ax_bwd, light_ref, wave_ref)
    step.clear_ends(stage_ref)
    step.clear_ends(quot_ref)
    squares = [sq_in_ref[0:1], sq_in_ref[1:2]]
    for quot_width, obj_width in ((12, 8), (4, 0)):
        step.blur(obj_ref, stage_ref)
        squares.append(step.compare(stage_ref, data_ref, quot_ref, quot_width))
        step.update(quot_ref, obj_ref, norm_ref, obj_width)

    ty, pat = src_of
    quads = step.blocks // ty
    lane = lane_iota((SUB, LANES))
    own = (lane // TILE) % 2 == 0
    last = jnp.concatenate(squares + [jnp.zeros((SUB - len(squares), LANES), F32)], axis=0)
    for i in range(ty):
        for k in range(pat):
            out_ref[i * pat + k, quads * step.planes : quads * step.planes + SUB] = last
        for q in range(quads):
            for z in range(0, step.planes, SUB):
                v0 = obj_ref[i * quads + q, z : z + SUB, 0:LANES]
                v1 = obj_ref[i * quads + q, z : z + SUB, LANES : 2 * LANES]
                v = jnp.where(own, v0, roll(v1, TILE))
                for k in range(pat):
                    out_ref[i * pat + k, q * step.planes + z : q * step.planes + z + SUB] = v


def final_kernel(dest_of_tile, rows, in_ref, out_ref, sq_ref):
    lane = lane_iota((SUB, LANES))
    planes = out_ref.shape[0] // rows
    tiles_half = LANES // TILE
    quads = rows // 4
    sq_ref[...] = jnp.sum(in_ref[:, quads * planes : quads * planes + SUB], axis=0)
    for half in range(len(dest_of_tile) // tiles_half):

        @pl.when(pl.program_id(0) == half)
        def _(half=half):
            for z in range(0, planes, SUB):
                for quad in range(quads):
                    row = quad * planes + z
                    v = [in_ref[dest_of_tile[half * tiles_half + t], row : row + SUB] for t in range(tiles_half)]
                    for g, piece in enumerate(quad_transpose(v, lane)):
                        out_ref[pl.ds(z * rows + 4 * quad + QUAD_ROWS[g], SUB, stride=rows), :] = piece


def masked_kernel(lateral_kernel, psf_radius):
    offsets = jnp.arange(TAPS) - RADIUS
    within = jnp.abs(offsets)[None, :] <= psf_radius[:, None]
    return jnp.where(within, lateral_kernel, jnp.zeros_like(lateral_kernel)).astype(BF16)


def shape(dims, dtype=F32):
    return jax.ShapeDtypeStruct(dims, dtype)


VMEM = pl.BlockSpec(memory_space=pltpu.VMEM)
SMEM = pl.BlockSpec(memory_space=pltpu.SMEM)


def tiled_device(sizes, estimate, data, axial, lateral_kernel, psf_radius, pattern_codes):
    ty, tx, pat = sizes["ty"], sizes["tx"], sizes["pat"]
    planes, rows, cols = estimate.shape
    pat_local = data.shape[0]
    patterns = pat_local * pat
    ny, nx = rows * ty, cols * tx
    members = ty * pat
    blocks = ny // ROWS_BLOCK
    axes = ("ty", "tx", "pat")

    owner = [(i, k if i % 2 == 0 else pat - 1 - k) for i in range(ty) for k in range(pat)]
    dest_of_tile = [i * pat + k for i, k in owner]
    order = [(i * tx + j) * pat + k for j in range(tx) for i, k in owner]
    to_right = [(a, b) for a, b in zip(order[:-1], order[1:])]
    to_left = [(b, a) for a, b in to_right]
    src_of = (ty, pat)

    ti = lax.axis_index("ty")

    def tile_of():
        i, j, k = (lax.axis_index(a) for a in axes)
        return j * members + i * pat + jnp.where(lax.rem(i, 2) == 0, k, pat - 1 - k)

    halves = cols // LANES
    piece_lanes = rows * TILE
    halo_lanes = ny * HALO

    def whole(dims):
        return pl.BlockSpec(dims, lambda h: (0,) * len(dims))

    def half_columns(height):
        return pl.BlockSpec((height, LANES), lambda h: (0, h))

    def edges(pieces, name):
        out = shape((pieces.shape[1] * pieces.shape[0] // ty, halo_lanes))
        return pl.pallas_call(
            functools.partial(edges_kernel, (ty, pieces.shape[0] // ty)),
            out_shape=(out, out),
            in_specs=[VMEM],
            out_specs=(VMEM,) * 2,
            name=name,
        )(pieces)

    def swap_edges(left, right):
        return lax.ppermute(right, axes, to_right), lax.ppermute(left, axes, to_left)

    message = pl.pallas_call(
        functools.partial(pack_kernel, dest_of_tile, rows),
        out_shape=shape((members, pat_local * planes, piece_lanes)),
        grid=(halves,),
        in_specs=[half_columns(data.size // cols)],
        out_specs=whole((members, pat_local * planes, piece_lanes)),
        name="pack",
    )(data.reshape(-1, cols))
    message, estimate = lax.optimization_barrier((message, estimate))
    mine = lax.all_to_all(message, ("ty", "pat"), 0, 0, tiled=True)

    pieces = pl.pallas_call(
        functools.partial(estimate_kernel, dest_of_tile, rows, pat),
        out_shape=shape((ty, planes, piece_lanes)),
        grid=(halves,),
        in_specs=[half_columns(planes * rows)],
        out_specs=whole((ty, planes, piece_lanes)),
        scratch_shapes=[pltpu.VMEM((members, planes, piece_lanes), F32)],
        name="prep_estimate",
    )(estimate.reshape(-1, cols))
    tile_rows = [lax.dynamic_index_in_dim(pieces, ti, 0, keepdims=False)]
    for shift in range(1, ty):
        sent = lax.dynamic_index_in_dim(pieces, (ti + shift) % ty, 0, keepdims=False)
        tile_rows.append(lax.ppermute(sent, "ty", [(i, (i + shift) % ty) for i in range(ty)]))
    tile_rows = jnp.stack(tile_rows)
    tile_rows = jnp.stack(
        [lax.dynamic_index_in_dim(tile_rows, (ti - i) % ty, 0, keepdims=False) for i in range(ty)]
    )
    est_left, est_right = swap_edges(*edges(tile_rows, "prep_edges"))

    weights, ax_fwd, ax_bwd, light = pl.pallas_call(
        functools.partial(tables_kernel, tile_of),
        out_shape=(
            shape((6, BLOCK, BLOCK), BF16),
            shape((patterns * planes, patterns * planes), BF16),
            shape((2 * planes, 6 * planes), BF16),
            shape((blocks, patterns, BLOCK)),
        ),
        in_specs=[SMEM] * 3 + [VMEM],
        out_specs=(VMEM,) * 4,
        name="tables",
    )(lateral_kernel, psf_radius, pattern_codes, axial)
    wave = np.cos(np.arange(planes, dtype=np.float32) * np.float32(TWO_PI * 3.0 / planes))
    wave = jnp.asarray(np.ascontiguousarray(np.broadcast_to(wave[:, None], (planes, BLOCK))))

    object_shape = shape((blocks, planes, BLOCK))
    field_shape = shape((blocks, patterns * planes, BLOCK))
    object_scratch = pltpu.VMEM(object_shape.shape, F32)
    stage = pltpu.VMEM((blocks + 2, patterns * planes, BLOCK), BF16)
    table_specs = [VMEM] * 5
    mine, est_left, est_right, weights = lax.optimization_barrier((mine, est_left, est_right, weights))
    from_left, from_right = swap_edges(*edges(mine, "edges"))
    tables = (weights, ax_fwd, ax_bwd, light, wave)
    current, norm, predicted = pl.pallas_call(
        functools.partial(forward_kernel, nx, tile_of, (ty, 1)),
        out_shape=(object_shape, object_shape, field_shape),
        in_specs=table_specs + [VMEM] * 3,
        out_specs=(VMEM,) * 3,
        scratch_shapes=[stage],
        name="forward",
    )(*tables, tile_rows, est_left, est_right)

    edge_shape = shape((planes, halo_lanes))
    data_all, current, left, right, sq_first = pl.pallas_call(
        functools.partial(first_kernel, nx, tile_of, src_of),
        out_shape=(field_shape, object_shape, edge_shape, edge_shape, shape((SUB, LANES))),
        in_specs=table_specs + [VMEM] * 6,
        out_specs=(VMEM,) * 5,
        scratch_shapes=[stage, stage],
        name="first",
    )(*tables, norm, current, predicted, mine, from_left, from_right)
    from_left, from_right = swap_edges(left, right)
    outgoing = pl.pallas_call(
        functools.partial(second_kernel, nx, tile_of, src_of),
        out_shape=shape((members, rows // 4 * planes + SUB, LANES)),
        in_specs=table_specs + [VMEM] * 6,
        out_specs=VMEM,
        scratch_shapes=[object_scratch, stage, stage],
        name="second",
    )(*tables, norm, data_all, current, from_left, from_right, sq_first)

    incoming = lax.all_to_all(outgoing, ("ty", "pat"), 0, 0, tiled=True)
    result, squares = pl.pallas_call(
        functools.partial(final_kernel, dest_of_tile, rows),
        out_shape=(shape((planes * rows, cols)), shape((SUB, LANES))),
        grid=(halves,),
        in_specs=[whole(incoming.shape)],
        out_specs=(half_columns(planes * rows), whole((SUB, LANES))),
        name="unpack",
    )(incoming)
    squares = lax.psum(jnp.sum(squares[:ITERS], axis=1), "tx")
    cell_count = float(patterns * planes * ny * nx)
    return result.reshape(estimate.shape), jnp.sqrt(squares / cell_count)


def extended(block, sides, width):
    for axis, dim in sides:
        count = lax.axis_size(axis)
        forward = [(i, i + 1) for i in range(count - 1)]
        backward = [(target, source) for source, target in forward]
        low = lax.ppermute(
            lax.slice_in_dim(block, block.shape[dim] - width, None, axis=dim), axis, forward
        )
        high = lax.ppermute(lax.slice_in_dim(block, 0, width, axis=dim), axis, backward)
        block = jnp.concatenate([low, block, high], axis=dim)
    return block


def wave_table(angle_code, phase_code, row_coord, col_coord, planes):
    step_col = jnp.where(angle_code == 0, 2, -1).astype(jnp.int32)
    step_row = jnp.where(angle_code == 0, 0, jnp.where(angle_code == 1, 2, -2)).astype(jnp.int32)
    argument = (
        step_col[:, None, None] * col_coord[None, None, :]
        + step_row[:, None, None] * row_coord[None, :, None]
        + phase_code[:, None, None]
    ) % 5
    lateral_wave = jnp.cos(argument.astype(jnp.float32) * (TWO_PI / 5.0))
    plane_index = jnp.arange(planes).astype(jnp.float32)
    axial_wave = jnp.cos(plane_index * (TWO_PI * 3.0 / planes))
    return 1.0 + 0.7 * lateral_wave[:, None, :, :] * axial_wave[None, :, None, None]


def tap_matrices(kernel, width_in, width_out):
    tap_count = 2 * RADIUS + 1
    offset = jnp.arange(width_in)[:, None] - jnp.arange(width_out)[None, :]
    onehot = (offset[None, :, :] == jnp.arange(tap_count)[:, None, None]).astype(jnp.float32)
    return jnp.einsum(
        "ij,jab->iab", kernel.astype(jnp.float32), onehot, precision=lax.Precision.HIGHEST
    ).astype(jnp.bfloat16)


def lateral_pass(padded, matrices, height):
    summed = None
    for tap_row in range(2 * RADIUS + 1):
        window = padded[..., tap_row : tap_row + height, :]
        product = jnp.dot(window, matrices[tap_row], preferred_element_type=jnp.float32)
        summed = product if summed is None else summed + product
    return summed


def general_device(estimate, data, axial, lateral_kernel, psf_radius, pattern_codes):
    planes, height, width = estimate.shape
    pat_local = data.shape[0]
    full_rows = height * lax.axis_size("ty")
    full_cols = width * lax.axis_size("tx")
    depth = 2 * RADIUS
    margin = depth - RADIUS
    row_coord = lax.axis_index("ty") * height - depth + jnp.arange(height + 2 * depth)
    col_coord = lax.axis_index("tx") * width - depth + jnp.arange(width + 2 * depth)
    codes_here = lax.dynamic_slice_in_dim(
        pattern_codes, lax.axis_index("pat") * pat_local, pat_local, 1
    )
    lighting = wave_table(codes_here[0], codes_here[1], row_coord, col_coord, planes)
    lighting_inner = lighting[:, :, depth : depth + height, depth : depth + width]
    kernel = masked_kernel(lateral_kernel, psf_radius)
    forward_taps = tap_matrices(kernel, width + 2 * depth, width + 2 * margin)
    adjoint_taps = tap_matrices(kernel[::-1, ::-1], width + 2 * RADIUS, width)
    axial_b = axial.astype(jnp.bfloat16)
    row_inside = (row_coord >= 0) & (row_coord < full_rows)
    col_inside = (col_coord >= 0) & (col_coord < full_cols)
    inside_all = row_inside[:, None] & col_inside[None, :]
    inside = inside_all[
        margin : margin + height + 2 * RADIUS, margin : margin + width + 2 * RADIUS
    ].astype(jnp.bfloat16)
    inside_mid = inside_all[
        RADIUS : RADIUS + height + 2 * margin, RADIUS : RADIUS + width + 2 * margin
    ]
    coverage = lateral_pass(inside[None], adjoint_taps, height).astype(jnp.bfloat16)
    spread = jnp.einsum(
        "ba,byx->ayx",
        axial_b,
        jnp.broadcast_to(coverage, (planes, height, width)),
        preferred_element_type=jnp.float32,
    )
    normalizer = lax.psum(jnp.sum(lighting_inner * spread[None], axis=0), "pat")
    cell_count = float(pat_local * lax.axis_size("pat") * planes * full_rows * full_cols)
    data_wide = extended(data, (("ty", 2), ("tx", 3)), RADIUS)
    current = estimate
    squares_list = []
    for iteration in range(ITERS):
        padded = extended(current, (("ty", 1), ("tx", 2)), depth)
        lighted = (lighting * padded[None]).astype(jnp.bfloat16)
        blurred = jnp.einsum(
            "ab,pbyx->payx", axial_b, lighted, preferred_element_type=jnp.float32
        ).astype(jnp.bfloat16)
        predicted = lateral_pass(blurred, forward_taps, height + 2 * margin)
        predicted_inner = predicted[:, :, margin : margin + height, margin : margin + width]
        misfit = data - predicted_inner
        local_square = jnp.sum(misfit * misfit)
        safe = jnp.where(inside_mid[None, None], predicted, 1.0)
        quotient_padded = jnp.where(inside_mid[None, None], data_wide / safe, 0.0).astype(
            jnp.bfloat16
        )
        backward = lateral_pass(quotient_padded, adjoint_taps, height).astype(jnp.bfloat16)
        gathered = jnp.einsum(
            "ba,pbyx->payx", axial_b, backward, preferred_element_type=jnp.float32
        )
        contribution = jnp.sum(lighting_inner * gathered, axis=0)
        summed = lax.psum(contribution, "pat")
        current = current * summed / normalizer
        squares_list.append(lax.psum(local_square, ("ty", "tx", "pat")))
    squares = jnp.stack(squares_list)
    return (current, jnp.sqrt(squares / cell_count))


def solution(mesh):
    sizes = dict(mesh.shape)
    in_specs = (P(None, "ty", "tx"), P("pat", None, "ty", "tx"), P(), P(), P(), P())
    out_specs = (P(None, "ty", "tx"), P())

    def per_device(estimate, data, *rest):
        planes, rows, cols = estimate.shape
        members = sizes["ty"] * sizes["pat"]
        fits = (
            cols == members * TILE
            and cols % LANES == 0
            and rows % 8 == 0
            and rows * sizes["ty"] <= 2 * TILE
            and planes == sizes["pat"] * SUB
        )
        if fits:
            return tiled_device(sizes, estimate, data, *rest)
        return general_device(estimate, data, *rest)

    return jax.shard_map(
        per_device, mesh=mesh, in_specs=in_specs, out_specs=out_specs, check_vma=False
    )
```

```python
import functools
import math

import jax
import jax.numpy as jnp
import numpy as np
from jax import lax
from jax.experimental import pallas as pl
from jax.experimental.pallas import tpu as pltpu
from jax.sharding import PartitionSpec as P

RADIUS = 4
TAPS = 2 * RADIUS + 1
ITERS = 4
TWO_PI = 2.0 * math.pi

TILE = 32
HALO = 16
GROUP = TILE + 2 * HALO
ROWS_BLOCK = RADIUS
BLOCK = ROWS_BLOCK * GROUP
LANES = 128
SUB = 8
QUAD_ROWS = (0, 2, 1, 3)
CHUNK = 4
OFFSET = 1 << 20
F32 = jnp.float32
BF16 = jnp.bfloat16


def lane_iota(shape):
    return lax.broadcasted_iota(jnp.int32, shape, len(shape) - 1)


def column_of(lane):
    inner = lane % GROUP
    return jnp.where(inner < TILE + HALO, inner, inner - GROUP)


def roll(x, shift):
    shift = shift % LANES
    return x if shift == 0 else pltpu.roll(x, shift, 1)


def quad_transpose(v, lane):
    group = lane // TILE
    out = []
    for t in range(4):
        value = roll(v[0], -TILE * t)
        for g in range(1, 4):
            value = jnp.where(group == g, roll(v[g], TILE * (g - t)), value)
        out.append(value)
    return out


def dest_of(dest_of_tile, c):
    return jnp.where(lax.rem(lax.axis_index("tx"), 2) == 0, dest_of_tile[c], dest_of_tile[-1 - c])


def pack_half(dest_of_tile, rows, half, groups, src_ref, out_ref):
    lane = lane_iota((SUB, LANES))
    tiles_half = LANES // TILE
    for i in range(groups):
        for quad in range(rows // 4):
            v = [src_ref[pl.ds(i * rows * SUB + 4 * quad + r, SUB, stride=rows), :] for r in QUAD_ROWS]
            for t, piece in enumerate(quad_transpose(v, lane)):
                dest = dest_of(dest_of_tile, half * tiles_half + t)
                out_ref[dest, i * SUB : (i + 1) * SUB, quad * LANES : (quad + 1) * LANES] = piece


def pack_kernel(dest_of_tile, rows, data_ref, out_ref):
    for half in range(len(dest_of_tile) * TILE // LANES):

        @pl.when(pl.program_id(0) == half)
        def _(half=half):
            pack_half(dest_of_tile, rows, half, data_ref.shape[0] // (rows * SUB), data_ref, out_ref)


def estimate_kernel(dest_of_tile, rows, pat, est_ref, out_ref, all_ref):
    halves = len(dest_of_tile) * TILE // LANES
    for half in range(halves):

        @pl.when(pl.program_id(0) == half)
        def _(half=half):
            pack_half(dest_of_tile, rows, half, est_ref.shape[0] // (rows * SUB), est_ref, all_ref)
            if half == halves - 1:
                for i in range(out_ref.shape[0]):
                    out_ref[i] = all_ref[i * pat + lax.axis_index("pat")]


def edge_messages(pieces, lane):
    left = right = None
    for u, (v, offset) in enumerate(pieces):
        slot = (lane // HALO) % 4 == u
        l_u, r_u = roll(v, HALO * u - offset), roll(v, HALO * (u - 1) - offset)
        left = l_u if left is None else jnp.where(slot, l_u, left)
        right = r_u if right is None else jnp.where(slot, r_u, right)
    return left, right


def edges_kernel(src_of, in_ref, left_ref, right_ref):
    lane = lane_iota((SUB, LANES))
    ty, pat = src_of
    groups = in_ref.shape[1] // SUB
    per_ty = in_ref.shape[2] // LANES // 2
    for k in range(pat):
        for g in range(groups):
            row = slice((k * groups + g) * SUB, (k * groups + g + 1) * SUB)
            for i in range(ty):
                for pair in range(per_ty):
                    pieces = []
                    for q in (2 * pair, 2 * pair + 1):
                        v = in_ref[i * pat + k, g * SUB : (g + 1) * SUB, q * LANES : (q + 1) * LANES]
                        pieces += [(v, 0), (v, TILE)]
                    left, right = edge_messages(pieces, lane)
                    vreg = i * per_ty + pair
                    left_ref[row, vreg * LANES : (vreg + 1) * LANES] = left
                    right_ref[row, vreg * LANES : (vreg + 1) * LANES] = right


def unpack_wide(src_of, in_ref, from_left_ref, from_right_ref, out_ref):
    lane = lane_iota((SUB, LANES))
    ty, pat = src_of
    groups = in_ref.shape[1] // SUB
    per_ty = in_ref.shape[2] // LANES // 2
    for k in range(pat):
        for g in range(groups):
            row = slice((k * groups + g) * SUB, (k * groups + g + 1) * SUB)
            for i in range(ty):
                for pair in range(per_ty):
                    vreg = i * per_ty + pair
                    from_left = from_left_ref[row, vreg * LANES : (vreg + 1) * LANES]
                    from_right = from_right_ref[row, vreg * LANES : (vreg + 1) * LANES]
                    own = []
                    for q in (2 * pair, 2 * pair + 1):
                        v = in_ref[i * pat + k, g * SUB : (g + 1) * SUB, q * LANES : (q + 1) * LANES]
                        own += [v, roll(v, -TILE)]
                    for u in range(4):
                        m = 4 * vreg + u
                        out_ref[m // 2, row, (m % 2) * LANES : (m % 2 + 1) * LANES] = with_halo(
                            own[u], u, from_right, from_left, lane
                        )


def with_halo(own, u, from_right, from_left, lane):
    inner = lane % GROUP
    value = jnp.where(inner < TILE, own, roll(from_right, HALO * (2 - u)))
    return jnp.where(inner < TILE + HALO, value, roll(from_left, HALO * (3 - u)))


def tables_kernel(tile_of, k_ref, radius_ref, codes_ref, axial_ref, w_ref, fwd_ref, bwd_ref, light_ref):
    lane = lane_iota((GROUP, LANES))
    row = lax.broadcasted_iota(jnp.int32, (GROUP, LANES), 0)
    tap = column_of(row) - column_of(lane) + RADIUS
    first = lane < GROUP
    hit = [tap == j for j in range(TAPS)]
    nothing = jnp.zeros((GROUP, LANES), BF16)

    def scalar(flip, i, j):
        if i < 0 or i >= TAPS:
            return jnp.float32(0.0)
        if flip:
            i, j = TAPS - 1 - i, TAPS - 1 - j
        return jnp.where(abs(j - RADIUS) <= radius_ref[i], k_ref[i, j], 0.0)

    for flip in range(2):
        for i0 in range(-2, TAPS + 3):
            value = jnp.zeros((GROUP, LANES), F32)
            if 0 <= i0 <= TAPS:
                for j in range(TAPS):
                    both = jnp.where(first, scalar(flip, i0, j), scalar(flip, i0 - 1, j))
                    value = jnp.where(hit[j], both, value)
            value = value.astype(BF16)
            for k in range(3):
                for r in range(ROWS_BLOCK):
                    for q in range(ROWS_BLOCK // 2):
                        if ROWS_BLOCK * (k - 1) + r - 2 * q + RADIUS == i0:
                            w_ref[
                                3 * flip + k,
                                r * GROUP : (r + 1) * GROUP,
                                q * LANES : (q + 1) * LANES,
                            ] = value

    planes, rows = axial_ref.shape[0], fwd_ref.shape[0]
    axial = axial_ref[...].astype(BF16)
    pick = lax.broadcasted_iota(jnp.int32, (planes, rows), 1) % planes
    pick = (pick == lax.broadcasted_iota(jnp.int32, (planes, rows), 0)).astype(F32).astype(BF16)
    plain = jnp.dot(axial, pick, preferred_element_type=F32)
    turned = lax.dot_general(axial, pick, (((0,), (0,)), ((), ())), preferred_element_type=F32)
    column = lax.broadcasted_iota(jnp.int32, (planes, rows), 1)
    for p in range(rows // planes):
        here = column // planes == p
        fwd_ref[p * planes : (p + 1) * planes] = jnp.where(here, plain, 0.0).astype(BF16)
    span = 3 * planes
    for h in range(2):
        here = (column >= h * span) & (column < (h + 1) * span)
        bwd_ref[h * planes : (h + 1) * planes] = jnp.where(here, turned, 0.0).astype(BF16)[:, : 2 * span]

    col = column_of(lane_iota((1, BLOCK)))
    within = lane_iota((1, BLOCK)) // GROUP
    x = tile_of() * TILE + col
    cosines = [0.7 * math.cos(TWO_PI * m / 5.0) for m in range(5)]
    patterns = light_ref.shape[1]
    for p in range(patterns):
        angle, phase = codes_ref[0, p], codes_ref[1, p]
        step_col = jnp.where(angle == 0, 2, -1)
        step_row = jnp.where(angle == 0, 0, jnp.where(angle == 1, 2, -2))
        for b in range(light_ref.shape[0]):
            y = within + b * ROWS_BLOCK
            turn = lax.rem(step_col * x + step_row * y + phase + 5 * OFFSET, 5)
            value = jnp.full((1, BLOCK), cosines[0], F32)
            for m in range(1, 5):
                value = jnp.where(turn == m, cosines[m], value)
            light_ref[b, p : p + 1] = value


def lateral(src_ref, w_ref, flip, b, count):
    total = None
    for k in range(3):
        v = src_ref[b + k : b + k + count]
        part = jnp.dot(v.reshape(-1, BLOCK), w_ref[3 * flip + k], preferred_element_type=F32)
        total = part if total is None else total + part
    return total.reshape(count, -1, BLOCK)


def split3(v):
    high = v.astype(BF16)
    rest = v - high.astype(F32)
    mid = rest.astype(BF16)
    return high, mid, (rest - mid.astype(F32)).astype(BF16)


class Step:
    def __init__(self, nx, tile_of, w_ref, ax_fwd, ax_bwd, light_ref, wave_ref):
        self.w, self.ax_fwd, self.ax_bwd, self.light, self.wave = w_ref, ax_fwd, ax_bwd, light_ref, wave_ref
        self.blocks, self.patterns = light_ref.shape[0], light_ref.shape[1]
        self.planes = wave_ref.shape[0]
        self.col = column_of(lane_iota((1, BLOCK)))
        place = tile_of() * TILE + self.col
        self.inside = (place >= 0) & (place < nx)

    def reach(self, width):
        return self.inside & (self.col >= -width) & (self.col < TILE + width)

    def clear_ends(self, ref):
        ref[0] = jnp.zeros(ref.shape[1:], BF16)
        ref[self.blocks + 1] = jnp.zeros(ref.shape[1:], BF16)

    def normalizer(self, norm_ref):
        depth = self.ax_bwd.shape[1]
        ones = lax.broadcasted_iota(jnp.int32, (depth, BLOCK), 0) < self.planes
        ones = jnp.where(ones, 1.0, 0.0).astype(BF16)
        colsum = jnp.dot(self.ax_bwd[...], ones, preferred_element_type=F32)[: self.planes]
        ones = jnp.broadcast_to(jnp.where(self.inside, 1.0, 0.0), (2 * SUB, BLOCK)).astype(BF16)
        parts = [jnp.dot(ones, self.w[3 + k], preferred_element_type=F32) for k in range(3)]
        for b in range(self.blocks):
            total = sum(parts[k] for k in range(3) if 0 <= b + k - 1 < self.blocks)
            cover = total.astype(BF16).astype(F32)[0:1]
            lat_sum = jnp.sum(self.light[b], axis=0, keepdims=True)
            norm_ref[b] = colsum * cover * (float(self.patterns) + lat_sum * self.wave[...])

    def blur(self, obj_ref, stage_ref):
        for b in range(self.blocks):
            lighting = 1.0 + self.light[b][:, None, :] * self.wave[...][None]
            lit = (lighting * obj_ref[b][None]).astype(BF16).reshape(-1, BLOCK)
            stage_ref[b + 1] = jnp.dot(self.ax_fwd[...], lit, preferred_element_type=F32).astype(BF16)

    def compare(self, stage_ref, data_ref, quot_ref, width, predicted_ref=None):
        ok = self.reach(width)[None]
        acc = jnp.zeros((SUB, BLOCK), F32)
        for b in range(0, self.blocks, CHUNK):
            if predicted_ref is None:
                predicted = lateral(stage_ref, self.w, 0, b, CHUNK)
            else:
                predicted = predicted_ref[b : b + CHUNK]
            data = data_ref[b : b + CHUNK]
            miss = data - predicted
            acc = acc + jnp.sum((miss * miss).reshape(-1, SUB, BLOCK), axis=0)
            quot_ref[b + 1 : b + 1 + CHUNK] = jnp.where(ok, data / predicted, 0.0).astype(BF16)
        row = jnp.sum(jnp.where((self.col >= 0) & (self.col < TILE), acc, 0.0), axis=0, keepdims=True)
        return sum(row[:, h * LANES : (h + 1) * LANES] for h in range(BLOCK // LANES))

    def update(self, quot_ref, obj_ref, norm_ref, width):
        ok = self.reach(width)
        for b0 in range(0, self.blocks, CHUNK):
            back = lateral(quot_ref, self.w, 1, b0, CHUNK).astype(BF16)
            for b in range(b0, b0 + CHUNK):
                part = back[b - b0].astype(F32).reshape(self.patterns, self.planes, BLOCK)
                plain = jnp.sum(part, axis=0)
                waved = jnp.sum(self.light[b][:, None, :] * part, axis=0)
                stack = jnp.concatenate(split3(plain) + split3(waved), axis=0)
                both = jnp.dot(self.ax_bwd[...], stack, preferred_element_type=F32)
                summed = both[: self.planes] + self.wave[...] * both[self.planes :]
                obj_ref[b] = jnp.where(ok, obj_ref[b] * summed / norm_ref[b], 0.0)


def put_halo(own_ref, from_left_ref, from_right_ref, out_ref):
    lane = lane_iota((SUB, LANES))
    for z in range(0, out_ref.shape[1], SUB):
        for vreg in range(out_ref.shape[0] // 2):
            from_left = from_left_ref[z : z + SUB, vreg * LANES : (vreg + 1) * LANES]
            from_right = from_right_ref[z : z + SUB, vreg * LANES : (vreg + 1) * LANES]
            for u in range(4):
                m = 4 * vreg + u
                at = (m // 2, slice(z, z + SUB), slice((m % 2) * LANES, (m % 2 + 1) * LANES))
                out_ref[at] = with_halo(own_ref[at], u, from_right, from_left, lane)


def forward_kernel(nx, tile_of, src_of, w_ref, ax_fwd, ax_bwd, light_ref, wave_ref,
                   est_ref, from_left_ref, from_right_ref, obj_ref, norm_ref, predicted_ref, stage_ref):
    unpack_wide(src_of, est_ref, from_left_ref, from_right_ref, obj_ref)
    step = Step(nx, tile_of, w_ref, ax_fwd, ax_bwd, light_ref, wave_ref)
    step.normalizer(norm_ref)
    step.clear_ends(stage_ref)
    step.blur(obj_ref, stage_ref)
    for b in range(0, step.blocks, CHUNK):
        predicted_ref[b : b + CHUNK] = lateral(stage_ref, w_ref, 0, b, CHUNK)


def first_kernel(nx, tile_of, src_of, w_ref, ax_fwd, ax_bwd, light_ref, wave_ref, norm_ref, obj_in_ref,
                 predicted_ref, in_ref, from_left_ref, from_right_ref, data_ref, obj_ref, left_ref, right_ref,
                 sq_ref, stage_ref, quot_ref):
    unpack_wide(src_of, in_ref, from_left_ref, from_right_ref, data_ref)
    step = Step(nx, tile_of, w_ref, ax_fwd, ax_bwd, light_ref, wave_ref)
    step.clear_ends(stage_ref)
    step.clear_ends(quot_ref)
    obj_ref[...] = obj_in_ref[...]
    sq_ref[...] = jnp.zeros(sq_ref.shape, F32)
    sq_ref[0:1] = step.compare(None, data_ref, quot_ref, 12, predicted_ref)
    step.update(quot_ref, obj_ref, norm_ref, 8)
    step.blur(obj_ref, stage_ref)
    sq_ref[1:2] = step.compare(stage_ref, data_ref, quot_ref, 4)
    step.update(quot_ref, obj_ref, norm_ref, 0)

    lane = lane_iota((SUB, LANES))
    for z in range(0, step.planes, SUB):
        for vreg in range(step.blocks // 2):
            pieces = []
            for u in range(4):
                m = 4 * vreg + u
                pieces.append((obj_ref[m // 2, z : z + SUB, (m % 2) * LANES : (m % 2 + 1) * LANES], 0))
            left, right = edge_messages(pieces, lane)
            left_ref[z : z + SUB, vreg * LANES : (vreg + 1) * LANES] = left
            right_ref[z : z + SUB, vreg * LANES : (vreg + 1) * LANES] = right


def second_kernel(nx, tile_of, src_of, w_ref, ax_fwd, ax_bwd, light_ref, wave_ref, norm_ref, data_ref,
                  obj_in_ref, from_left_ref, from_right_ref, sq_in_ref, out_ref, obj_ref, stage_ref, quot_ref):
    put_halo(obj_in_ref, from_left_ref, from_right_ref, obj_ref)
    step = Step(nx, tile_of, w_ref, ax_fwd, ax_bwd, light_ref, wave_ref)
    step.clear_ends(stage_ref)
    step.clear_ends(quot_ref)
    squares = [sq_in_ref[0:1], sq_in_ref[1:2]]
    for quot_width, obj_width in ((12, 8), (4, 0)):
        step.blur(obj_ref, stage_ref)
        squares.append(step.compare(stage_ref, data_ref, quot_ref, quot_width))
        step.update(quot_ref, obj_ref, norm_ref, obj_width)

    ty, pat = src_of
    quads = step.blocks // ty
    lane = lane_iota((SUB, LANES))
    own = (lane // TILE) % 2 == 0
    last = jnp.concatenate(squares + [jnp.zeros((SUB - len(squares), LANES), F32)], axis=0)
    for i in range(ty):
        for k in range(pat):
            out_ref[i * pat + k, quads * step.planes : quads * step.planes + SUB] = last
        for q in range(quads):
            for z in range(0, step.planes, SUB):
                v0 = obj_ref[i * quads + q, z : z + SUB, 0:LANES]
                v1 = obj_ref[i * quads + q, z : z + SUB, LANES : 2 * LANES]
                v = jnp.where(own, v0, roll(v1, TILE))
                for k in range(pat):
                    out_ref[i * pat + k, q * step.planes + z : q * step.planes + z + SUB] = v


def final_kernel(dest_of_tile, rows, in_ref, out_ref):
    lane = lane_iota((SUB, LANES))
    planes = out_ref.shape[0] // rows
    tiles_half = LANES // TILE
    quads = rows // 4
    for half in range(len(dest_of_tile) // tiles_half):

        @pl.when(pl.program_id(0) == half)
        def _(half=half):
            for z in range(0, planes, SUB):
                for quad in range(quads):
                    row = quad * planes + z
                    v = [in_ref[dest_of(dest_of_tile, half * tiles_half + t), row : row + SUB] for t in range(tiles_half)]
                    for g, piece in enumerate(quad_transpose(v, lane)):
                        out_ref[pl.ds(z * rows + 4 * quad + QUAD_ROWS[g], SUB, stride=rows), :] = piece


def masked_kernel(lateral_kernel, psf_radius):
    offsets = jnp.arange(TAPS) - RADIUS
    within = jnp.abs(offsets)[None, :] <= psf_radius[:, None]
    return jnp.where(within, lateral_kernel, jnp.zeros_like(lateral_kernel)).astype(BF16)


def shape(dims, dtype=F32):
    return jax.ShapeDtypeStruct(dims, dtype)


PARAMS = pltpu.CompilerParams(vmem_limit_bytes=24 * 2**20)
VMEM = pl.BlockSpec(memory_space=pltpu.VMEM)
SMEM = pl.BlockSpec(memory_space=pltpu.SMEM)


def over_tx(value, size):
    if size & (size - 1):
        return lax.psum(value, "tx")
    step = 1
    while step < size:
        value = value + lax.ppermute(value, "tx", [(i, i ^ step) for i in range(size)])
        step *= 2
    return value


def tiled_device(sizes, estimate, data, axial, lateral_kernel, psf_radius, pattern_codes):
    ty, tx, pat = sizes["ty"], sizes["tx"], sizes["pat"]
    planes, rows, cols = estimate.shape
    pat_local = data.shape[0]
    patterns = pat_local * pat
    ny, nx = rows * ty, cols * tx
    members = ty * pat
    blocks = ny // ROWS_BLOCK
    axes = ("ty", "tx", "pat")

    owner = [(i, k if i % 2 == 0 else pat - 1 - k) for i in range(ty) for k in range(pat)]
    dest_of_tile = [i * pat + k for i, k in owner]
    order = [(i * tx + j) * pat + k for j in range(tx) for i, k in (owner if j % 2 == 0 else owner[::-1])]
    to_right = [(a, b) for a, b in zip(order[:-1], order[1:])]
    to_left = [(b, a) for a, b in to_right]
    src_of = (ty, pat)

    ti = lax.axis_index("ty")

    def tile_of():
        i, j, k = (lax.axis_index(a) for a in axes)
        c = i * pat + jnp.where(lax.rem(i, 2) == 0, k, pat - 1 - k)
        return j * members + jnp.where(lax.rem(j, 2) == 0, c, members - 1 - c)

    halves = cols // LANES
    piece_lanes = rows * TILE
    halo_lanes = ny * HALO

    def whole(dims):
        return pl.BlockSpec(dims, lambda h: (0,) * len(dims))

    def half_columns(height):
        return pl.BlockSpec((height, LANES), lambda h: (0, h))

    def edges(pieces, name):
        out = shape((pieces.shape[1] * pieces.shape[0] // ty, halo_lanes))
        return pl.pallas_call(
            functools.partial(edges_kernel, (ty, pieces.shape[0] // ty)),
            out_shape=(out, out),
            in_specs=[VMEM],
            out_specs=(VMEM,) * 2,
            compiler_params=PARAMS,
            name=name,
        )(pieces)

    def swap_edges(left, right):
        return lax.ppermute(right, axes, to_right), lax.ppermute(left, axes, to_left)

    message = pl.pallas_call(
        functools.partial(pack_kernel, dest_of_tile, rows),
        out_shape=shape((members, pat_local * planes, piece_lanes)),
        grid=(halves,),
        in_specs=[half_columns(data.size // cols)],
        out_specs=whole((members, pat_local * planes, piece_lanes)),
        compiler_params=PARAMS,
        name="pack",
    )(data.reshape(-1, cols))
    message, estimate = lax.optimization_barrier((message, estimate))
    mine = lax.all_to_all(message, ("ty", "pat"), 0, 0, tiled=True)

    pieces = pl.pallas_call(
        functools.partial(estimate_kernel, dest_of_tile, rows, pat),
        out_shape=shape((ty, planes, piece_lanes)),
        grid=(halves,),
        in_specs=[half_columns(planes * rows)],
        out_specs=whole((ty, planes, piece_lanes)),
        scratch_shapes=[pltpu.VMEM((members, planes, piece_lanes), F32)],
        compiler_params=PARAMS,
        name="prep_estimate",
    )(estimate.reshape(-1, cols))
    tile_rows = [lax.dynamic_index_in_dim(pieces, ti, 0, keepdims=False)]
    for shift in range(1, ty):
        sent = lax.dynamic_index_in_dim(pieces, (ti + shift) % ty, 0, keepdims=False)
        tile_rows.append(lax.ppermute(sent, "ty", [(i, (i + shift) % ty) for i in range(ty)]))
    tile_rows = jnp.stack(tile_rows)
    tile_rows = jnp.stack(
        [lax.dynamic_index_in_dim(tile_rows, (ti - i) % ty, 0, keepdims=False) for i in range(ty)]
    )
    est_left, est_right = swap_edges(*edges(tile_rows, "prep_edges"))

    weights, ax_fwd, ax_bwd, light = pl.pallas_call(
        functools.partial(tables_kernel, tile_of),
        out_shape=(
            shape((6, BLOCK, BLOCK), BF16),
            shape((patterns * planes, patterns * planes), BF16),
            shape((2 * planes, 6 * planes), BF16),
            shape((blocks, patterns, BLOCK)),
        ),
        in_specs=[SMEM] * 3 + [VMEM],
        out_specs=(VMEM,) * 4,
        compiler_params=PARAMS,
        name="tables",
    )(lateral_kernel, psf_radius, pattern_codes, axial)
    wave = np.cos(np.arange(planes, dtype=np.float32) * np.float32(TWO_PI * 3.0 / planes))
    wave = jnp.asarray(np.ascontiguousarray(np.broadcast_to(wave[:, None], (planes, BLOCK))))

    object_shape = shape((blocks, planes, BLOCK))
    field_shape = shape((blocks, patterns * planes, BLOCK))
    object_scratch = pltpu.VMEM(object_shape.shape, F32)
    stage = pltpu.VMEM((blocks + 2, patterns * planes, BLOCK), BF16)
    table_specs = [VMEM] * 5
    mine, est_left, est_right, weights = lax.optimization_barrier((mine, est_left, est_right, weights))
    from_left, from_right = swap_edges(*edges(mine, "edges"))
    tables = (weights, ax_fwd, ax_bwd, light, wave)
    current, norm, predicted = pl.pallas_call(
        functools.partial(forward_kernel, nx, tile_of, (ty, 1)),
        out_shape=(object_shape, object_shape, field_shape),
        in_specs=table_specs + [VMEM] * 3,
        out_specs=(VMEM,) * 3,
        scratch_shapes=[stage],
        compiler_params=PARAMS,
        name="forward",
    )(*tables, tile_rows, est_left, est_right)

    edge_shape = shape((planes, halo_lanes))
    data_all, current, left, right, sq_first = pl.pallas_call(
        functools.partial(first_kernel, nx, tile_of, src_of),
        out_shape=(field_shape, object_shape, edge_shape, edge_shape, shape((SUB, LANES))),
        in_specs=table_specs + [VMEM] * 6,
        out_specs=(VMEM,) * 5,
        scratch_shapes=[stage, stage],
        compiler_params=PARAMS,
        name="first",
    )(*tables, norm, current, predicted, mine, from_left, from_right)
    from_left, from_right = swap_edges(left, right)
    outgoing = pl.pallas_call(
        functools.partial(second_kernel, nx, tile_of, src_of),
        out_shape=shape((members, rows // 4 * planes + SUB, LANES)),
        in_specs=table_specs + [VMEM] * 6,
        out_specs=VMEM,
        scratch_shapes=[object_scratch, stage, stage],
        compiler_params=PARAMS,
        name="second",
    )(*tables, norm, data_all, current, from_left, from_right, sq_first)

    incoming = lax.all_to_all(outgoing, ("ty", "pat"), 0, 0, tiled=True)
    squares = jnp.sum(incoming[:, rows // 4 * planes : rows // 4 * planes + ITERS], axis=(0, 2))
    squares = over_tx(squares, tx)
    result = pl.pallas_call(
        functools.partial(final_kernel, dest_of_tile, rows),
        out_shape=shape((planes * rows, cols)),
        grid=(halves,),
        in_specs=[whole(incoming.shape)],
        out_specs=half_columns(planes * rows),
        compiler_params=PARAMS,
        name="unpack",
    )(incoming)
    cell_count = float(patterns * planes * ny * nx)
    return result.reshape(estimate.shape), jnp.sqrt(squares / cell_count)


def extended(block, sides, width):
    for axis, dim in sides:
        count = lax.axis_size(axis)
        forward = [(i, i + 1) for i in range(count - 1)]
        backward = [(target, source) for source, target in forward]
        low = lax.ppermute(
            lax.slice_in_dim(block, block.shape[dim] - width, None, axis=dim), axis, forward
        )
        high = lax.ppermute(lax.slice_in_dim(block, 0, width, axis=dim), axis, backward)
        block = jnp.concatenate([low, block, high], axis=dim)
    return block


def wave_table(angle_code, phase_code, row_coord, col_coord, planes):
    step_col = jnp.where(angle_code == 0, 2, -1).astype(jnp.int32)
    step_row = jnp.where(angle_code == 0, 0, jnp.where(angle_code == 1, 2, -2)).astype(jnp.int32)
    argument = (
        step_col[:, None, None] * col_coord[None, None, :]
        + step_row[:, None, None] * row_coord[None, :, None]
        + phase_code[:, None, None]
    ) % 5
    lateral_wave = jnp.cos(argument.astype(jnp.float32) * (TWO_PI / 5.0))
    plane_index = jnp.arange(planes).astype(jnp.float32)
    axial_wave = jnp.cos(plane_index * (TWO_PI * 3.0 / planes))
    return 1.0 + 0.7 * lateral_wave[:, None, :, :] * axial_wave[None, :, None, None]


def tap_matrices(kernel, width_in, width_out):
    tap_count = 2 * RADIUS + 1
    offset = jnp.arange(width_in)[:, None] - jnp.arange(width_out)[None, :]
    onehot = (offset[None, :, :] == jnp.arange(tap_count)[:, None, None]).astype(jnp.float32)
    return jnp.einsum(
        "ij,jab->iab", kernel.astype(jnp.float32), onehot, precision=lax.Precision.HIGHEST
    ).astype(jnp.bfloat16)


def lateral_pass(padded, matrices, height):
    summed = None
    for tap_row in range(2 * RADIUS + 1):
        window = padded[..., tap_row : tap_row + height, :]
        product = jnp.dot(window, matrices[tap_row], preferred_element_type=jnp.float32)
        summed = product if summed is None else summed + product
    return summed


def general_device(estimate, data, axial, lateral_kernel, psf_radius, pattern_codes):
    planes, height, width = estimate.shape
    pat_local = data.shape[0]
    full_rows = height * lax.axis_size("ty")
    full_cols = width * lax.axis_size("tx")
    depth = 2 * RADIUS
    margin = depth - RADIUS
    row_coord = lax.axis_index("ty") * height - depth + jnp.arange(height + 2 * depth)
    col_coord = lax.axis_index("tx") * width - depth + jnp.arange(width + 2 * depth)
    codes_here = lax.dynamic_slice_in_dim(
        pattern_codes, lax.axis_index("pat") * pat_local, pat_local, 1
    )
    lighting = wave_table(codes_here[0], codes_here[1], row_coord, col_coord, planes)
    lighting_inner = lighting[:, :, depth : depth + height, depth : depth + width]
    kernel = masked_kernel(lateral_kernel, psf_radius)
    forward_taps = tap_matrices(kernel, width + 2 * depth, width + 2 * margin)
    adjoint_taps = tap_matrices(kernel[::-1, ::-1], width + 2 * RADIUS, width)
    axial_b = axial.astype(jnp.bfloat16)
    row_inside = (row_coord >= 0) & (row_coord < full_rows)
    col_inside = (col_coord >= 0) & (col_coord < full_cols)
    inside_all = row_inside[:, None] & col_inside[None, :]
    inside = inside_all[
        margin : margin + height + 2 * RADIUS, margin : margin + width + 2 * RADIUS
    ].astype(jnp.bfloat16)
    inside_mid = inside_all[
        RADIUS : RADIUS + height + 2 * margin, RADIUS : RADIUS + width + 2 * margin
    ]
    coverage = lateral_pass(inside[None], adjoint_taps, height).astype(jnp.bfloat16)
    spread = jnp.einsum(
        "ba,byx->ayx",
        axial_b,
        jnp.broadcast_to(coverage, (planes, height, width)),
        preferred_element_type=jnp.float32,
    )
    normalizer = lax.psum(jnp.sum(lighting_inner * spread[None], axis=0), "pat")
    cell_count = float(pat_local * lax.axis_size("pat") * planes * full_rows * full_cols)
    data_wide = extended(data, (("ty", 2), ("tx", 3)), RADIUS)
    current = estimate
    squares_list = []
    for iteration in range(ITERS):
        padded = extended(current, (("ty", 1), ("tx", 2)), depth)
        lighted = (lighting * padded[None]).astype(jnp.bfloat16)
        blurred = jnp.einsum(
            "ab,pbyx->payx", axial_b, lighted, preferred_element_type=jnp.float32
        ).astype(jnp.bfloat16)
        predicted = lateral_pass(blurred, forward_taps, height + 2 * margin)
        predicted_inner = predicted[:, :, margin : margin + height, margin : margin + width]
        misfit = data - predicted_inner
        local_square = jnp.sum(misfit * misfit)
        safe = jnp.where(inside_mid[None, None], predicted, 1.0)
        quotient_padded = jnp.where(inside_mid[None, None], data_wide / safe, 0.0).astype(
            jnp.bfloat16
        )
        backward = lateral_pass(quotient_padded, adjoint_taps, height).astype(jnp.bfloat16)
        gathered = jnp.einsum(
            "ba,pbyx->payx", axial_b, backward, preferred_element_type=jnp.float32
        )
        contribution = jnp.sum(lighting_inner * gathered, axis=0)
        summed = lax.psum(contribution, "pat")
        current = current * summed / normalizer
        squares_list.append(lax.psum(local_square, ("ty", "tx", "pat")))
    squares = jnp.stack(squares_list)
    return (current, jnp.sqrt(squares / cell_count))


def solution(mesh):
    sizes = dict(mesh.shape)
    in_specs = (P(None, "ty", "tx"), P("pat", None, "ty", "tx"), P(), P(), P(), P())
    out_specs = (P(None, "ty", "tx"), P())

    def per_device(estimate, data, *rest):
        planes, rows, cols = estimate.shape
        members = sizes["ty"] * sizes["pat"]
        fits = (
            cols == members * TILE
            and cols % LANES == 0
            and rows % 8 == 0
            and rows * sizes["ty"] <= 2 * TILE
            and planes == sizes["pat"] * SUB
        )
        if fits:
            return tiled_device(sizes, estimate, data, *rest)
        return general_device(estimate, data, *rest)

    return jax.shard_map(
        per_device, mesh=mesh, in_specs=in_specs, out_specs=out_specs, check_vma=False
    )
```

```python
import functools
import math

import jax
import jax.numpy as jnp
import numpy as np
from jax import lax
from jax.experimental import pallas as pl
from jax.experimental.pallas import tpu as pltpu
from jax.sharding import PartitionSpec as P

RADIUS = 4
TAPS = 2 * RADIUS + 1
ITERS = 4
TWO_PI = 2.0 * math.pi

TILE = 32
HALO = 16
GROUP = TILE + 2 * HALO
ROWS_BLOCK = RADIUS
BLOCK = ROWS_BLOCK * GROUP
LANES = 128
SUB = 8
QUAD_ROWS = (0, 2, 1, 3)
CHUNK = 4
OFFSET = 1 << 20
F32 = jnp.float32
BF16 = jnp.bfloat16


def lane_iota(shape):
    return lax.broadcasted_iota(jnp.int32, shape, len(shape) - 1)


def column_of(lane):
    inner = lane % GROUP
    return jnp.where(inner < TILE + HALO, inner, inner - GROUP)


def roll(x, shift):
    shift = shift % LANES
    return x if shift == 0 else pltpu.roll(x, shift, 1)


def quad_transpose(v, lane):
    group = lane // TILE
    out = []
    for t in range(4):
        value = roll(v[0], -TILE * t)
        for g in range(1, 4):
            value = jnp.where(group == g, roll(v[g], TILE * (g - t)), value)
        out.append(value)
    return out


def dest_of(dest_of_tile, c):
    return jnp.where(lax.rem(lax.axis_index("tx"), 2) == 0, dest_of_tile[c], dest_of_tile[-1 - c])


def pack_half(dest_of_tile, rows, half, groups, src_ref, out_ref):
    lane = lane_iota((SUB, LANES))
    tiles_half = LANES // TILE
    for i in range(groups):
        for quad in range(rows // 4):
            v = [src_ref[pl.ds(i * rows * SUB + 4 * quad + r, SUB, stride=rows), :] for r in QUAD_ROWS]
            for t, piece in enumerate(quad_transpose(v, lane)):
                dest = dest_of(dest_of_tile, half * tiles_half + t)
                out_ref[dest, i * SUB : (i + 1) * SUB, quad * LANES : (quad + 1) * LANES] = piece


DATA_LOW, DATA_HIGH, TOP = 0.1, 6.0, 2**24 - 1
DATA_SCALE = TOP / (DATA_HIGH - DATA_LOW)
BIAS = 2**15


def to_fixed(v):
    return jnp.clip((v - DATA_LOW) * DATA_SCALE + 0.5, 0.0, float(TOP)).astype(jnp.int32)


def from_fixed(t):
    return t.astype(F32) * (1.0 / DATA_SCALE) + DATA_LOW


def encode(first, second):
    low = ((first & 255) << 8) + (second & 255)
    return tuple((v - BIAS).astype(jnp.int16) for v in (first >> 8, second >> 8, low))


def decode(first, second, low):
    first, second, low = (v.astype(jnp.int32) + BIAS for v in (first, second, low))
    return (first << 8) + (low >> 8), (second << 8) + (low & 255)


def pack_kernel(dest_of_tile, rows, data_ref, out_ref):
    lane = lane_iota((SUB, LANES))
    tiles_half = LANES // TILE
    part = out_ref.shape[1] // 3
    per_pattern = part // SUB

    def pieces(group, quad):
        start = group * rows * SUB + 4 * quad
        v = [to_fixed(data_ref[pl.ds(start + r, SUB, stride=rows), :]) for r in QUAD_ROWS]
        return quad_transpose(v, lane)

    for half in range(len(dest_of_tile) // tiles_half):

        @pl.when(pl.program_id(0) == half)
        def _(half=half):
            for g in range(0, per_pattern, 2):
                for quad in range(rows // 4):
                    a0, a1 = pieces(g, quad), pieces(g + 1, quad)
                    b0, b1 = pieces(per_pattern + g, quad), pieces(per_pattern + g + 1, quad)
                    for t in range(tiles_half):
                        dest = dest_of(dest_of_tile, half * tiles_half + t)
                        coded = encode(jnp.concatenate([a0[t], a1[t]]), jnp.concatenate([b0[t], b1[t]]))
                        for n, v in enumerate(coded):
                            row = n * part + g * SUB
                            out_ref[dest, row : row + 2 * SUB, quad * LANES : (quad + 1) * LANES] = v


def estimate_kernel(dest_of_tile, rows, pat, est_ref, out_ref, all_ref):
    halves = len(dest_of_tile) * TILE // LANES
    for half in range(halves):

        @pl.when(pl.program_id(0) == half)
        def _(half=half):
            pack_half(dest_of_tile, rows, half, est_ref.shape[0] // (rows * SUB), est_ref, all_ref)
            if half == halves - 1:
                for i in range(out_ref.shape[0]):
                    out_ref[i] = all_ref[i * pat + lax.axis_index("pat")]


def edge_messages(pieces, lane):
    left = right = None
    for u, (v, offset) in enumerate(pieces):
        slot = (lane // HALO) % 4 == u
        l_u, r_u = roll(v, HALO * u - offset), roll(v, HALO * (u - 1) - offset)
        left = l_u if left is None else jnp.where(slot, l_u, left)
        right = r_u if right is None else jnp.where(slot, r_u, right)
    return left, right


def edges_kernel(src_of, in_ref, left_ref, right_ref):
    lane = lane_iota((SUB, LANES))
    ty, pat = src_of
    groups = in_ref.shape[1] // SUB
    per_ty = in_ref.shape[2] // LANES // 2
    for k in range(pat):
        for g in range(groups):
            row = slice((k * groups + g) * SUB, (k * groups + g + 1) * SUB)
            for i in range(ty):
                for pair in range(per_ty):
                    pieces = []
                    for q in (2 * pair, 2 * pair + 1):
                        v = in_ref[i * pat + k, g * SUB : (g + 1) * SUB, q * LANES : (q + 1) * LANES]
                        pieces += [(v, 0), (v, TILE)]
                    left, right = edge_messages(pieces, lane)
                    vreg = i * per_ty + pair
                    left_ref[row, vreg * LANES : (vreg + 1) * LANES] = left
                    right_ref[row, vreg * LANES : (vreg + 1) * LANES] = right


def coded_rows(k, g, part, pat):
    first = 2 * k * part + g
    return [slice(r, r + 2 * SUB) for r in (first, first + part, 2 * pat * part + k * part + g)]


def own_coded(in_ref, source, g, part, q):
    rows = [slice(n * part + g, n * part + g + 2 * SUB) for n in range(3)]
    return decode(*(in_ref[source, r, q * LANES : (q + 1) * LANES] for r in rows))


def data_edges_kernel(src_of, in_ref, left_ref, right_ref):
    lane = lane_iota((2 * SUB, LANES))
    ty, pat = src_of
    part = in_ref.shape[1] // 3
    per_ty = in_ref.shape[2] // LANES // 2
    for k in range(pat):
        for g in range(0, part, 2 * SUB):
            for i in range(ty):
                for pair in range(per_ty):
                    both = [own_coded(in_ref, i * pat + k, g, part, q) for q in (2 * pair, 2 * pair + 1)]
                    sides = []
                    for p in range(2):
                        sides.append(edge_messages([(v[p], o) for v in both for o in (0, TILE)], lane))
                    vreg = i * per_ty + pair
                    for side, ref in enumerate((left_ref, right_ref)):
                        for r, v in zip(coded_rows(k, g, part, pat), encode(sides[0][side], sides[1][side])):
                            ref[r, vreg * LANES : (vreg + 1) * LANES] = v


def unpack_data(src_of, in_ref, from_left_ref, from_right_ref, out_ref):
    lane = lane_iota((2 * SUB, LANES))
    ty, pat = src_of
    part = in_ref.shape[1] // 3
    per_ty = in_ref.shape[2] // LANES // 2
    for k in range(pat):
        for g in range(0, part, 2 * SUB):
            rows = coded_rows(k, g, part, pat)
            for i in range(ty):
                for pair in range(per_ty):
                    vreg = i * per_ty + pair
                    at = slice(vreg * LANES, (vreg + 1) * LANES)
                    from_left = decode(*(from_left_ref[r, at] for r in rows))
                    from_right = decode(*(from_right_ref[r, at] for r in rows))
                    both = [own_coded(in_ref, i * pat + k, g, part, q) for q in (2 * pair, 2 * pair + 1)]
                    for p in range(2):
                        own = [x for v in both for x in (v[p], roll(v[p], -TILE))]
                        for u in range(4):
                            m = 4 * vreg + u
                            out_ref[m // 2, rows[p], (m % 2) * LANES : (m % 2 + 1) * LANES] = from_fixed(
                                with_halo(own[u], u, from_right[p], from_left[p], lane)
                            )


def unpack_wide(src_of, in_ref, from_left_ref, from_right_ref, out_ref):
    lane = lane_iota((SUB, LANES))
    ty, pat = src_of
    groups = in_ref.shape[1] // SUB
    per_ty = in_ref.shape[2] // LANES // 2
    for k in range(pat):
        for g in range(groups):
            row = slice((k * groups + g) * SUB, (k * groups + g + 1) * SUB)
            for i in range(ty):
                for pair in range(per_ty):
                    vreg = i * per_ty + pair
                    from_left = from_left_ref[row, vreg * LANES : (vreg + 1) * LANES]
                    from_right = from_right_ref[row, vreg * LANES : (vreg + 1) * LANES]
                    own = []
                    for q in (2 * pair, 2 * pair + 1):
                        v = in_ref[i * pat + k, g * SUB : (g + 1) * SUB, q * LANES : (q + 1) * LANES]
                        own += [v, roll(v, -TILE)]
                    for u in range(4):
                        m = 4 * vreg + u
                        out_ref[m // 2, row, (m % 2) * LANES : (m % 2 + 1) * LANES] = with_halo(
                            own[u], u, from_right, from_left, lane
                        )


def with_halo(own, u, from_right, from_left, lane):
    inner = lane % GROUP
    value = jnp.where(inner < TILE, own, roll(from_right, HALO * (2 - u)))
    return jnp.where(inner < TILE + HALO, value, roll(from_left, HALO * (3 - u)))


def tables_kernel(tile_of, k_ref, radius_ref, codes_ref, axial_ref, w_ref, fwd_ref, bwd_ref, light_ref):
    lane = lane_iota((GROUP, LANES))
    row = lax.broadcasted_iota(jnp.int32, (GROUP, LANES), 0)
    tap = column_of(row) - column_of(lane) + RADIUS
    first = lane < GROUP
    hit = [tap == j for j in range(TAPS)]
    nothing = jnp.zeros((GROUP, LANES), BF16)

    def scalar(flip, i, j):
        if i < 0 or i >= TAPS:
            return jnp.float32(0.0)
        if flip:
            i, j = TAPS - 1 - i, TAPS - 1 - j
        return jnp.where(abs(j - RADIUS) <= radius_ref[i], k_ref[i, j], 0.0)

    for flip in range(2):
        for i0 in range(-2, TAPS + 3):
            value = jnp.zeros((GROUP, LANES), F32)
            if 0 <= i0 <= TAPS:
                for j in range(TAPS):
                    both = jnp.where(first, scalar(flip, i0, j), scalar(flip, i0 - 1, j))
                    value = jnp.where(hit[j], both, value)
            value = value.astype(BF16)
            for k in range(3):
                for r in range(ROWS_BLOCK):
                    for q in range(ROWS_BLOCK // 2):
                        if ROWS_BLOCK * (k - 1) + r - 2 * q + RADIUS == i0:
                            w_ref[
                                3 * flip + k,
                                r * GROUP : (r + 1) * GROUP,
                                q * LANES : (q + 1) * LANES,
                            ] = value

    planes, rows = axial_ref.shape[0], fwd_ref.shape[0]
    axial = axial_ref[...].astype(BF16)
    pick = lax.broadcasted_iota(jnp.int32, (planes, rows), 1) % planes
    pick = (pick == lax.broadcasted_iota(jnp.int32, (planes, rows), 0)).astype(F32).astype(BF16)
    plain = jnp.dot(axial, pick, preferred_element_type=F32)
    turned = lax.dot_general(axial, pick, (((0,), (0,)), ((), ())), preferred_element_type=F32)
    column = lax.broadcasted_iota(jnp.int32, (planes, rows), 1)
    for p in range(rows // planes):
        here = column // planes == p
        fwd_ref[p * planes : (p + 1) * planes] = jnp.where(here, plain, 0.0).astype(BF16)
    span = 3 * planes
    for h in range(2):
        here = (column >= h * span) & (column < (h + 1) * span)
        bwd_ref[h * planes : (h + 1) * planes] = jnp.where(here, turned, 0.0).astype(BF16)[:, : 2 * span]

    col = column_of(lane_iota((1, BLOCK)))
    within = lane_iota((1, BLOCK)) // GROUP
    x = tile_of() * TILE + col
    cosines = [0.7 * math.cos(TWO_PI * m / 5.0) for m in range(5)]
    patterns = light_ref.shape[1]
    for p in range(patterns):
        angle, phase = codes_ref[0, p], codes_ref[1, p]
        step_col = jnp.where(angle == 0, 2, -1)
        step_row = jnp.where(angle == 0, 0, jnp.where(angle == 1, 2, -2))
        for b in range(light_ref.shape[0]):
            y = within + b * ROWS_BLOCK
            turn = lax.rem(step_col * x + step_row * y + phase + 5 * OFFSET, 5)
            value = jnp.full((1, BLOCK), cosines[0], F32)
            for m in range(1, 5):
                value = jnp.where(turn == m, cosines[m], value)
            light_ref[b, p : p + 1] = value


def lateral(src_ref, w_ref, flip, b, count):
    total = None
    for k in range(3):
        v = src_ref[b + k : b + k + count]
        part = jnp.dot(v.reshape(-1, BLOCK), w_ref[3 * flip + k], preferred_element_type=F32)
        total = part if total is None else total + part
    return total.reshape(count, -1, BLOCK)


def split3(v):
    high = v.astype(BF16)
    rest = v - high.astype(F32)
    mid = rest.astype(BF16)
    return high, mid, (rest - mid.astype(F32)).astype(BF16)


class Step:
    def __init__(self, nx, tile_of, w_ref, ax_fwd, ax_bwd, light_ref, wave_ref):
        self.w, self.ax_fwd, self.ax_bwd, self.light, self.wave = w_ref, ax_fwd, ax_bwd, light_ref, wave_ref
        self.blocks, self.patterns = light_ref.shape[0], light_ref.shape[1]
        self.planes = wave_ref.shape[0]
        self.col = column_of(lane_iota((1, BLOCK)))
        place = tile_of() * TILE + self.col
        self.inside = (place >= 0) & (place < nx)

    def reach(self, width):
        return self.inside & (self.col >= -width) & (self.col < TILE + width)

    def clear_ends(self, ref):
        ref[0] = jnp.zeros(ref.shape[1:], BF16)
        ref[self.blocks + 1] = jnp.zeros(ref.shape[1:], BF16)

    def normalizer(self, norm_ref):
        depth = self.ax_bwd.shape[1]
        ones = lax.broadcasted_iota(jnp.int32, (depth, BLOCK), 0) < self.planes
        ones = jnp.where(ones, 1.0, 0.0).astype(BF16)
        colsum = jnp.dot(self.ax_bwd[...], ones, preferred_element_type=F32)[: self.planes]
        ones = jnp.broadcast_to(jnp.where(self.inside, 1.0, 0.0), (2 * SUB, BLOCK)).astype(BF16)
        parts = [jnp.dot(ones, self.w[3 + k], preferred_element_type=F32) for k in range(3)]
        for b in range(self.blocks):
            total = sum(parts[k] for k in range(3) if 0 <= b + k - 1 < self.blocks)
            cover = total.astype(BF16).astype(F32)[0:1]
            lat_sum = jnp.sum(self.light[b], axis=0, keepdims=True)
            norm_ref[b] = colsum * cover * (float(self.patterns) + lat_sum * self.wave[...])

    def blur(self, obj_ref, stage_ref):
        for b in range(self.blocks):
            lighting = 1.0 + self.light[b][:, None, :] * self.wave[...][None]
            lit = (lighting * obj_ref[b][None]).astype(BF16).reshape(-1, BLOCK)
            stage_ref[b + 1] = jnp.dot(self.ax_fwd[...], lit, preferred_element_type=F32).astype(BF16)

    def compare(self, stage_ref, data_ref, quot_ref, width, predicted_ref=None):
        ok = self.reach(width)[None]
        acc = jnp.zeros((SUB, BLOCK), F32)
        for b in range(0, self.blocks, CHUNK):
            if predicted_ref is None:
                predicted = lateral(stage_ref, self.w, 0, b, CHUNK)
            else:
                predicted = predicted_ref[b : b + CHUNK]
            data = data_ref[b : b + CHUNK]
            miss = data - predicted
            acc = acc + jnp.sum((miss * miss).reshape(-1, SUB, BLOCK), axis=0)
            quot_ref[b + 1 : b + 1 + CHUNK] = jnp.where(ok, data / predicted, 0.0).astype(BF16)
        row = jnp.sum(jnp.where((self.col >= 0) & (self.col < TILE), acc, 0.0), axis=0, keepdims=True)
        return sum(row[:, h * LANES : (h + 1) * LANES] for h in range(BLOCK // LANES))

    def update(self, quot_ref, obj_ref, norm_ref, width):
        ok = self.reach(width)
        for b0 in range(0, self.blocks, CHUNK):
            back = lateral(quot_ref, self.w, 1, b0, CHUNK).astype(BF16)
            for b in range(b0, b0 + CHUNK):
                part = back[b - b0].astype(F32).reshape(self.patterns, self.planes, BLOCK)
                plain = jnp.sum(part, axis=0)
                waved = jnp.sum(self.light[b][:, None, :] * part, axis=0)
                stack = jnp.concatenate(split3(plain) + split3(waved), axis=0)
                both = jnp.dot(self.ax_bwd[...], stack, preferred_element_type=F32)
                summed = both[: self.planes] + self.wave[...] * both[self.planes :]
                obj_ref[b] = jnp.where(ok, obj_ref[b] * summed / norm_ref[b], 0.0)


def put_halo(own_ref, from_left_ref, from_right_ref, out_ref):
    lane = lane_iota((SUB, LANES))
    for z in range(0, out_ref.shape[1], SUB):
        for vreg in range(out_ref.shape[0] // 2):
            from_left = from_left_ref[z : z + SUB, vreg * LANES : (vreg + 1) * LANES]
            from_right = from_right_ref[z : z + SUB, vreg * LANES : (vreg + 1) * LANES]
            for u in range(4):
                m = 4 * vreg + u
                at = (m // 2, slice(z, z + SUB), slice((m % 2) * LANES, (m % 2 + 1) * LANES))
                out_ref[at] = with_halo(own_ref[at], u, from_right, from_left, lane)


def forward_kernel(nx, tile_of, src_of, w_ref, ax_fwd, ax_bwd, light_ref, wave_ref,
                   est_ref, from_left_ref, from_right_ref, obj_ref, norm_ref, predicted_ref, stage_ref):
    unpack_wide(src_of, est_ref, from_left_ref, from_right_ref, obj_ref)
    step = Step(nx, tile_of, w_ref, ax_fwd, ax_bwd, light_ref, wave_ref)
    step.normalizer(norm_ref)
    step.clear_ends(stage_ref)
    step.blur(obj_ref, stage_ref)
    for b in range(0, step.blocks, CHUNK):
        predicted_ref[b : b + CHUNK] = lateral(stage_ref, w_ref, 0, b, CHUNK)


def first_kernel(nx, tile_of, src_of, w_ref, ax_fwd, ax_bwd, light_ref, wave_ref, norm_ref, obj_in_ref,
                 predicted_ref, in_ref, from_left_ref, from_right_ref, data_ref, obj_ref, left_ref, right_ref,
                 sq_ref, stage_ref, quot_ref):
    unpack_data(src_of, in_ref, from_left_ref, from_right_ref, data_ref)
    step = Step(nx, tile_of, w_ref, ax_fwd, ax_bwd, light_ref, wave_ref)
    step.clear_ends(stage_ref)
    step.clear_ends(quot_ref)
    obj_ref[...] = obj_in_ref[...]
    sq_ref[...] = jnp.zeros(sq_ref.shape, F32)
    sq_ref[0:1] = step.compare(None, data_ref, quot_ref, 12, predicted_ref)
    step.update(quot_ref, obj_ref, norm_ref, 8)
    step.blur(obj_ref, stage_ref)
    sq_ref[1:2] = step.compare(stage_ref, data_ref, quot_ref, 4)
    step.update(quot_ref, obj_ref, norm_ref, 0)

    lane = lane_iota((SUB, LANES))
    for z in range(0, step.planes, SUB):
        for vreg in range(step.blocks // 2):
            pieces = []
            for u in range(4):
                m = 4 * vreg + u
                pieces.append((obj_ref[m // 2, z : z + SUB, (m % 2) * LANES : (m % 2 + 1) * LANES], 0))
            left, right = edge_messages(pieces, lane)
            left_ref[z : z + SUB, vreg * LANES : (vreg + 1) * LANES] = left
            right_ref[z : z + SUB, vreg * LANES : (vreg + 1) * LANES] = right


def second_kernel(nx, tile_of, src_of, w_ref, ax_fwd, ax_bwd, light_ref, wave_ref, norm_ref, data_ref,
                  obj_in_ref, from_left_ref, from_right_ref, sq_in_ref, out_ref, obj_ref, stage_ref, quot_ref):
    put_halo(obj_in_ref, from_left_ref, from_right_ref, obj_ref)
    step = Step(nx, tile_of, w_ref, ax_fwd, ax_bwd, light_ref, wave_ref)
    step.clear_ends(stage_ref)
    step.clear_ends(quot_ref)
    squares = [sq_in_ref[0:1], sq_in_ref[1:2]]
    for quot_width, obj_width in ((12, 8), (4, 0)):
        step.blur(obj_ref, stage_ref)
        squares.append(step.compare(stage_ref, data_ref, quot_ref, quot_width))
        step.update(quot_ref, obj_ref, norm_ref, obj_width)

    ty, pat = src_of
    quads = step.blocks // ty
    lane = lane_iota((SUB, LANES))
    own = (lane // TILE) % 2 == 0
    last = jnp.concatenate(squares + [jnp.zeros((SUB - len(squares), LANES), F32)], axis=0)
    for i in range(ty):
        for k in range(pat):
            out_ref[i * pat + k, quads * step.planes : quads * step.planes + SUB] = last
        for q in range(quads):
            for z in range(0, step.planes, SUB):
                v0 = obj_ref[i * quads + q, z : z + SUB, 0:LANES]
                v1 = obj_ref[i * quads + q, z : z + SUB, LANES : 2 * LANES]
                v = jnp.where(own, v0, roll(v1, TILE))
                for k in range(pat):
                    out_ref[i * pat + k, q * step.planes + z : q * step.planes + z + SUB] = v


def final_kernel(dest_of_tile, rows, in_ref, out_ref):
    lane = lane_iota((SUB, LANES))
    planes = out_ref.shape[0] // rows
    tiles_half = LANES // TILE
    quads = rows // 4
    for half in range(len(dest_of_tile) // tiles_half):

        @pl.when(pl.program_id(0) == half)
        def _(half=half):
            for z in range(0, planes, SUB):
                for quad in range(quads):
                    row = quad * planes + z
                    v = [in_ref[dest_of(dest_of_tile, half * tiles_half + t), row : row + SUB] for t in range(tiles_half)]
                    for g, piece in enumerate(quad_transpose(v, lane)):
                        out_ref[pl.ds(z * rows + 4 * quad + QUAD_ROWS[g], SUB, stride=rows), :] = piece


def masked_kernel(lateral_kernel, psf_radius):
    offsets = jnp.arange(TAPS) - RADIUS
    within = jnp.abs(offsets)[None, :] <= psf_radius[:, None]
    return jnp.where(within, lateral_kernel, jnp.zeros_like(lateral_kernel)).astype(BF16)


def shape(dims, dtype=F32):
    return jax.ShapeDtypeStruct(dims, dtype)


PARAMS = pltpu.CompilerParams(vmem_limit_bytes=24 * 2**20)
VMEM = pl.BlockSpec(memory_space=pltpu.VMEM)
SMEM = pl.BlockSpec(memory_space=pltpu.SMEM)


def over_tx(value, size):
    if size & (size - 1):
        return lax.psum(value, "tx")
    step = 1
    while step < size:
        value = value + lax.ppermute(value, "tx", [(i, i ^ step) for i in range(size)])
        step *= 2
    return value


def tiled_device(sizes, estimate, data, axial, lateral_kernel, psf_radius, pattern_codes):
    ty, tx, pat = sizes["ty"], sizes["tx"], sizes["pat"]
    planes, rows, cols = estimate.shape
    pat_local = data.shape[0]
    patterns = pat_local * pat
    ny, nx = rows * ty, cols * tx
    members = ty * pat
    blocks = ny // ROWS_BLOCK
    axes = ("ty", "tx", "pat")

    owner = [(i, k if i % 2 == 0 else pat - 1 - k) for i in range(ty) for k in range(pat)]
    dest_of_tile = [i * pat + k for i, k in owner]
    order = [(i * tx + j) * pat + k for j in range(tx) for i, k in (owner if j % 2 == 0 else owner[::-1])]
    to_right = [(a, b) for a, b in zip(order[:-1], order[1:])]
    to_left = [(b, a) for a, b in to_right]
    src_of = (ty, pat)

    ti = lax.axis_index("ty")

    def tile_of():
        i, j, k = (lax.axis_index(a) for a in axes)
        c = i * pat + jnp.where(lax.rem(i, 2) == 0, k, pat - 1 - k)
        return j * members + jnp.where(lax.rem(j, 2) == 0, c, members - 1 - c)

    halves = cols // LANES
    piece_lanes = rows * TILE
    halo_lanes = ny * HALO

    def whole(dims):
        return pl.BlockSpec(dims, lambda h: (0,) * len(dims))

    def half_columns(height):
        return pl.BlockSpec((height, LANES), lambda h: (0, h))

    def edges(pieces, body, name):
        out = shape((pieces.shape[1] * pieces.shape[0] // ty, halo_lanes), pieces.dtype)
        return pl.pallas_call(
            functools.partial(body, (ty, pieces.shape[0] // ty)),
            out_shape=(out, out),
            in_specs=[VMEM],
            out_specs=(VMEM,) * 2,
            compiler_params=PARAMS,
            name=name,
        )(pieces)

    def swap_edges(left, right):
        return lax.ppermute(right, axes, to_right), lax.ppermute(left, axes, to_left)

    message = pl.pallas_call(
        functools.partial(pack_kernel, dest_of_tile, rows),
        out_shape=shape((members, 3 * planes, piece_lanes), jnp.int16),
        grid=(halves,),
        in_specs=[half_columns(data.size // cols)],
        out_specs=whole((members, 3 * planes, piece_lanes)),
        compiler_params=PARAMS,
        name="pack",
    )(data.reshape(-1, cols))
    message, estimate = lax.optimization_barrier((message, estimate))
    mine = lax.all_to_all(message, ("ty", "pat"), 0, 0, tiled=True)

    pieces = pl.pallas_call(
        functools.partial(estimate_kernel, dest_of_tile, rows, pat),
        out_shape=shape((ty, planes, piece_lanes)),
        grid=(halves,),
        in_specs=[half_columns(planes * rows)],
        out_specs=whole((ty, planes, piece_lanes)),
        scratch_shapes=[pltpu.VMEM((members, planes, piece_lanes), F32)],
        compiler_params=PARAMS,
        name="prep_estimate",
    )(estimate.reshape(-1, cols))
    tile_rows = [lax.dynamic_index_in_dim(pieces, ti, 0, keepdims=False)]
    for shift in range(1, ty):
        sent = lax.dynamic_index_in_dim(pieces, (ti + shift) % ty, 0, keepdims=False)
        tile_rows.append(lax.ppermute(sent, "ty", [(i, (i + shift) % ty) for i in range(ty)]))
    tile_rows = jnp.stack(tile_rows)
    tile_rows = jnp.stack(
        [lax.dynamic_index_in_dim(tile_rows, (ti - i) % ty, 0, keepdims=False) for i in range(ty)]
    )
    est_left, est_right = swap_edges(*edges(tile_rows, edges_kernel, "prep_edges"))

    weights, ax_fwd, ax_bwd, light = pl.pallas_call(
        functools.partial(tables_kernel, tile_of),
        out_shape=(
            shape((6, BLOCK, BLOCK), BF16),
            shape((patterns * planes, patterns * planes), BF16),
            shape((2 * planes, 6 * planes), BF16),
            shape((blocks, patterns, BLOCK)),
        ),
        in_specs=[SMEM] * 3 + [VMEM],
        out_specs=(VMEM,) * 4,
        compiler_params=PARAMS,
        name="tables",
    )(lateral_kernel, psf_radius, pattern_codes, axial)
    wave = np.cos(np.arange(planes, dtype=np.float32) * np.float32(TWO_PI * 3.0 / planes))
    wave = jnp.asarray(np.ascontiguousarray(np.broadcast_to(wave[:, None], (planes, BLOCK))))

    object_shape = shape((blocks, planes, BLOCK))
    field_shape = shape((blocks, patterns * planes, BLOCK))
    object_scratch = pltpu.VMEM(object_shape.shape, F32)
    stage = pltpu.VMEM((blocks + 2, patterns * planes, BLOCK), BF16)
    table_specs = [VMEM] * 5
    mine, est_left, est_right, weights = lax.optimization_barrier((mine, est_left, est_right, weights))
    from_left, from_right = swap_edges(*edges(mine, data_edges_kernel, "edges"))
    tables = (weights, ax_fwd, ax_bwd, light, wave)
    current, norm, predicted = pl.pallas_call(
        functools.partial(forward_kernel, nx, tile_of, (ty, 1)),
        out_shape=(object_shape, object_shape, field_shape),
        in_specs=table_specs + [VMEM] * 3,
        out_specs=(VMEM,) * 3,
        scratch_shapes=[stage],
        compiler_params=PARAMS,
        name="forward",
    )(*tables, tile_rows, est_left, est_right)

    edge_shape = shape((planes, halo_lanes))
    data_all, current, left, right, sq_first = pl.pallas_call(
        functools.partial(first_kernel, nx, tile_of, src_of),
        out_shape=(field_shape, object_shape, edge_shape, edge_shape, shape((SUB, LANES))),
        in_specs=table_specs + [VMEM] * 6,
        out_specs=(VMEM,) * 5,
        scratch_shapes=[stage, stage],
        compiler_params=PARAMS,
        name="first",
    )(*tables, norm, current, predicted, mine, from_left, from_right)
    from_left, from_right = swap_edges(left, right)
    outgoing = pl.pallas_call(
        functools.partial(second_kernel, nx, tile_of, src_of),
        out_shape=shape((members, rows // 4 * planes + SUB, LANES)),
        in_specs=table_specs + [VMEM] * 6,
        out_specs=VMEM,
        scratch_shapes=[object_scratch, stage, stage],
        compiler_params=PARAMS,
        name="second",
    )(*tables, norm, data_all, current, from_left, from_right, sq_first)

    incoming = lax.all_to_all(outgoing, ("ty", "pat"), 0, 0, tiled=True)
    squares = jnp.sum(incoming[:, rows // 4 * planes : rows // 4 * planes + ITERS], axis=(0, 2))
    squares = over_tx(squares, tx)
    result = pl.pallas_call(
        functools.partial(final_kernel, dest_of_tile, rows),
        out_shape=shape((planes * rows, cols)),
        grid=(halves,),
        in_specs=[whole(incoming.shape)],
        out_specs=half_columns(planes * rows),
        compiler_params=PARAMS,
        name="unpack",
    )(incoming)
    cell_count = float(patterns * planes * ny * nx)
    return result.reshape(estimate.shape), jnp.sqrt(squares / cell_count)


def extended(block, sides, width):
    for axis, dim in sides:
        count = lax.axis_size(axis)
        forward = [(i, i + 1) for i in range(count - 1)]
        backward = [(target, source) for source, target in forward]
        low = lax.ppermute(
            lax.slice_in_dim(block, block.shape[dim] - width, None, axis=dim), axis, forward
        )
        high = lax.ppermute(lax.slice_in_dim(block, 0, width, axis=dim), axis, backward)
        block = jnp.concatenate([low, block, high], axis=dim)
    return block


def wave_table(angle_code, phase_code, row_coord, col_coord, planes):
    step_col = jnp.where(angle_code == 0, 2, -1).astype(jnp.int32)
    step_row = jnp.where(angle_code == 0, 0, jnp.where(angle_code == 1, 2, -2)).astype(jnp.int32)
    argument = (
        step_col[:, None, None] * col_coord[None, None, :]
        + step_row[:, None, None] * row_coord[None, :, None]
        + phase_code[:, None, None]
    ) % 5
    lateral_wave = jnp.cos(argument.astype(jnp.float32) * (TWO_PI / 5.0))
    plane_index = jnp.arange(planes).astype(jnp.float32)
    axial_wave = jnp.cos(plane_index * (TWO_PI * 3.0 / planes))
    return 1.0 + 0.7 * lateral_wave[:, None, :, :] * axial_wave[None, :, None, None]


def tap_matrices(kernel, width_in, width_out):
    tap_count = 2 * RADIUS + 1
    offset = jnp.arange(width_in)[:, None] - jnp.arange(width_out)[None, :]
    onehot = (offset[None, :, :] == jnp.arange(tap_count)[:, None, None]).astype(jnp.float32)
    return jnp.einsum(
        "ij,jab->iab", kernel.astype(jnp.float32), onehot, precision=lax.Precision.HIGHEST
    ).astype(jnp.bfloat16)


def lateral_pass(padded, matrices, height):
    summed = None
    for tap_row in range(2 * RADIUS + 1):
        window = padded[..., tap_row : tap_row + height, :]
        product = jnp.dot(window, matrices[tap_row], preferred_element_type=jnp.float32)
        summed = product if summed is None else summed + product
    return summed


def general_device(estimate, data, axial, lateral_kernel, psf_radius, pattern_codes):
    planes, height, width = estimate.shape
    pat_local = data.shape[0]
    full_rows = height * lax.axis_size("ty")
    full_cols = width * lax.axis_size("tx")
    depth = 2 * RADIUS
    margin = depth - RADIUS
    row_coord = lax.axis_index("ty") * height - depth + jnp.arange(height + 2 * depth)
    col_coord = lax.axis_index("tx") * width - depth + jnp.arange(width + 2 * depth)
    codes_here = lax.dynamic_slice_in_dim(
        pattern_codes, lax.axis_index("pat") * pat_local, pat_local, 1
    )
    lighting = wave_table(codes_here[0], codes_here[1], row_coord, col_coord, planes)
    lighting_inner = lighting[:, :, depth : depth + height, depth : depth + width]
    kernel = masked_kernel(lateral_kernel, psf_radius)
    forward_taps = tap_matrices(kernel, width + 2 * depth, width + 2 * margin)
    adjoint_taps = tap_matrices(kernel[::-1, ::-1], width + 2 * RADIUS, width)
    axial_b = axial.astype(jnp.bfloat16)
    row_inside = (row_coord >= 0) & (row_coord < full_rows)
    col_inside = (col_coord >= 0) & (col_coord < full_cols)
    inside_all = row_inside[:, None] & col_inside[None, :]
    inside = inside_all[
        margin : margin + height + 2 * RADIUS, margin : margin + width + 2 * RADIUS
    ].astype(jnp.bfloat16)
    inside_mid = inside_all[
        RADIUS : RADIUS + height + 2 * margin, RADIUS : RADIUS + width + 2 * margin
    ]
    coverage = lateral_pass(inside[None], adjoint_taps, height).astype(jnp.bfloat16)
    spread = jnp.einsum(
        "ba,byx->ayx",
        axial_b,
        jnp.broadcast_to(coverage, (planes, height, width)),
        preferred_element_type=jnp.float32,
    )
    normalizer = lax.psum(jnp.sum(lighting_inner * spread[None], axis=0), "pat")
    cell_count = float(pat_local * lax.axis_size("pat") * planes * full_rows * full_cols)
    data_wide = extended(data, (("ty", 2), ("tx", 3)), RADIUS)
    current = estimate
    squares_list = []
    for iteration in range(ITERS):
        padded = extended(current, (("ty", 1), ("tx", 2)), depth)
        lighted = (lighting * padded[None]).astype(jnp.bfloat16)
        blurred = jnp.einsum(
            "ab,pbyx->payx", axial_b, lighted, preferred_element_type=jnp.float32
        ).astype(jnp.bfloat16)
        predicted = lateral_pass(blurred, forward_taps, height + 2 * margin)
        predicted_inner = predicted[:, :, margin : margin + height, margin : margin + width]
        misfit = data - predicted_inner
        local_square = jnp.sum(misfit * misfit)
        safe = jnp.where(inside_mid[None, None], predicted, 1.0)
        quotient_padded = jnp.where(inside_mid[None, None], data_wide / safe, 0.0).astype(
            jnp.bfloat16
        )
        backward = lateral_pass(quotient_padded, adjoint_taps, height).astype(jnp.bfloat16)
        gathered = jnp.einsum(
            "ba,pbyx->payx", axial_b, backward, preferred_element_type=jnp.float32
        )
        contribution = jnp.sum(lighting_inner * gathered, axis=0)
        summed = lax.psum(contribution, "pat")
        current = current * summed / normalizer
        squares_list.append(lax.psum(local_square, ("ty", "tx", "pat")))
    squares = jnp.stack(squares_list)
    return (current, jnp.sqrt(squares / cell_count))


def solution(mesh):
    sizes = dict(mesh.shape)
    in_specs = (P(None, "ty", "tx"), P("pat", None, "ty", "tx"), P(), P(), P(), P())
    out_specs = (P(None, "ty", "tx"), P())

    def per_device(estimate, data, *rest):
        planes, rows, cols = estimate.shape
        members = sizes["ty"] * sizes["pat"]
        fits = (
            cols == members * TILE
            and cols % LANES == 0
            and rows % 8 == 0
            and rows * sizes["ty"] <= 2 * TILE
            and planes % (2 * SUB) == 0
            and data.shape[0] == 2
        )
        if fits:
            return tiled_device(sizes, estimate, data, *rest)
        return general_device(estimate, data, *rest)

    return jax.shard_map(
        per_device, mesh=mesh, in_specs=in_specs, out_specs=out_specs, check_vma=False
    )
```

```python
import functools
import math

import jax
import jax.numpy as jnp
import numpy as np
from jax import lax
from jax.experimental import pallas as pl
from jax.experimental.pallas import tpu as pltpu
from jax.sharding import PartitionSpec as P

RADIUS = 4
TAPS = 2 * RADIUS + 1
ITERS = 4
TWO_PI = 2.0 * math.pi

TILE = 32
HALO = 16
GROUP = TILE + 2 * HALO
ROWS_BLOCK = RADIUS
BLOCK = ROWS_BLOCK * GROUP
LANES = 128
SUB = 8
QUAD_ROWS = (0, 2, 1, 3)
CHUNK = 4
OFFSET = 1 << 20
F32 = jnp.float32
BF16 = jnp.bfloat16


def lane_iota(shape):
    return lax.broadcasted_iota(jnp.int32, shape, len(shape) - 1)


def column_of(lane):
    inner = lane % GROUP
    return jnp.where(inner < TILE + HALO, inner, inner - GROUP)


def roll(x, shift):
    shift = shift % LANES
    return x if shift == 0 else pltpu.roll(x, shift, 1)


def quad_transpose(v, lane):
    group = lane // TILE
    out = []
    for t in range(4):
        value = roll(v[0], -TILE * t)
        for g in range(1, 4):
            value = jnp.where(group == g, roll(v[g], TILE * (g - t)), value)
        out.append(value)
    return out


def dest_of(dest_of_tile, c):
    return jnp.where(lax.rem(lax.axis_index("tx"), 2) == 0, dest_of_tile[c], dest_of_tile[-1 - c])


def pack_half(dest_of_tile, rows, half, groups, src_ref, out_ref):
    lane = lane_iota((SUB, LANES))
    tiles_half = LANES // TILE
    for i in range(groups):
        for quad in range(rows // 4):
            v = [src_ref[pl.ds(i * rows * SUB + 4 * quad + r, SUB, stride=rows), :] for r in QUAD_ROWS]
            for t, piece in enumerate(quad_transpose(v, lane)):
                dest = dest_of(dest_of_tile, half * tiles_half + t)
                out_ref[dest, i * SUB : (i + 1) * SUB, quad * LANES : (quad + 1) * LANES] = piece


DATA_LOW, DATA_HIGH, TOP = 0.1, 6.0, 2**24 - 1
DATA_SCALE = TOP / (DATA_HIGH - DATA_LOW)
BIAS = 2**15


def to_fixed(v):
    return jnp.clip((v - DATA_LOW) * DATA_SCALE + 0.5, 0.0, float(TOP)).astype(jnp.int32)


def from_fixed(t):
    return t.astype(F32) * (1.0 / DATA_SCALE) + DATA_LOW


def encode(first, second):
    low = ((first & 255) << 8) + (second & 255)
    return tuple((v - BIAS).astype(jnp.int16) for v in (first >> 8, second >> 8, low))


def decode(first, second, low):
    first, second, low = (v.astype(jnp.int32) + BIAS for v in (first, second, low))
    return (first << 8) + (low >> 8), (second << 8) + (low & 255)


LOG_SCALE, LOG_BIAS, LN2 = 2.0**16, 128.0, math.log(2.0)


def to_log(v):
    t = (jnp.log(jnp.maximum(v, 2.0**-126)) * (1.0 / LN2) + LOG_BIAS) * LOG_SCALE + 0.5
    return jnp.where(v > 0, jnp.clip(t, 1.0, float(TOP)), 0.0).astype(jnp.int32)


def from_log(t):
    return jnp.where(t > 0, jnp.exp2(t.astype(F32) * (1.0 / LOG_SCALE) - LOG_BIAS), 0.0)


def pack_kernel(dest_of_tile, rows, data_ref, out_ref):
    lane = lane_iota((SUB, LANES))
    tiles_half = LANES // TILE
    part = out_ref.shape[1] // 3
    per_pattern = part // SUB

    def pieces(group, quad):
        start = group * rows * SUB + 4 * quad
        v = [to_fixed(data_ref[pl.ds(start + r, SUB, stride=rows), :]) for r in QUAD_ROWS]
        return quad_transpose(v, lane)

    for half in range(len(dest_of_tile) // tiles_half):

        @pl.when(pl.program_id(0) == half)
        def _(half=half):
            for g in range(0, per_pattern, 2):
                for quad in range(rows // 4):
                    a0, a1 = pieces(g, quad), pieces(g + 1, quad)
                    b0, b1 = pieces(per_pattern + g, quad), pieces(per_pattern + g + 1, quad)
                    for t in range(tiles_half):
                        dest = dest_of(dest_of_tile, half * tiles_half + t)
                        coded = encode(jnp.concatenate([a0[t], a1[t]]), jnp.concatenate([b0[t], b1[t]]))
                        for n, v in enumerate(coded):
                            row = n * part + g * SUB
                            out_ref[dest, row : row + 2 * SUB, quad * LANES : (quad + 1) * LANES] = v


def estimate_kernel(dest_of_tile, rows, pat, est_ref, out_ref, all_ref):
    halves = len(dest_of_tile) * TILE // LANES
    for half in range(halves):

        @pl.when(pl.program_id(0) == half)
        def _(half=half):
            pack_half(dest_of_tile, rows, half, est_ref.shape[0] // (rows * SUB), est_ref, all_ref)
            if half == halves - 1:
                for i in range(out_ref.shape[0]):
                    out_ref[i] = all_ref[i * pat + lax.axis_index("pat")]


def edge_messages(pieces, lane):
    left = right = None
    for u, (v, offset) in enumerate(pieces):
        slot = (lane // HALO) % 4 == u
        l_u, r_u = roll(v, HALO * u - offset), roll(v, HALO * (u - 1) - offset)
        left = l_u if left is None else jnp.where(slot, l_u, left)
        right = r_u if right is None else jnp.where(slot, r_u, right)
    return left, right


def edges_kernel(src_of, in_ref, left_ref, right_ref):
    lane = lane_iota((SUB, LANES))
    ty, pat = src_of
    groups = in_ref.shape[1] // SUB
    per_ty = in_ref.shape[2] // LANES // 2
    for k in range(pat):
        for g in range(groups):
            row = slice((k * groups + g) * SUB, (k * groups + g + 1) * SUB)
            for i in range(ty):
                for pair in range(per_ty):
                    pieces = []
                    for q in (2 * pair, 2 * pair + 1):
                        v = in_ref[i * pat + k, g * SUB : (g + 1) * SUB, q * LANES : (q + 1) * LANES]
                        pieces += [(v, 0), (v, TILE)]
                    left, right = edge_messages(pieces, lane)
                    vreg = i * per_ty + pair
                    left_ref[row, vreg * LANES : (vreg + 1) * LANES] = left
                    right_ref[row, vreg * LANES : (vreg + 1) * LANES] = right


def coded_rows(k, g, part, pat):
    first = 2 * k * part + g
    return [slice(r, r + 2 * SUB) for r in (first, first + part, 2 * pat * part + k * part + g)]


def own_coded(in_ref, source, g, part, q):
    rows = [slice(n * part + g, n * part + g + 2 * SUB) for n in range(3)]
    return decode(*(in_ref[source, r, q * LANES : (q + 1) * LANES] for r in rows))


def data_edges_kernel(src_of, in_ref, left_ref, right_ref):
    lane = lane_iota((2 * SUB, LANES))
    ty, pat = src_of
    part = in_ref.shape[1] // 3
    per_ty = in_ref.shape[2] // LANES // 2
    for k in range(pat):
        for g in range(0, part, 2 * SUB):
            for i in range(ty):
                for pair in range(per_ty):
                    both = [own_coded(in_ref, i * pat + k, g, part, q) for q in (2 * pair, 2 * pair + 1)]
                    sides = []
                    for p in range(2):
                        sides.append(edge_messages([(v[p], o) for v in both for o in (0, TILE)], lane))
                    vreg = i * per_ty + pair
                    for side, ref in enumerate((left_ref, right_ref)):
                        for r, v in zip(coded_rows(k, g, part, pat), encode(sides[0][side], sides[1][side])):
                            ref[r, vreg * LANES : (vreg + 1) * LANES] = v


def unpack_data(src_of, in_ref, from_left_ref, from_right_ref, out_ref):
    lane = lane_iota((2 * SUB, LANES))
    ty, pat = src_of
    part = in_ref.shape[1] // 3
    per_ty = in_ref.shape[2] // LANES // 2
    for k in range(pat):
        for g in range(0, part, 2 * SUB):
            rows = coded_rows(k, g, part, pat)
            for i in range(ty):
                for pair in range(per_ty):
                    vreg = i * per_ty + pair
                    at = slice(vreg * LANES, (vreg + 1) * LANES)
                    from_left = decode(*(from_left_ref[r, at] for r in rows))
                    from_right = decode(*(from_right_ref[r, at] for r in rows))
                    both = [own_coded(in_ref, i * pat + k, g, part, q) for q in (2 * pair, 2 * pair + 1)]
                    for p in range(2):
                        own = [x for v in both for x in (v[p], roll(v[p], -TILE))]
                        for u in range(4):
                            m = 4 * vreg + u
                            out_ref[m // 2, rows[p], (m % 2) * LANES : (m % 2 + 1) * LANES] = from_fixed(
                                with_halo(own[u], u, from_right[p], from_left[p], lane)
                            )


def unpack_wide(src_of, in_ref, from_left_ref, from_right_ref, out_ref):
    lane = lane_iota((SUB, LANES))
    ty, pat = src_of
    groups = in_ref.shape[1] // SUB
    per_ty = in_ref.shape[2] // LANES // 2
    for k in range(pat):
        for g in range(groups):
            row = slice((k * groups + g) * SUB, (k * groups + g + 1) * SUB)
            for i in range(ty):
                for pair in range(per_ty):
                    vreg = i * per_ty + pair
                    from_left = from_left_ref[row, vreg * LANES : (vreg + 1) * LANES]
                    from_right = from_right_ref[row, vreg * LANES : (vreg + 1) * LANES]
                    own = []
                    for q in (2 * pair, 2 * pair + 1):
                        v = in_ref[i * pat + k, g * SUB : (g + 1) * SUB, q * LANES : (q + 1) * LANES]
                        own += [v, roll(v, -TILE)]
                    for u in range(4):
                        m = 4 * vreg + u
                        out_ref[m // 2, row, (m % 2) * LANES : (m % 2 + 1) * LANES] = with_halo(
                            own[u], u, from_right, from_left, lane
                        )


def with_halo(own, u, from_right, from_left, lane):
    inner = lane % GROUP
    value = jnp.where(inner < TILE, own, roll(from_right, HALO * (2 - u)))
    return jnp.where(inner < TILE + HALO, value, roll(from_left, HALO * (3 - u)))


def tables_kernel(tile_of, k_ref, radius_ref, codes_ref, axial_ref, w_ref, fwd_ref, bwd_ref, light_ref):
    lane = lane_iota((GROUP, LANES))
    row = lax.broadcasted_iota(jnp.int32, (GROUP, LANES), 0)
    tap = column_of(row) - column_of(lane) + RADIUS
    first = lane < GROUP
    hit = [tap == j for j in range(TAPS)]
    nothing = jnp.zeros((GROUP, LANES), BF16)

    def scalar(flip, i, j):
        if i < 0 or i >= TAPS:
            return jnp.float32(0.0)
        if flip:
            i, j = TAPS - 1 - i, TAPS - 1 - j
        return jnp.where(abs(j - RADIUS) <= radius_ref[i], k_ref[i, j], 0.0)

    for flip in range(2):
        for i0 in range(-2, TAPS + 3):
            value = jnp.zeros((GROUP, LANES), F32)
            if 0 <= i0 <= TAPS:
                for j in range(TAPS):
                    both = jnp.where(first, scalar(flip, i0, j), scalar(flip, i0 - 1, j))
                    value = jnp.where(hit[j], both, value)
            value = value.astype(BF16)
            for k in range(3):
                for r in range(ROWS_BLOCK):
                    for q in range(ROWS_BLOCK // 2):
                        if ROWS_BLOCK * (k - 1) + r - 2 * q + RADIUS == i0:
                            w_ref[
                                3 * flip + k,
                                r * GROUP : (r + 1) * GROUP,
                                q * LANES : (q + 1) * LANES,
                            ] = value

    planes, rows = axial_ref.shape[0], fwd_ref.shape[0]
    axial = axial_ref[...].astype(BF16)
    pick = lax.broadcasted_iota(jnp.int32, (planes, rows), 1) % planes
    pick = (pick == lax.broadcasted_iota(jnp.int32, (planes, rows), 0)).astype(F32).astype(BF16)
    plain = jnp.dot(axial, pick, preferred_element_type=F32)
    turned = lax.dot_general(axial, pick, (((0,), (0,)), ((), ())), preferred_element_type=F32)
    column = lax.broadcasted_iota(jnp.int32, (planes, rows), 1)
    for p in range(rows // planes):
        here = column // planes == p
        fwd_ref[p * planes : (p + 1) * planes] = jnp.where(here, plain, 0.0).astype(BF16)
    span = 3 * planes
    for h in range(2):
        here = (column >= h * span) & (column < (h + 1) * span)
        bwd_ref[h * planes : (h + 1) * planes] = jnp.where(here, turned, 0.0).astype(BF16)[:, : 2 * span]

    col = column_of(lane_iota((1, BLOCK)))
    within = lane_iota((1, BLOCK)) // GROUP
    x = tile_of() * TILE + col
    cosines = [0.7 * math.cos(TWO_PI * m / 5.0) for m in range(5)]
    patterns = light_ref.shape[1]
    for p in range(patterns):
        angle, phase = codes_ref[0, p], codes_ref[1, p]
        step_col = jnp.where(angle == 0, 2, -1)
        step_row = jnp.where(angle == 0, 0, jnp.where(angle == 1, 2, -2))
        for b in range(light_ref.shape[0]):
            y = within + b * ROWS_BLOCK
            turn = lax.rem(step_col * x + step_row * y + phase + 5 * OFFSET, 5)
            value = jnp.full((1, BLOCK), cosines[0], F32)
            for m in range(1, 5):
                value = jnp.where(turn == m, cosines[m], value)
            light_ref[b, p : p + 1] = value


def lateral(src_ref, w_ref, flip, b, count):
    total = None
    for k in range(3):
        v = src_ref[b + k : b + k + count]
        part = jnp.dot(v.reshape(-1, BLOCK), w_ref[3 * flip + k], preferred_element_type=F32)
        total = part if total is None else total + part
    return total.reshape(count, -1, BLOCK)


def split3(v):
    high = v.astype(BF16)
    rest = v - high.astype(F32)
    mid = rest.astype(BF16)
    return high, mid, (rest - mid.astype(F32)).astype(BF16)


class Step:
    def __init__(self, nx, tile_of, w_ref, ax_fwd, ax_bwd, light_ref, wave_ref):
        self.w, self.ax_fwd, self.ax_bwd, self.light, self.wave = w_ref, ax_fwd, ax_bwd, light_ref, wave_ref
        self.blocks, self.patterns = light_ref.shape[0], light_ref.shape[1]
        self.planes = wave_ref.shape[0]
        self.col = column_of(lane_iota((1, BLOCK)))
        place = tile_of() * TILE + self.col
        self.inside = (place >= 0) & (place < nx)

    def reach(self, width):
        return self.inside & (self.col >= -width) & (self.col < TILE + width)

    def clear_ends(self, ref):
        ref[0] = jnp.zeros(ref.shape[1:], BF16)
        ref[self.blocks + 1] = jnp.zeros(ref.shape[1:], BF16)

    def normalizer(self, norm_ref):
        depth = self.ax_bwd.shape[1]
        ones = lax.broadcasted_iota(jnp.int32, (depth, BLOCK), 0) < self.planes
        ones = jnp.where(ones, 1.0, 0.0).astype(BF16)
        colsum = jnp.dot(self.ax_bwd[...], ones, preferred_element_type=F32)[: self.planes]
        ones = jnp.broadcast_to(jnp.where(self.inside, 1.0, 0.0), (2 * SUB, BLOCK)).astype(BF16)
        parts = [jnp.dot(ones, self.w[3 + k], preferred_element_type=F32) for k in range(3)]
        for b in range(self.blocks):
            total = sum(parts[k] for k in range(3) if 0 <= b + k - 1 < self.blocks)
            cover = total.astype(BF16).astype(F32)[0:1]
            lat_sum = jnp.sum(self.light[b], axis=0, keepdims=True)
            norm_ref[b] = colsum * cover * (float(self.patterns) + lat_sum * self.wave[...])

    def blur(self, obj_ref, stage_ref):
        for b in range(self.blocks):
            lighting = 1.0 + self.light[b][:, None, :] * self.wave[...][None]
            lit = (lighting * obj_ref[b][None]).astype(BF16).reshape(-1, BLOCK)
            stage_ref[b + 1] = jnp.dot(self.ax_fwd[...], lit, preferred_element_type=F32).astype(BF16)

    def compare(self, stage_ref, data_ref, quot_ref, width, predicted_ref=None):
        ok = self.reach(width)[None]
        acc = jnp.zeros((SUB, BLOCK), F32)
        for b in range(0, self.blocks, CHUNK):
            if predicted_ref is None:
                predicted = lateral(stage_ref, self.w, 0, b, CHUNK)
            else:
                predicted = predicted_ref[b : b + CHUNK]
            data = data_ref[b : b + CHUNK]
            miss = data - predicted
            acc = acc + jnp.sum((miss * miss).reshape(-1, SUB, BLOCK), axis=0)
            quot_ref[b + 1 : b + 1 + CHUNK] = jnp.where(ok, data / predicted, 0.0).astype(BF16)
        row = jnp.sum(jnp.where((self.col >= 0) & (self.col < TILE), acc, 0.0), axis=0, keepdims=True)
        return sum(row[:, h * LANES : (h + 1) * LANES] for h in range(BLOCK // LANES))

    def update(self, quot_ref, obj_ref, norm_ref, width):
        ok = self.reach(width)
        for b0 in range(0, self.blocks, CHUNK):
            back = lateral(quot_ref, self.w, 1, b0, CHUNK).astype(BF16)
            for b in range(b0, b0 + CHUNK):
                part = back[b - b0].astype(F32).reshape(self.patterns, self.planes, BLOCK)
                plain = jnp.sum(part, axis=0)
                waved = jnp.sum(self.light[b][:, None, :] * part, axis=0)
                stack = jnp.concatenate(split3(plain) + split3(waved), axis=0)
                both = jnp.dot(self.ax_bwd[...], stack, preferred_element_type=F32)
                summed = both[: self.planes] + self.wave[...] * both[self.planes :]
                obj_ref[b] = jnp.where(ok, obj_ref[b] * summed / norm_ref[b], 0.0)


def put_halo(own_ref, from_left_ref, from_right_ref, out_ref):
    lane = lane_iota((SUB, LANES))
    for z in range(0, out_ref.shape[1], SUB):
        for vreg in range(out_ref.shape[0] // 2):
            from_left = from_left_ref[z : z + SUB, vreg * LANES : (vreg + 1) * LANES]
            from_right = from_right_ref[z : z + SUB, vreg * LANES : (vreg + 1) * LANES]
            for u in range(4):
                m = 4 * vreg + u
                at = (m // 2, slice(z, z + SUB), slice((m % 2) * LANES, (m % 2 + 1) * LANES))
                out_ref[at] = with_halo(own_ref[at], u, from_right, from_left, lane)


def forward_kernel(nx, tile_of, src_of, w_ref, ax_fwd, ax_bwd, light_ref, wave_ref,
                   est_ref, from_left_ref, from_right_ref, obj_ref, norm_ref, predicted_ref, stage_ref):
    unpack_wide(src_of, est_ref, from_left_ref, from_right_ref, obj_ref)
    step = Step(nx, tile_of, w_ref, ax_fwd, ax_bwd, light_ref, wave_ref)
    step.normalizer(norm_ref)
    step.clear_ends(stage_ref)
    step.blur(obj_ref, stage_ref)
    for b in range(0, step.blocks, CHUNK):
        predicted_ref[b : b + CHUNK] = lateral(stage_ref, w_ref, 0, b, CHUNK)


def first_kernel(nx, tile_of, src_of, w_ref, ax_fwd, ax_bwd, light_ref, wave_ref, norm_ref, obj_in_ref,
                 predicted_ref, in_ref, from_left_ref, from_right_ref, data_ref, obj_ref, left_ref, right_ref,
                 sq_ref, stage_ref, quot_ref):
    unpack_data(src_of, in_ref, from_left_ref, from_right_ref, data_ref)
    step = Step(nx, tile_of, w_ref, ax_fwd, ax_bwd, light_ref, wave_ref)
    step.clear_ends(stage_ref)
    step.clear_ends(quot_ref)
    obj_ref[...] = obj_in_ref[...]
    sq_ref[...] = jnp.zeros(sq_ref.shape, F32)
    sq_ref[0:1] = step.compare(None, data_ref, quot_ref, 12, predicted_ref)
    step.update(quot_ref, obj_ref, norm_ref, 8)
    step.blur(obj_ref, stage_ref)
    sq_ref[1:2] = step.compare(stage_ref, data_ref, quot_ref, 4)
    step.update(quot_ref, obj_ref, norm_ref, 0)

    lane = lane_iota((SUB, LANES))
    for z in range(0, step.planes, SUB):
        for vreg in range(step.blocks // 2):
            pieces = []
            for u in range(4):
                m = 4 * vreg + u
                pieces.append((obj_ref[m // 2, z : z + SUB, (m % 2) * LANES : (m % 2 + 1) * LANES], 0))
            left, right = edge_messages(pieces, lane)
            left_ref[z : z + SUB, vreg * LANES : (vreg + 1) * LANES] = left
            right_ref[z : z + SUB, vreg * LANES : (vreg + 1) * LANES] = right


def second_kernel(nx, tile_of, src_of, w_ref, ax_fwd, ax_bwd, light_ref, wave_ref, norm_ref, data_ref,
                  obj_in_ref, from_left_ref, from_right_ref, sq_in_ref, out_ref, obj_ref, stage_ref, quot_ref):
    put_halo(obj_in_ref, from_left_ref, from_right_ref, obj_ref)
    step = Step(nx, tile_of, w_ref, ax_fwd, ax_bwd, light_ref, wave_ref)
    step.clear_ends(stage_ref)
    step.clear_ends(quot_ref)
    squares = [sq_in_ref[0:1], sq_in_ref[1:2]]
    for quot_width, obj_width in ((12, 8), (4, 0)):
        step.blur(obj_ref, stage_ref)
        squares.append(step.compare(stage_ref, data_ref, quot_ref, quot_width))
        step.update(quot_ref, obj_ref, norm_ref, obj_width)

    ty, pat = src_of
    quads = step.blocks // ty
    planes = step.planes
    lane = lane_iota((2 * SUB, LANES))
    own = (lane // TILE) % 2 == 0
    last = to_log(jnp.concatenate(squares + [jnp.zeros((SUB - len(squares), LANES), F32)], axis=0))
    last = (jnp.concatenate([last >> 8, last & 255]) - BIAS).astype(jnp.int16)
    low_rows, last_rows = quads * planes, quads * planes * 3 // 2
    for i in range(ty):
        for k in range(pat):
            out_ref[i * pat + k, last_rows : last_rows + 2 * SUB] = last
        for q in range(0, quads, 2):
            for z in range(0, planes, 2 * SUB):
                fixed = []
                for b in (i * quads + q, i * quads + q + 1):
                    v0 = obj_ref[b, z : z + 2 * SUB, 0:LANES]
                    v1 = obj_ref[b, z : z + 2 * SUB, LANES : 2 * LANES]
                    fixed.append(to_log(jnp.where(own, v0, roll(v1, TILE))))
                starts = (q * planes + z, (q + 1) * planes + z, low_rows + q // 2 * planes + z)
                for row, v in zip(starts, encode(*fixed)):
                    for k in range(pat):
                        out_ref[i * pat + k, row : row + 2 * SUB] = v


def final_kernel(dest_of_tile, rows, in_ref, out_ref):
    lane = lane_iota((2 * SUB, LANES))
    planes = out_ref.shape[0] // rows
    tiles_half = LANES // TILE
    quads = rows // 4
    low_rows = quads * planes
    for half in range(len(dest_of_tile) // tiles_half):

        @pl.when(pl.program_id(0) == half)
        def _(half=half):
            for z in range(0, planes, 2 * SUB):
                for q in range(0, quads, 2):
                    starts = (q * planes + z, (q + 1) * planes + z, low_rows + q // 2 * planes + z)
                    both = []
                    for t in range(tiles_half):
                        dest = dest_of(dest_of_tile, half * tiles_half + t)
                        coded = decode(*(in_ref[dest, row : row + 2 * SUB] for row in starts))
                        both.append([from_log(v) for v in coded])
                    for p in range(2):
                        for g, piece in enumerate(quad_transpose([v[p] for v in both], lane)):
                            for h in range(2):
                                start = (z + h * SUB) * rows + 4 * (q + p) + QUAD_ROWS[g]
                                out_ref[pl.ds(start, SUB, stride=rows), :] = piece[h * SUB : (h + 1) * SUB]


def masked_kernel(lateral_kernel, psf_radius):
    offsets = jnp.arange(TAPS) - RADIUS
    within = jnp.abs(offsets)[None, :] <= psf_radius[:, None]
    return jnp.where(within, lateral_kernel, jnp.zeros_like(lateral_kernel)).astype(BF16)


def shape(dims, dtype=F32):
    return jax.ShapeDtypeStruct(dims, dtype)


PARAMS = pltpu.CompilerParams(vmem_limit_bytes=24 * 2**20)
VMEM = pl.BlockSpec(memory_space=pltpu.VMEM)
SMEM = pl.BlockSpec(memory_space=pltpu.SMEM)


def over_tx(value, size):
    if size & (size - 1):
        return lax.psum(value, "tx")
    step = 1
    while step < size:
        value = value + lax.ppermute(value, "tx", [(i, i ^ step) for i in range(size)])
        step *= 2
    return value


def tiled_device(sizes, estimate, data, axial, lateral_kernel, psf_radius, pattern_codes):
    ty, tx, pat = sizes["ty"], sizes["tx"], sizes["pat"]
    planes, rows, cols = estimate.shape
    pat_local = data.shape[0]
    patterns = pat_local * pat
    ny, nx = rows * ty, cols * tx
    members = ty * pat
    blocks = ny // ROWS_BLOCK
    axes = ("ty", "tx", "pat")

    owner = [(i, k if i % 2 == 0 else pat - 1 - k) for i in range(ty) for k in range(pat)]
    dest_of_tile = [i * pat + k for i, k in owner]
    order = [(i * tx + j) * pat + k for j in range(tx) for i, k in (owner if j % 2 == 0 else owner[::-1])]
    to_right = [(a, b) for a, b in zip(order[:-1], order[1:])]
    to_left = [(b, a) for a, b in to_right]
    src_of = (ty, pat)

    ti = lax.axis_index("ty")

    def tile_of():
        i, j, k = (lax.axis_index(a) for a in axes)
        c = i * pat + jnp.where(lax.rem(i, 2) == 0, k, pat - 1 - k)
        return j * members + jnp.where(lax.rem(j, 2) == 0, c, members - 1 - c)

    halves = cols // LANES
    piece_lanes = rows * TILE
    halo_lanes = ny * HALO

    def whole(dims):
        return pl.BlockSpec(dims, lambda h: (0,) * len(dims))

    def half_columns(height):
        return pl.BlockSpec((height, LANES), lambda h: (0, h))

    def edges(pieces, body, name):
        out = shape((pieces.shape[1] * pieces.shape[0] // ty, halo_lanes), pieces.dtype)
        return pl.pallas_call(
            functools.partial(body, (ty, pieces.shape[0] // ty)),
            out_shape=(out, out),
            in_specs=[VMEM],
            out_specs=(VMEM,) * 2,
            compiler_params=PARAMS,
            name=name,
        )(pieces)

    def swap_edges(left, right):
        return lax.ppermute(right, axes, to_right), lax.ppermute(left, axes, to_left)

    message = pl.pallas_call(
        functools.partial(pack_kernel, dest_of_tile, rows),
        out_shape=shape((members, 3 * planes, piece_lanes), jnp.int16),
        grid=(halves,),
        in_specs=[half_columns(data.size // cols)],
        out_specs=whole((members, 3 * planes, piece_lanes)),
        compiler_params=PARAMS,
        name="pack",
    )(data.reshape(-1, cols))
    message, estimate = lax.optimization_barrier((message, estimate))
    mine = lax.all_to_all(message, ("ty", "pat"), 0, 0, tiled=True)

    pieces = pl.pallas_call(
        functools.partial(estimate_kernel, dest_of_tile, rows, pat),
        out_shape=shape((ty, planes, piece_lanes)),
        grid=(halves,),
        in_specs=[half_columns(planes * rows)],
        out_specs=whole((ty, planes, piece_lanes)),
        scratch_shapes=[pltpu.VMEM((members, planes, piece_lanes), F32)],
        compiler_params=PARAMS,
        name="prep_estimate",
    )(estimate.reshape(-1, cols))
    tile_rows = [lax.dynamic_index_in_dim(pieces, ti, 0, keepdims=False)]
    for shift in range(1, ty):
        sent = lax.dynamic_index_in_dim(pieces, (ti + shift) % ty, 0, keepdims=False)
        tile_rows.append(lax.ppermute(sent, "ty", [(i, (i + shift) % ty) for i in range(ty)]))
    tile_rows = jnp.stack(tile_rows)
    tile_rows = jnp.stack(
        [lax.dynamic_index_in_dim(tile_rows, (ti - i) % ty, 0, keepdims=False) for i in range(ty)]
    )
    est_left, est_right = swap_edges(*edges(tile_rows, edges_kernel, "prep_edges"))

    weights, ax_fwd, ax_bwd, light = pl.pallas_call(
        functools.partial(tables_kernel, tile_of),
        out_shape=(
            shape((6, BLOCK, BLOCK), BF16),
            shape((patterns * planes, patterns * planes), BF16),
            shape((2 * planes, 6 * planes), BF16),
            shape((blocks, patterns, BLOCK)),
        ),
        in_specs=[SMEM] * 3 + [VMEM],
        out_specs=(VMEM,) * 4,
        compiler_params=PARAMS,
        name="tables",
    )(lateral_kernel, psf_radius, pattern_codes, axial)
    wave = np.cos(np.arange(planes, dtype=np.float32) * np.float32(TWO_PI * 3.0 / planes))
    wave = jnp.asarray(np.ascontiguousarray(np.broadcast_to(wave[:, None], (planes, BLOCK))))

    object_shape = shape((blocks, planes, BLOCK))
    field_shape = shape((blocks, patterns * planes, BLOCK))
    object_scratch = pltpu.VMEM(object_shape.shape, F32)
    stage = pltpu.VMEM((blocks + 2, patterns * planes, BLOCK), BF16)
    table_specs = [VMEM] * 5
    mine, est_left, est_right, weights = lax.optimization_barrier((mine, est_left, est_right, weights))
    from_left, from_right = swap_edges(*edges(mine, data_edges_kernel, "edges"))
    tables = (weights, ax_fwd, ax_bwd, light, wave)
    current, norm, predicted = pl.pallas_call(
        functools.partial(forward_kernel, nx, tile_of, (ty, 1)),
        out_shape=(object_shape, object_shape, field_shape),
        in_specs=table_specs + [VMEM] * 3,
        out_specs=(VMEM,) * 3,
        scratch_shapes=[stage],
        compiler_params=PARAMS,
        name="forward",
    )(*tables, tile_rows, est_left, est_right)

    edge_shape = shape((planes, halo_lanes))
    data_all, current, left, right, sq_first = pl.pallas_call(
        functools.partial(first_kernel, nx, tile_of, src_of),
        out_shape=(field_shape, object_shape, edge_shape, edge_shape, shape((SUB, LANES))),
        in_specs=table_specs + [VMEM] * 6,
        out_specs=(VMEM,) * 5,
        scratch_shapes=[stage, stage],
        compiler_params=PARAMS,
        name="first",
    )(*tables, norm, current, predicted, mine, from_left, from_right)
    from_left, from_right = swap_edges(left, right)
    outgoing = pl.pallas_call(
        functools.partial(second_kernel, nx, tile_of, src_of),
        out_shape=shape((members, rows // 4 * planes * 3 // 2 + 2 * SUB, LANES), jnp.int16),
        in_specs=table_specs + [VMEM] * 6,
        out_specs=VMEM,
        scratch_shapes=[object_scratch, stage, stage],
        compiler_params=PARAMS,
        name="second",
    )(*tables, norm, data_all, current, from_left, from_right, sq_first)

    incoming = lax.all_to_all(outgoing, ("ty", "pat"), 0, 0, tiled=True)
    last = incoming[:, rows // 4 * planes * 3 // 2 :].astype(jnp.int32) + BIAS
    squares = jnp.sum(from_log((last[:, :ITERS] << 8) + last[:, SUB : SUB + ITERS]), axis=(0, 2))
    squares = over_tx(squares, tx)
    result = pl.pallas_call(
        functools.partial(final_kernel, dest_of_tile, rows),
        out_shape=shape((planes * rows, cols)),
        grid=(halves,),
        in_specs=[whole(incoming.shape)],
        out_specs=half_columns(planes * rows),
        compiler_params=PARAMS,
        name="unpack",
    )(incoming)
    cell_count = float(patterns * planes * ny * nx)
    return result.reshape(estimate.shape), jnp.sqrt(squares / cell_count)


def extended(block, sides, width):
    for axis, dim in sides:
        count = lax.axis_size(axis)
        forward = [(i, i + 1) for i in range(count - 1)]
        backward = [(target, source) for source, target in forward]
        low = lax.ppermute(
            lax.slice_in_dim(block, block.shape[dim] - width, None, axis=dim), axis, forward
        )
        high = lax.ppermute(lax.slice_in_dim(block, 0, width, axis=dim), axis, backward)
        block = jnp.concatenate([low, block, high], axis=dim)
    return block


def wave_table(angle_code, phase_code, row_coord, col_coord, planes):
    step_col = jnp.where(angle_code == 0, 2, -1).astype(jnp.int32)
    step_row = jnp.where(angle_code == 0, 0, jnp.where(angle_code == 1, 2, -2)).astype(jnp.int32)
    argument = (
        step_col[:, None, None] * col_coord[None, None, :]
        + step_row[:, None, None] * row_coord[None, :, None]
        + phase_code[:, None, None]
    ) % 5
    lateral_wave = jnp.cos(argument.astype(jnp.float32) * (TWO_PI / 5.0))
    plane_index = jnp.arange(planes).astype(jnp.float32)
    axial_wave = jnp.cos(plane_index * (TWO_PI * 3.0 / planes))
    return 1.0 + 0.7 * lateral_wave[:, None, :, :] * axial_wave[None, :, None, None]


def tap_matrices(kernel, width_in, width_out):
    tap_count = 2 * RADIUS + 1
    offset = jnp.arange(width_in)[:, None] - jnp.arange(width_out)[None, :]
    onehot = (offset[None, :, :] == jnp.arange(tap_count)[:, None, None]).astype(jnp.float32)
    return jnp.einsum(
        "ij,jab->iab", kernel.astype(jnp.float32), onehot, precision=lax.Precision.HIGHEST
    ).astype(jnp.bfloat16)


def lateral_pass(padded, matrices, height):
    summed = None
    for tap_row in range(2 * RADIUS + 1):
        window = padded[..., tap_row : tap_row + height, :]
        product = jnp.dot(window, matrices[tap_row], preferred_element_type=jnp.float32)
        summed = product if summed is None else summed + product
    return summed


def general_device(estimate, data, axial, lateral_kernel, psf_radius, pattern_codes):
    planes, height, width = estimate.shape
    pat_local = data.shape[0]
    full_rows = height * lax.axis_size("ty")
    full_cols = width * lax.axis_size("tx")
    depth = 2 * RADIUS
    margin = depth - RADIUS
    row_coord = lax.axis_index("ty") * height - depth + jnp.arange(height + 2 * depth)
    col_coord = lax.axis_index("tx") * width - depth + jnp.arange(width + 2 * depth)
    codes_here = lax.dynamic_slice_in_dim(
        pattern_codes, lax.axis_index("pat") * pat_local, pat_local, 1
    )
    lighting = wave_table(codes_here[0], codes_here[1], row_coord, col_coord, planes)
    lighting_inner = lighting[:, :, depth : depth + height, depth : depth + width]
    kernel = masked_kernel(lateral_kernel, psf_radius)
    forward_taps = tap_matrices(kernel, width + 2 * depth, width + 2 * margin)
    adjoint_taps = tap_matrices(kernel[::-1, ::-1], width + 2 * RADIUS, width)
    axial_b = axial.astype(jnp.bfloat16)
    row_inside = (row_coord >= 0) & (row_coord < full_rows)
    col_inside = (col_coord >= 0) & (col_coord < full_cols)
    inside_all = row_inside[:, None] & col_inside[None, :]
    inside = inside_all[
        margin : margin + height + 2 * RADIUS, margin : margin + width + 2 * RADIUS
    ].astype(jnp.bfloat16)
    inside_mid = inside_all[
        RADIUS : RADIUS + height + 2 * margin, RADIUS : RADIUS + width + 2 * margin
    ]
    coverage = lateral_pass(inside[None], adjoint_taps, height).astype(jnp.bfloat16)
    spread = jnp.einsum(
        "ba,byx->ayx",
        axial_b,
        jnp.broadcast_to(coverage, (planes, height, width)),
        preferred_element_type=jnp.float32,
    )
    normalizer = lax.psum(jnp.sum(lighting_inner * spread[None], axis=0), "pat")
    cell_count = float(pat_local * lax.axis_size("pat") * planes * full_rows * full_cols)
    data_wide = extended(data, (("ty", 2), ("tx", 3)), RADIUS)
    current = estimate
    squares_list = []
    for iteration in range(ITERS):
        padded = extended(current, (("ty", 1), ("tx", 2)), depth)
        lighted = (lighting * padded[None]).astype(jnp.bfloat16)
        blurred = jnp.einsum(
            "ab,pbyx->payx", axial_b, lighted, preferred_element_type=jnp.float32
        ).astype(jnp.bfloat16)
        predicted = lateral_pass(blurred, forward_taps, height + 2 * margin)
        predicted_inner = predicted[:, :, margin : margin + height, margin : margin + width]
        misfit = data - predicted_inner
        local_square = jnp.sum(misfit * misfit)
        safe = jnp.where(inside_mid[None, None], predicted, 1.0)
        quotient_padded = jnp.where(inside_mid[None, None], data_wide / safe, 0.0).astype(
            jnp.bfloat16
        )
        backward = lateral_pass(quotient_padded, adjoint_taps, height).astype(jnp.bfloat16)
        gathered = jnp.einsum(
            "ba,pbyx->payx", axial_b, backward, preferred_element_type=jnp.float32
        )
        contribution = jnp.sum(lighting_inner * gathered, axis=0)
        summed = lax.psum(contribution, "pat")
        current = current * summed / normalizer
        squares_list.append(lax.psum(local_square, ("ty", "tx", "pat")))
    squares = jnp.stack(squares_list)
    return (current, jnp.sqrt(squares / cell_count))


def solution(mesh):
    sizes = dict(mesh.shape)
    in_specs = (P(None, "ty", "tx"), P("pat", None, "ty", "tx"), P(), P(), P(), P())
    out_specs = (P(None, "ty", "tx"), P())

    def per_device(estimate, data, *rest):
        planes, rows, cols = estimate.shape
        members = sizes["ty"] * sizes["pat"]
        fits = (
            cols == members * TILE
            and cols % LANES == 0
            and rows % 8 == 0
            and rows * sizes["ty"] <= 2 * TILE
            and planes % (2 * SUB) == 0
            and data.shape[0] == 2
        )
        if fits:
            return tiled_device(sizes, estimate, data, *rest)
        return general_device(estimate, data, *rest)

    return jax.shard_map(
        per_device, mesh=mesh, in_specs=in_specs, out_specs=out_specs, check_vma=False
    )
```

```python
import functools
import math

import jax
import jax.numpy as jnp
import numpy as np
from jax import lax
from jax.experimental import pallas as pl
from jax.experimental.pallas import tpu as pltpu
from jax.sharding import PartitionSpec as P

RADIUS = 4
TAPS = 2 * RADIUS + 1
ITERS = 4
TWO_PI = 2.0 * math.pi

TILE = 32
HALO = 16
GROUP = TILE + 2 * HALO
ROWS_BLOCK = RADIUS
BLOCK = ROWS_BLOCK * GROUP
LANES = 128
SUB = 8
QUAD_ROWS = (0, 2, 1, 3)
CHUNK = 4
OFFSET = 1 << 20
F32 = jnp.float32
BF16 = jnp.bfloat16


def lane_iota(shape):
    return lax.broadcasted_iota(jnp.int32, shape, len(shape) - 1)


def column_of(lane):
    inner = lane % GROUP
    return jnp.where(inner < TILE + HALO, inner, inner - GROUP)


def roll(x, shift):
    shift = shift % LANES
    return x if shift == 0 else pltpu.roll(x, shift, 1)


def quad_transpose(v, lane):
    group = lane // TILE
    out = []
    for t in range(4):
        value = roll(v[0], -TILE * t)
        for g in range(1, 4):
            value = jnp.where(group == g, roll(v[g], TILE * (g - t)), value)
        out.append(value)
    return out


def dest_of(dest_of_tile, c):
    return jnp.where(lax.rem(lax.axis_index("tx"), 2) == 0, dest_of_tile[c], dest_of_tile[-1 - c])


def pack_half(dest_of_tile, rows, half, groups, src_ref, out_ref):
    lane = lane_iota((SUB, LANES))
    tiles_half = LANES // TILE
    for i in range(groups):
        for quad in range(rows // 4):
            v = [src_ref[pl.ds(i * rows * SUB + 4 * quad + r, SUB, stride=rows), :] for r in QUAD_ROWS]
            for t, piece in enumerate(quad_transpose(v, lane)):
                dest = dest_of(dest_of_tile, half * tiles_half + t)
                out_ref[dest, i * SUB : (i + 1) * SUB, quad * LANES : (quad + 1) * LANES] = piece


TOP = 2**24 - 1
DATA_BITS = 20
ROOT_LOW, ROOT_HIGH = math.sqrt(0.1), math.sqrt(6.0)
DATA_TOP = float(2**DATA_BITS - 1)
DATA_SCALE = DATA_TOP / (ROOT_HIGH - ROOT_LOW)
BIAS = 2**15


def to_fixed(v):
    return jnp.clip((jnp.sqrt(v) - ROOT_LOW) * DATA_SCALE + 0.5, 0.0, DATA_TOP).astype(jnp.int32)


def from_fixed(t):
    root = t.astype(F32) * (1.0 / DATA_SCALE) + ROOT_LOW
    return root * root


def encode_four(values):
    low = sum((v & 15) << (4 * n) for n, v in enumerate(values))
    return [(v - BIAS).astype(jnp.int16) for v in [v >> 4 for v in values] + [low]]


def decode_four(words):
    *high, low = [v.astype(jnp.int32) + BIAS for v in words]
    return [(v << 4) + ((low >> (4 * n)) & 15) for n, v in enumerate(high)]


def encode(first, second):
    low = ((first & 255) << 8) + (second & 255)
    return tuple((v - BIAS).astype(jnp.int16) for v in (first >> 8, second >> 8, low))


def decode(first, second, low):
    first, second, low = (v.astype(jnp.int32) + BIAS for v in (first, second, low))
    return (first << 8) + (low >> 8), (second << 8) + (low & 255)


LOG_SCALE, LOG_BIAS, LN2 = 2.0**16, 128.0, math.log(2.0)


def to_log(v):
    t = (jnp.log(jnp.maximum(v, 2.0**-126)) * (1.0 / LN2) + LOG_BIAS) * LOG_SCALE + 0.5
    return jnp.where(v > 0, jnp.clip(t, 1.0, float(TOP)), 0.0).astype(jnp.int32)


def from_log(t):
    return jnp.where(t > 0, jnp.exp2(t.astype(F32) * (1.0 / LOG_SCALE) - LOG_BIAS), 0.0)


def pack_kernel(dest_of_tile, rows, data_ref, out_ref):
    lane = lane_iota((SUB, LANES))
    tiles_half = LANES // TILE
    part = out_ref.shape[1] * 2 // 5
    rows_of = coded_rows(0, part, 1)

    def pieces(row, quad):
        start = row * rows + 4 * quad
        v = [to_fixed(data_ref[pl.ds(start + r, SUB, stride=rows), :]) for r in QUAD_ROWS]
        return quad_transpose(v, lane)

    for half in range(len(dest_of_tile) // tiles_half):

        @pl.when(pl.program_id(0) == half)
        def _(half=half):
            for quad in range(rows // 4):
                found = [(pieces(r.start, quad), pieces(r.start + SUB, quad)) for r in rows_of[:4]]
                for t in range(tiles_half):
                    dest = dest_of(dest_of_tile, half * tiles_half + t)
                    coded = encode_four([jnp.concatenate([v[t], w[t]]) for v, w in found])
                    for r, v in zip(rows_of, coded):
                        out_ref[dest, r, quad * LANES : (quad + 1) * LANES] = v


def estimate_kernel(dest_of_tile, rows, pat, est_ref, out_ref, all_ref):
    halves = len(dest_of_tile) * TILE // LANES
    for half in range(halves):

        @pl.when(pl.program_id(0) == half)
        def _(half=half):
            pack_half(dest_of_tile, rows, half, est_ref.shape[0] // (rows * SUB), est_ref, all_ref)
            if half == halves - 1:
                for i in range(out_ref.shape[0]):
                    out_ref[i] = all_ref[i * pat + lax.axis_index("pat")]


def edge_messages(pieces, lane):
    left = right = None
    for u, (v, offset) in enumerate(pieces):
        slot = (lane // HALO) % 4 == u
        l_u, r_u = roll(v, HALO * u - offset), roll(v, HALO * (u - 1) - offset)
        left = l_u if left is None else jnp.where(slot, l_u, left)
        right = r_u if right is None else jnp.where(slot, r_u, right)
    return left, right


def edges_kernel(src_of, in_ref, left_ref, right_ref):
    lane = lane_iota((SUB, LANES))
    ty, pat = src_of
    groups = in_ref.shape[1] // SUB
    per_ty = in_ref.shape[2] // LANES // 2
    for k in range(pat):
        for g in range(groups):
            row = slice((k * groups + g) * SUB, (k * groups + g + 1) * SUB)
            for i in range(ty):
                for pair in range(per_ty):
                    pieces = []
                    for q in (2 * pair, 2 * pair + 1):
                        v = in_ref[i * pat + k, g * SUB : (g + 1) * SUB, q * LANES : (q + 1) * LANES]
                        pieces += [(v, 0), (v, TILE)]
                    left, right = edge_messages(pieces, lane)
                    vreg = i * per_ty + pair
                    left_ref[row, vreg * LANES : (vreg + 1) * LANES] = left
                    right_ref[row, vreg * LANES : (vreg + 1) * LANES] = right


def coded_rows(k, part, pat):
    first = 2 * k * part
    starts = (first, first + part, first + part // 2, first + part + part // 2, 2 * pat * part + k * part // 2)
    return [slice(r, r + 2 * SUB) for r in starts]


def own_coded(in_ref, source, part, q):
    return decode_four([in_ref[source, r, q * LANES : (q + 1) * LANES] for r in coded_rows(0, part, 1)])


def data_edges_kernel(src_of, in_ref, left_ref, right_ref):
    lane = lane_iota((2 * SUB, LANES))
    ty, pat = src_of
    part = in_ref.shape[1] * 2 // 5
    per_ty = in_ref.shape[2] // LANES // 2
    for k in range(pat):
        rows = coded_rows(k, part, pat)
        for i in range(ty):
            for pair in range(per_ty):
                both = [own_coded(in_ref, i * pat + k, part, q) for q in (2 * pair, 2 * pair + 1)]
                sides = [edge_messages([(v[n], o) for v in both for o in (0, TILE)], lane) for n in range(4)]
                vreg = i * per_ty + pair
                for side, ref in enumerate((left_ref, right_ref)):
                    for r, v in zip(rows, encode_four([found[side] for found in sides])):
                        ref[r, vreg * LANES : (vreg + 1) * LANES] = v


def unpack_data(src_of, in_ref, from_left_ref, from_right_ref, out_ref):
    lane = lane_iota((2 * SUB, LANES))
    ty, pat = src_of
    part = in_ref.shape[1] * 2 // 5
    per_ty = in_ref.shape[2] // LANES // 2
    for k in range(pat):
        rows = coded_rows(k, part, pat)
        for i in range(ty):
            for pair in range(per_ty):
                vreg = i * per_ty + pair
                at = slice(vreg * LANES, (vreg + 1) * LANES)
                from_left = decode_four([from_left_ref[r, at] for r in rows])
                from_right = decode_four([from_right_ref[r, at] for r in rows])
                both = [own_coded(in_ref, i * pat + k, part, q) for q in (2 * pair, 2 * pair + 1)]
                for n in range(4):
                    own = [x for v in both for x in (v[n], roll(v[n], -TILE))]
                    for u in range(4):
                        m = 4 * vreg + u
                        out_ref[m // 2, rows[n], (m % 2) * LANES : (m % 2 + 1) * LANES] = from_fixed(
                            with_halo(own[u], u, from_right[n], from_left[n], lane)
                        )


def unpack_wide(src_of, in_ref, from_left_ref, from_right_ref, out_ref):
    lane = lane_iota((SUB, LANES))
    ty, pat = src_of
    groups = in_ref.shape[1] // SUB
    per_ty = in_ref.shape[2] // LANES // 2
    for k in range(pat):
        for g in range(groups):
            row = slice((k * groups + g) * SUB, (k * groups + g + 1) * SUB)
            for i in range(ty):
                for pair in range(per_ty):
                    vreg = i * per_ty + pair
                    from_left = from_left_ref[row, vreg * LANES : (vreg + 1) * LANES]
                    from_right = from_right_ref[row, vreg * LANES : (vreg + 1) * LANES]
                    own = []
                    for q in (2 * pair, 2 * pair + 1):
                        v = in_ref[i * pat + k, g * SUB : (g + 1) * SUB, q * LANES : (q + 1) * LANES]
                        own += [v, roll(v, -TILE)]
                    for u in range(4):
                        m = 4 * vreg + u
                        out_ref[m // 2, row, (m % 2) * LANES : (m % 2 + 1) * LANES] = with_halo(
                            own[u], u, from_right, from_left, lane
                        )


def with_halo(own, u, from_right, from_left, lane):
    inner = lane % GROUP
    value = jnp.where(inner < TILE, own, roll(from_right, HALO * (2 - u)))
    return jnp.where(inner < TILE + HALO, value, roll(from_left, HALO * (3 - u)))


def tables_kernel(tile_of, k_ref, radius_ref, codes_ref, axial_ref, w_ref, fwd_ref, bwd_ref, light_ref):
    lane = lane_iota((GROUP, LANES))
    row = lax.broadcasted_iota(jnp.int32, (GROUP, LANES), 0)
    tap = column_of(row) - column_of(lane) + RADIUS
    first = lane < GROUP
    hit = [tap == j for j in range(TAPS)]
    nothing = jnp.zeros((GROUP, LANES), BF16)

    def scalar(flip, i, j):
        if i < 0 or i >= TAPS:
            return jnp.float32(0.0)
        if flip:
            i, j = TAPS - 1 - i, TAPS - 1 - j
        return jnp.where(abs(j - RADIUS) <= radius_ref[i], k_ref[i, j], 0.0)

    for flip in range(2):
        for i0 in range(-2, TAPS + 3):
            value = jnp.zeros((GROUP, LANES), F32)
            if 0 <= i0 <= TAPS:
                for j in range(TAPS):
                    both = jnp.where(first, scalar(flip, i0, j), scalar(flip, i0 - 1, j))
                    value = jnp.where(hit[j], both, value)
            value = value.astype(BF16)
            for k in range(3):
                for r in range(ROWS_BLOCK):
                    for q in range(ROWS_BLOCK // 2):
                        if ROWS_BLOCK * (k - 1) + r - 2 * q + RADIUS == i0:
                            w_ref[
                                3 * flip + k,
                                r * GROUP : (r + 1) * GROUP,
                                q * LANES : (q + 1) * LANES,
                            ] = value

    planes, rows = axial_ref.shape[0], fwd_ref.shape[0]
    axial = axial_ref[...].astype(BF16)
    pick = lax.broadcasted_iota(jnp.int32, (planes, rows), 1) % planes
    pick = (pick == lax.broadcasted_iota(jnp.int32, (planes, rows), 0)).astype(F32).astype(BF16)
    plain = jnp.dot(axial, pick, preferred_element_type=F32)
    turned = lax.dot_general(axial, pick, (((0,), (0,)), ((), ())), preferred_element_type=F32)
    column = lax.broadcasted_iota(jnp.int32, (planes, rows), 1)
    for p in range(rows // planes):
        here = column // planes == p
        fwd_ref[p * planes : (p + 1) * planes] = jnp.where(here, plain, 0.0).astype(BF16)
    span = 3 * planes
    for h in range(2):
        here = (column >= h * span) & (column < (h + 1) * span)
        bwd_ref[h * planes : (h + 1) * planes] = jnp.where(here, turned, 0.0).astype(BF16)[:, : 2 * span]

    col = column_of(lane_iota((1, BLOCK)))
    within = lane_iota((1, BLOCK)) // GROUP
    x = tile_of() * TILE + col
    cosines = [0.7 * math.cos(TWO_PI * m / 5.0) for m in range(5)]
    patterns = light_ref.shape[1]
    for p in range(patterns):
        angle, phase = codes_ref[0, p], codes_ref[1, p]
        step_col = jnp.where(angle == 0, 2, -1)
        step_row = jnp.where(angle == 0, 0, jnp.where(angle == 1, 2, -2))
        for b in range(light_ref.shape[0]):
            y = within + b * ROWS_BLOCK
            turn = lax.rem(step_col * x + step_row * y + phase + 5 * OFFSET, 5)
            value = jnp.full((1, BLOCK), cosines[0], F32)
            for m in range(1, 5):
                value = jnp.where(turn == m, cosines[m], value)
            light_ref[b, p : p + 1] = value


def lateral(src_ref, w_ref, flip, b, count):
    total = None
    for k in range(3):
        v = src_ref[b + k : b + k + count]
        part = jnp.dot(v.reshape(-1, BLOCK), w_ref[3 * flip + k], preferred_element_type=F32)
        total = part if total is None else total + part
    return total.reshape(count, -1, BLOCK)


def split3(v):
    high = v.astype(BF16)
    rest = v - high.astype(F32)
    mid = rest.astype(BF16)
    return high, mid, (rest - mid.astype(F32)).astype(BF16)


class Step:
    def __init__(self, nx, tile_of, w_ref, ax_fwd, ax_bwd, light_ref, wave_ref):
        self.w, self.ax_fwd, self.ax_bwd, self.light, self.wave = w_ref, ax_fwd, ax_bwd, light_ref, wave_ref
        self.blocks, self.patterns = light_ref.shape[0], light_ref.shape[1]
        self.planes = wave_ref.shape[0]
        self.col = column_of(lane_iota((1, BLOCK)))
        place = tile_of() * TILE + self.col
        self.inside = (place >= 0) & (place < nx)

    def reach(self, width):
        return self.inside & (self.col >= -width) & (self.col < TILE + width)

    def clear_ends(self, ref):
        ref[0] = jnp.zeros(ref.shape[1:], BF16)
        ref[self.blocks + 1] = jnp.zeros(ref.shape[1:], BF16)

    def normalizer(self, norm_ref):
        depth = self.ax_bwd.shape[1]
        ones = lax.broadcasted_iota(jnp.int32, (depth, BLOCK), 0) < self.planes
        ones = jnp.where(ones, 1.0, 0.0).astype(BF16)
        colsum = jnp.dot(self.ax_bwd[...], ones, preferred_element_type=F32)[: self.planes]
        ones = jnp.broadcast_to(jnp.where(self.inside, 1.0, 0.0), (2 * SUB, BLOCK)).astype(BF16)
        parts = [jnp.dot(ones, self.w[3 + k], preferred_element_type=F32) for k in range(3)]
        for b in range(self.blocks):
            total = sum(parts[k] for k in range(3) if 0 <= b + k - 1 < self.blocks)
            cover = total.astype(BF16).astype(F32)[0:1]
            lat_sum = jnp.sum(self.light[b], axis=0, keepdims=True)
            norm_ref[b] = colsum * cover * (float(self.patterns) + lat_sum * self.wave[...])

    def blur(self, obj_ref, stage_ref):
        for b in range(self.blocks):
            lighting = 1.0 + self.light[b][:, None, :] * self.wave[...][None]
            lit = (lighting * obj_ref[b][None]).astype(BF16).reshape(-1, BLOCK)
            stage_ref[b + 1] = jnp.dot(self.ax_fwd[...], lit, preferred_element_type=F32).astype(BF16)

    def compare(self, stage_ref, data_ref, quot_ref, width, predicted_ref=None):
        ok = self.reach(width)[None]
        acc = jnp.zeros((SUB, BLOCK), F32)
        for b in range(0, self.blocks, CHUNK):
            if predicted_ref is None:
                predicted = lateral(stage_ref, self.w, 0, b, CHUNK)
            else:
                predicted = predicted_ref[b : b + CHUNK]
            data = data_ref[b : b + CHUNK]
            miss = data - predicted
            acc = acc + jnp.sum((miss * miss).reshape(-1, SUB, BLOCK), axis=0)
            quot_ref[b + 1 : b + 1 + CHUNK] = jnp.where(ok, data / predicted, 0.0).astype(BF16)
        row = jnp.sum(jnp.where((self.col >= 0) & (self.col < TILE), acc, 0.0), axis=0, keepdims=True)
        return sum(row[:, h * LANES : (h + 1) * LANES] for h in range(BLOCK // LANES))

    def update(self, quot_ref, obj_ref, norm_ref, width):
        ok = self.reach(width)
        for b0 in range(0, self.blocks, CHUNK):
            back = lateral(quot_ref, self.w, 1, b0, CHUNK).astype(BF16)
            for b in range(b0, b0 + CHUNK):
                part = back[b - b0].astype(F32).reshape(self.patterns, self.planes, BLOCK)
                plain = jnp.sum(part, axis=0)
                waved = jnp.sum(self.light[b][:, None, :] * part, axis=0)
                stack = jnp.concatenate(split3(plain) + split3(waved), axis=0)
                both = jnp.dot(self.ax_bwd[...], stack, preferred_element_type=F32)
                summed = both[: self.planes] + self.wave[...] * both[self.planes :]
                obj_ref[b] = jnp.where(ok, obj_ref[b] * summed / norm_ref[b], 0.0)


def put_halo(own_ref, from_left_ref, from_right_ref, out_ref):
    lane = lane_iota((SUB, LANES))
    for z in range(0, out_ref.shape[1], SUB):
        for vreg in range(out_ref.shape[0] // 2):
            from_left = from_left_ref[z : z + SUB, vreg * LANES : (vreg + 1) * LANES]
            from_right = from_right_ref[z : z + SUB, vreg * LANES : (vreg + 1) * LANES]
            for u in range(4):
                m = 4 * vreg + u
                at = (m // 2, slice(z, z + SUB), slice((m % 2) * LANES, (m % 2 + 1) * LANES))
                out_ref[at] = with_halo(own_ref[at], u, from_right, from_left, lane)


def forward_kernel(nx, tile_of, src_of, w_ref, ax_fwd, ax_bwd, light_ref, wave_ref,
                   est_ref, from_left_ref, from_right_ref, obj_ref, norm_ref, predicted_ref, stage_ref):
    unpack_wide(src_of, est_ref, from_left_ref, from_right_ref, obj_ref)
    step = Step(nx, tile_of, w_ref, ax_fwd, ax_bwd, light_ref, wave_ref)
    step.normalizer(norm_ref)
    step.clear_ends(stage_ref)
    step.blur(obj_ref, stage_ref)
    for b in range(0, step.blocks, CHUNK):
        predicted_ref[b : b + CHUNK] = lateral(stage_ref, w_ref, 0, b, CHUNK)


def first_kernel(nx, tile_of, src_of, w_ref, ax_fwd, ax_bwd, light_ref, wave_ref, norm_ref, obj_in_ref,
                 predicted_ref, in_ref, from_left_ref, from_right_ref, data_ref, obj_ref, left_ref, right_ref,
                 sq_ref, stage_ref, quot_ref):
    unpack_data(src_of, in_ref, from_left_ref, from_right_ref, data_ref)
    step = Step(nx, tile_of, w_ref, ax_fwd, ax_bwd, light_ref, wave_ref)
    step.clear_ends(stage_ref)
    step.clear_ends(quot_ref)
    obj_ref[...] = obj_in_ref[...]
    sq_ref[...] = jnp.zeros(sq_ref.shape, F32)
    sq_ref[0:1] = step.compare(None, data_ref, quot_ref, 12, predicted_ref)
    step.update(quot_ref, obj_ref, norm_ref, 8)
    step.blur(obj_ref, stage_ref)
    sq_ref[1:2] = step.compare(stage_ref, data_ref, quot_ref, 4)
    step.update(quot_ref, obj_ref, norm_ref, 0)

    lane = lane_iota((SUB, LANES))
    for z in range(0, step.planes, SUB):
        for vreg in range(step.blocks // 2):
            pieces = []
            for u in range(4):
                m = 4 * vreg + u
                pieces.append((obj_ref[m // 2, z : z + SUB, (m % 2) * LANES : (m % 2 + 1) * LANES], 0))
            left, right = edge_messages(pieces, lane)
            left_ref[z : z + SUB, vreg * LANES : (vreg + 1) * LANES] = left
            right_ref[z : z + SUB, vreg * LANES : (vreg + 1) * LANES] = right


def second_kernel(nx, tile_of, src_of, w_ref, ax_fwd, ax_bwd, light_ref, wave_ref, norm_ref, data_ref,
                  obj_in_ref, from_left_ref, from_right_ref, sq_in_ref, out_ref, obj_ref, stage_ref, quot_ref):
    put_halo(obj_in_ref, from_left_ref, from_right_ref, obj_ref)
    step = Step(nx, tile_of, w_ref, ax_fwd, ax_bwd, light_ref, wave_ref)
    step.clear_ends(stage_ref)
    step.clear_ends(quot_ref)
    squares = [sq_in_ref[0:1], sq_in_ref[1:2]]
    for quot_width, obj_width in ((12, 8), (4, 0)):
        step.blur(obj_ref, stage_ref)
        squares.append(step.compare(stage_ref, data_ref, quot_ref, quot_width))
        step.update(quot_ref, obj_ref, norm_ref, obj_width)

    ty, pat = src_of
    quads = step.blocks // ty
    planes = step.planes
    lane = lane_iota((2 * SUB, LANES))
    own = (lane // TILE) % 2 == 0
    last = to_log(jnp.concatenate(squares + [jnp.zeros((SUB - len(squares), LANES), F32)], axis=0))
    last = (jnp.concatenate([last >> 8, last & 255]) - BIAS).astype(jnp.int16)
    low_rows, last_rows = quads * planes, quads * planes * 3 // 2
    for i in range(ty):
        for k in range(pat):
            out_ref[i * pat + k, last_rows : last_rows + 2 * SUB] = last
        for q in range(0, quads, 2):
            for z in range(0, planes, 2 * SUB):
                fixed = []
                for b in (i * quads + q, i * quads + q + 1):
                    v0 = obj_ref[b, z : z + 2 * SUB, 0:LANES]
                    v1 = obj_ref[b, z : z + 2 * SUB, LANES : 2 * LANES]
                    fixed.append(to_log(jnp.where(own, v0, roll(v1, TILE))))
                starts = (q * planes + z, (q + 1) * planes + z, low_rows + q // 2 * planes + z)
                for row, v in zip(starts, encode(*fixed)):
                    for k in range(pat):
                        out_ref[i * pat + k, row : row + 2 * SUB] = v


def final_kernel(dest_of_tile, rows, in_ref, out_ref):
    lane = lane_iota((2 * SUB, LANES))
    planes = out_ref.shape[0] // rows
    tiles_half = LANES // TILE
    quads = rows // 4
    low_rows = quads * planes
    for half in range(len(dest_of_tile) // tiles_half):

        @pl.when(pl.program_id(0) == half)
        def _(half=half):
            for z in range(0, planes, 2 * SUB):
                for q in range(0, quads, 2):
                    starts = (q * planes + z, (q + 1) * planes + z, low_rows + q // 2 * planes + z)
                    both = []
                    for t in range(tiles_half):
                        dest = dest_of(dest_of_tile, half * tiles_half + t)
                        coded = decode(*(in_ref[dest, row : row + 2 * SUB] for row in starts))
                        both.append([from_log(v) for v in coded])
                    for p in range(2):
                        for g, piece in enumerate(quad_transpose([v[p] for v in both], lane)):
                            for h in range(2):
                                start = (z + h * SUB) * rows + 4 * (q + p) + QUAD_ROWS[g]
                                out_ref[pl.ds(start, SUB, stride=rows), :] = piece[h * SUB : (h + 1) * SUB]


def masked_kernel(lateral_kernel, psf_radius):
    offsets = jnp.arange(TAPS) - RADIUS
    within = jnp.abs(offsets)[None, :] <= psf_radius[:, None]
    return jnp.where(within, lateral_kernel, jnp.zeros_like(lateral_kernel)).astype(BF16)


def shape(dims, dtype=F32):
    return jax.ShapeDtypeStruct(dims, dtype)


PARAMS = pltpu.CompilerParams(vmem_limit_bytes=24 * 2**20)
VMEM = pl.BlockSpec(memory_space=pltpu.VMEM)
SMEM = pl.BlockSpec(memory_space=pltpu.SMEM)


def over_tx(value, size):
    if size & (size - 1):
        return lax.psum(value, "tx")
    step = 1
    while step < size:
        value = value + lax.ppermute(value, "tx", [(i, i ^ step) for i in range(size)])
        step *= 2
    return value


def tiled_device(sizes, estimate, data, axial, lateral_kernel, psf_radius, pattern_codes):
    ty, tx, pat = sizes["ty"], sizes["tx"], sizes["pat"]
    planes, rows, cols = estimate.shape
    pat_local = data.shape[0]
    patterns = pat_local * pat
    ny, nx = rows * ty, cols * tx
    members = ty * pat
    blocks = ny // ROWS_BLOCK
    axes = ("ty", "tx", "pat")

    owner = [(i, k if i % 2 == 0 else pat - 1 - k) for i in range(ty) for k in range(pat)]
    dest_of_tile = [i * pat + k for i, k in owner]
    order = [(i * tx + j) * pat + k for j in range(tx) for i, k in (owner if j % 2 == 0 else owner[::-1])]
    to_right = [(a, b) for a, b in zip(order[:-1], order[1:])]
    to_left = [(b, a) for a, b in to_right]
    src_of = (ty, pat)

    ti = lax.axis_index("ty")

    def tile_of():
        i, j, k = (lax.axis_index(a) for a in axes)
        c = i * pat + jnp.where(lax.rem(i, 2) == 0, k, pat - 1 - k)
        return j * members + jnp.where(lax.rem(j, 2) == 0, c, members - 1 - c)

    halves = cols // LANES
    piece_lanes = rows * TILE
    halo_lanes = ny * HALO

    def whole(dims):
        return pl.BlockSpec(dims, lambda h: (0,) * len(dims))

    def half_columns(height):
        return pl.BlockSpec((height, LANES), lambda h: (0, h))

    def edges(pieces, body, name):
        out = shape((pieces.shape[1] * pieces.shape[0] // ty, halo_lanes), pieces.dtype)
        return pl.pallas_call(
            functools.partial(body, (ty, pieces.shape[0] // ty)),
            out_shape=(out, out),
            in_specs=[VMEM],
            out_specs=(VMEM,) * 2,
            compiler_params=PARAMS,
            name=name,
        )(pieces)

    def swap_edges(left, right):
        return lax.ppermute(right, axes, to_right), lax.ppermute(left, axes, to_left)

    message = pl.pallas_call(
        functools.partial(pack_kernel, dest_of_tile, rows),
        out_shape=shape((members, 5 * planes // 2, piece_lanes), jnp.int16),
        grid=(halves,),
        in_specs=[half_columns(data.size // cols)],
        out_specs=whole((members, 5 * planes // 2, piece_lanes)),
        compiler_params=PARAMS,
        name="pack",
    )(data.reshape(-1, cols))
    message, estimate = lax.optimization_barrier((message, estimate))
    mine = lax.all_to_all(message, ("ty", "pat"), 0, 0, tiled=True)

    pieces = pl.pallas_call(
        functools.partial(estimate_kernel, dest_of_tile, rows, pat),
        out_shape=shape((ty, planes, piece_lanes)),
        grid=(halves,),
        in_specs=[half_columns(planes * rows)],
        out_specs=whole((ty, planes, piece_lanes)),
        scratch_shapes=[pltpu.VMEM((members, planes, piece_lanes), F32)],
        compiler_params=PARAMS,
        name="prep_estimate",
    )(estimate.reshape(-1, cols))
    tile_rows = [lax.dynamic_index_in_dim(pieces, ti, 0, keepdims=False)]
    for shift in range(1, ty):
        sent = lax.dynamic_index_in_dim(pieces, (ti + shift) % ty, 0, keepdims=False)
        tile_rows.append(lax.ppermute(sent, "ty", [(i, (i + shift) % ty) for i in range(ty)]))
    tile_rows = jnp.stack(tile_rows)
    tile_rows = jnp.stack(
        [lax.dynamic_index_in_dim(tile_rows, (ti - i) % ty, 0, keepdims=False) for i in range(ty)]
    )
    est_left, est_right = swap_edges(*edges(tile_rows, edges_kernel, "prep_edges"))

    weights, ax_fwd, ax_bwd, light = pl.pallas_call(
        functools.partial(tables_kernel, tile_of),
        out_shape=(
            shape((6, BLOCK, BLOCK), BF16),
            shape((patterns * planes, patterns * planes), BF16),
            shape((2 * planes, 6 * planes), BF16),
            shape((blocks, patterns, BLOCK)),
        ),
        in_specs=[SMEM] * 3 + [VMEM],
        out_specs=(VMEM,) * 4,
        compiler_params=PARAMS,
        name="tables",
    )(lateral_kernel, psf_radius, pattern_codes, axial)
    wave = np.cos(np.arange(planes, dtype=np.float32) * np.float32(TWO_PI * 3.0 / planes))
    wave = jnp.asarray(np.ascontiguousarray(np.broadcast_to(wave[:, None], (planes, BLOCK))))

    object_shape = shape((blocks, planes, BLOCK))
    field_shape = shape((blocks, patterns * planes, BLOCK))
    object_scratch = pltpu.VMEM(object_shape.shape, F32)
    stage = pltpu.VMEM((blocks + 2, patterns * planes, BLOCK), BF16)
    table_specs = [VMEM] * 5
    mine, est_left, est_right, weights = lax.optimization_barrier((mine, est_left, est_right, weights))
    from_left, from_right = swap_edges(*edges(mine, data_edges_kernel, "edges"))
    tables = (weights, ax_fwd, ax_bwd, light, wave)
    current, norm, predicted = pl.pallas_call(
        functools.partial(forward_kernel, nx, tile_of, (ty, 1)),
        out_shape=(object_shape, object_shape, field_shape),
        in_specs=table_specs + [VMEM] * 3,
        out_specs=(VMEM,) * 3,
        scratch_shapes=[stage],
        compiler_params=PARAMS,
        name="forward",
    )(*tables, tile_rows, est_left, est_right)

    edge_shape = shape((planes, halo_lanes))
    data_all, current, left, right, sq_first = pl.pallas_call(
        functools.partial(first_kernel, nx, tile_of, src_of),
        out_shape=(field_shape, object_shape, edge_shape, edge_shape, shape((SUB, LANES))),
        in_specs=table_specs + [VMEM] * 6,
        out_specs=(VMEM,) * 5,
        scratch_shapes=[stage, stage],
        compiler_params=PARAMS,
        name="first",
    )(*tables, norm, current, predicted, mine, from_left, from_right)
    from_left, from_right = swap_edges(left, right)
    outgoing = pl.pallas_call(
        functools.partial(second_kernel, nx, tile_of, src_of),
        out_shape=shape((members, rows // 4 * planes * 3 // 2 + 2 * SUB, LANES), jnp.int16),
        in_specs=table_specs + [VMEM] * 6,
        out_specs=VMEM,
        scratch_shapes=[object_scratch, stage, stage],
        compiler_params=PARAMS,
        name="second",
    )(*tables, norm, data_all, current, from_left, from_right, sq_first)

    incoming = lax.all_to_all(outgoing, ("ty", "pat"), 0, 0, tiled=True)
    last = incoming[:, rows // 4 * planes * 3 // 2 :].astype(jnp.int32) + BIAS
    squares = jnp.sum(from_log((last[:, :ITERS] << 8) + last[:, SUB : SUB + ITERS]), axis=(0, 2))
    squares = over_tx(squares, tx)
    result = pl.pallas_call(
        functools.partial(final_kernel, dest_of_tile, rows),
        out_shape=shape((planes * rows, cols)),
        grid=(halves,),
        in_specs=[whole(incoming.shape)],
        out_specs=half_columns(planes * rows),
        compiler_params=PARAMS,
        name="unpack",
    )(incoming)
    cell_count = float(patterns * planes * ny * nx)
    return result.reshape(estimate.shape), jnp.sqrt(squares / cell_count)


def extended(block, sides, width):
    for axis, dim in sides:
        count = lax.axis_size(axis)
        forward = [(i, i + 1) for i in range(count - 1)]
        backward = [(target, source) for source, target in forward]
        low = lax.ppermute(
            lax.slice_in_dim(block, block.shape[dim] - width, None, axis=dim), axis, forward
        )
        high = lax.ppermute(lax.slice_in_dim(block, 0, width, axis=dim), axis, backward)
        block = jnp.concatenate([low, block, high], axis=dim)
    return block


def wave_table(angle_code, phase_code, row_coord, col_coord, planes):
    step_col = jnp.where(angle_code == 0, 2, -1).astype(jnp.int32)
    step_row = jnp.where(angle_code == 0, 0, jnp.where(angle_code == 1, 2, -2)).astype(jnp.int32)
    argument = (
        step_col[:, None, None] * col_coord[None, None, :]
        + step_row[:, None, None] * row_coord[None, :, None]
        + phase_code[:, None, None]
    ) % 5
    lateral_wave = jnp.cos(argument.astype(jnp.float32) * (TWO_PI / 5.0))
    plane_index = jnp.arange(planes).astype(jnp.float32)
    axial_wave = jnp.cos(plane_index * (TWO_PI * 3.0 / planes))
    return 1.0 + 0.7 * lateral_wave[:, None, :, :] * axial_wave[None, :, None, None]


def tap_matrices(kernel, width_in, width_out):
    tap_count = 2 * RADIUS + 1
    offset = jnp.arange(width_in)[:, None] - jnp.arange(width_out)[None, :]
    onehot = (offset[None, :, :] == jnp.arange(tap_count)[:, None, None]).astype(jnp.float32)
    return jnp.einsum(
        "ij,jab->iab", kernel.astype(jnp.float32), onehot, precision=lax.Precision.HIGHEST
    ).astype(jnp.bfloat16)


def lateral_pass(padded, matrices, height):
    summed = None
    for tap_row in range(2 * RADIUS + 1):
        window = padded[..., tap_row : tap_row + height, :]
        product = jnp.dot(window, matrices[tap_row], preferred_element_type=jnp.float32)
        summed = product if summed is None else summed + product
    return summed


def general_device(estimate, data, axial, lateral_kernel, psf_radius, pattern_codes):
    planes, height, width = estimate.shape
    pat_local = data.shape[0]
    full_rows = height * lax.axis_size("ty")
    full_cols = width * lax.axis_size("tx")
    depth = 2 * RADIUS
    margin = depth - RADIUS
    row_coord = lax.axis_index("ty") * height - depth + jnp.arange(height + 2 * depth)
    col_coord = lax.axis_index("tx") * width - depth + jnp.arange(width + 2 * depth)
    codes_here = lax.dynamic_slice_in_dim(
        pattern_codes, lax.axis_index("pat") * pat_local, pat_local, 1
    )
    lighting = wave_table(codes_here[0], codes_here[1], row_coord, col_coord, planes)
    lighting_inner = lighting[:, :, depth : depth + height, depth : depth + width]
    kernel = masked_kernel(lateral_kernel, psf_radius)
    forward_taps = tap_matrices(kernel, width + 2 * depth, width + 2 * margin)
    adjoint_taps = tap_matrices(kernel[::-1, ::-1], width + 2 * RADIUS, width)
    axial_b = axial.astype(jnp.bfloat16)
    row_inside = (row_coord >= 0) & (row_coord < full_rows)
    col_inside = (col_coord >= 0) & (col_coord < full_cols)
    inside_all = row_inside[:, None] & col_inside[None, :]
    inside = inside_all[
        margin : margin + height + 2 * RADIUS, margin : margin + width + 2 * RADIUS
    ].astype(jnp.bfloat16)
    inside_mid = inside_all[
        RADIUS : RADIUS + height + 2 * margin, RADIUS : RADIUS + width + 2 * margin
    ]
    coverage = lateral_pass(inside[None], adjoint_taps, height).astype(jnp.bfloat16)
    spread = jnp.einsum(
        "ba,byx->ayx",
        axial_b,
        jnp.broadcast_to(coverage, (planes, height, width)),
        preferred_element_type=jnp.float32,
    )
    normalizer = lax.psum(jnp.sum(lighting_inner * spread[None], axis=0), "pat")
    cell_count = float(pat_local * lax.axis_size("pat") * planes * full_rows * full_cols)
    data_wide = extended(data, (("ty", 2), ("tx", 3)), RADIUS)
    current = estimate
    squares_list = []
    for iteration in range(ITERS):
        padded = extended(current, (("ty", 1), ("tx", 2)), depth)
        lighted = (lighting * padded[None]).astype(jnp.bfloat16)
        blurred = jnp.einsum(
            "ab,pbyx->payx", axial_b, lighted, preferred_element_type=jnp.float32
        ).astype(jnp.bfloat16)
        predicted = lateral_pass(blurred, forward_taps, height + 2 * margin)
        predicted_inner = predicted[:, :, margin : margin + height, margin : margin + width]
        misfit = data - predicted_inner
        local_square = jnp.sum(misfit * misfit)
        safe = jnp.where(inside_mid[None, None], predicted, 1.0)
        quotient_padded = jnp.where(inside_mid[None, None], data_wide / safe, 0.0).astype(
            jnp.bfloat16
        )
        backward = lateral_pass(quotient_padded, adjoint_taps, height).astype(jnp.bfloat16)
        gathered = jnp.einsum(
            "ba,pbyx->payx", axial_b, backward, preferred_element_type=jnp.float32
        )
        contribution = jnp.sum(lighting_inner * gathered, axis=0)
        summed = lax.psum(contribution, "pat")
        current = current * summed / normalizer
        squares_list.append(lax.psum(local_square, ("ty", "tx", "pat")))
    squares = jnp.stack(squares_list)
    return (current, jnp.sqrt(squares / cell_count))


def solution(mesh):
    sizes = dict(mesh.shape)
    in_specs = (P(None, "ty", "tx"), P("pat", None, "ty", "tx"), P(), P(), P(), P())
    out_specs = (P(None, "ty", "tx"), P())

    def per_device(estimate, data, *rest):
        planes, rows, cols = estimate.shape
        members = sizes["ty"] * sizes["pat"]
        fits = (
            cols == members * TILE
            and cols % LANES == 0
            and rows % 8 == 0
            and rows * sizes["ty"] <= 2 * TILE
            and planes == 4 * SUB
            and data.shape[0] == 2
        )
        if fits:
            return tiled_device(sizes, estimate, data, *rest)
        return general_device(estimate, data, *rest)

    return jax.shard_map(
        per_device, mesh=mesh, in_specs=in_specs, out_specs=out_specs, check_vma=False
    )
```

```python
import functools
import math

import jax
import jax.numpy as jnp
import numpy as np
from jax import lax
from jax.experimental import pallas as pl
from jax.experimental.pallas import tpu as pltpu
from jax.sharding import PartitionSpec as P

RADIUS = 4
TAPS = 2 * RADIUS + 1
ITERS = 4
TWO_PI = 2.0 * math.pi

TILE = 32
HALO = 16
GROUP = TILE + 2 * HALO
ROWS_BLOCK = RADIUS
BLOCK = ROWS_BLOCK * GROUP
LANES = 128
SUB = 8
QUAD_ROWS = (0, 2, 1, 3)
CHUNK = 4
OFFSET = 1 << 20
F32 = jnp.float32
BF16 = jnp.bfloat16


def lane_iota(shape):
    return lax.broadcasted_iota(jnp.int32, shape, len(shape) - 1)


def column_of(lane):
    inner = lane % GROUP
    return jnp.where(inner < TILE + HALO, inner, inner - GROUP)


def roll(x, shift):
    shift = shift % LANES
    return x if shift == 0 else pltpu.roll(x, shift, 1)


def quad_transpose(v, lane):
    group = lane // TILE
    out = []
    for t in range(4):
        value = roll(v[0], -TILE * t)
        for g in range(1, 4):
            value = jnp.where(group == g, roll(v[g], TILE * (g - t)), value)
        out.append(value)
    return out


def dest_of(dest_of_tile, c):
    return jnp.where(lax.rem(lax.axis_index("tx"), 2) == 0, dest_of_tile[c], dest_of_tile[-1 - c])


def pack_half(dest_of_tile, rows, half, groups, src_ref, out_ref):
    lane = lane_iota((SUB, LANES))
    tiles_half = LANES // TILE
    for i in range(groups):
        for quad in range(rows // 4):
            v = [src_ref[pl.ds(i * rows * SUB + 4 * quad + r, SUB, stride=rows), :] for r in QUAD_ROWS]
            for t, piece in enumerate(quad_transpose(v, lane)):
                dest = dest_of(dest_of_tile, half * tiles_half + t)
                out_ref[dest, i * SUB : (i + 1) * SUB, quad * LANES : (quad + 1) * LANES] = piece


TOP = 2**24 - 1
DATA_BITS = 20
ROOT_LOW, ROOT_HIGH = math.sqrt(0.1), math.sqrt(6.0)
DATA_TOP = float(2**DATA_BITS - 1)
DATA_SCALE = DATA_TOP / (ROOT_HIGH - ROOT_LOW)
BIAS = 2**15


def to_fixed(v):
    return jnp.clip((jnp.sqrt(v) - ROOT_LOW) * DATA_SCALE + 0.5, 0.0, DATA_TOP).astype(jnp.int32)


def from_fixed(t):
    root = t.astype(F32) * (1.0 / DATA_SCALE) + ROOT_LOW
    return root * root


def encode_four(values):
    low = sum((v & 15) << (4 * n) for n, v in enumerate(values))
    return [(v - BIAS).astype(jnp.int16) for v in [v >> 4 for v in values] + [low]]


def decode_four(words):
    *high, low = [v.astype(jnp.int32) + BIAS for v in words]
    return [(v << 4) + ((low >> (4 * n)) & 15) for n, v in enumerate(high)]


def encode(first, second):
    low = ((first & 255) << 8) + (second & 255)
    return tuple((v - BIAS).astype(jnp.int16) for v in (first >> 8, second >> 8, low))


def decode(first, second, low):
    first, second, low = (v.astype(jnp.int32) + BIAS for v in (first, second, low))
    return (first << 8) + (low >> 8), (second << 8) + (low & 255)


LOG_SCALE, LOG_BIAS, LN2 = 2.0**16, 128.0, math.log(2.0)


def to_log(v):
    t = (jnp.log(jnp.maximum(v, 2.0**-126)) * (1.0 / LN2) + LOG_BIAS) * LOG_SCALE + 0.5
    return jnp.where(v > 0, jnp.clip(t, 1.0, float(TOP)), 0.0).astype(jnp.int32)


def from_log(t):
    return jnp.where(t > 0, jnp.exp2(t.astype(F32) * (1.0 / LOG_SCALE) - LOG_BIAS), 0.0)


def pack_kernel(dest_of_tile, rows, data_ref, out_ref):
    lane = lane_iota((SUB, LANES))
    tiles_half = LANES // TILE
    part = out_ref.shape[1] * 2 // 5
    rows_of = coded_rows(0, part, 1)

    def pieces(row, quad):
        start = row * rows + 4 * quad
        v = [to_fixed(data_ref[pl.ds(start + r, SUB, stride=rows), :]) for r in QUAD_ROWS]
        return quad_transpose(v, lane)

    for half in range(len(dest_of_tile) // tiles_half):

        @pl.when(pl.program_id(0) == half)
        def _(half=half):
            for quad in range(rows // 4):
                found = [(pieces(r.start, quad), pieces(r.start + SUB, quad)) for r in rows_of[:4]]
                for t in range(tiles_half):
                    dest = dest_of(dest_of_tile, half * tiles_half + t)
                    coded = encode_four([jnp.concatenate([v[t], w[t]]) for v, w in found])
                    for r, v in zip(rows_of, coded):
                        out_ref[dest, r, quad * LANES : (quad + 1) * LANES] = v


def estimate_kernel(dest_of_tile, rows, pat, est_ref, out_ref, all_ref):
    halves = len(dest_of_tile) * TILE // LANES
    for half in range(halves):

        @pl.when(pl.program_id(0) == half)
        def _(half=half):
            pack_half(dest_of_tile, rows, half, est_ref.shape[0] // (rows * SUB), est_ref, all_ref)
            if half == halves - 1:
                for i in range(out_ref.shape[0]):
                    out_ref[i] = all_ref[i * pat + lax.axis_index("pat")]


def edge_messages(pieces, lane):
    left = right = None
    for u, (v, offset) in enumerate(pieces):
        slot = (lane // HALO) % 4 == u
        l_u, r_u = roll(v, HALO * u - offset), roll(v, HALO * (u - 1) - offset)
        left = l_u if left is None else jnp.where(slot, l_u, left)
        right = r_u if right is None else jnp.where(slot, r_u, right)
    return left, right


def edges_kernel(src_of, in_ref, left_ref, right_ref):
    lane = lane_iota((SUB, LANES))
    ty, pat = src_of
    groups = in_ref.shape[1] // SUB
    per_ty = in_ref.shape[2] // LANES // 2
    for k in range(pat):
        for g in range(groups):
            row = slice((k * groups + g) * SUB, (k * groups + g + 1) * SUB)
            for i in range(ty):
                for pair in range(per_ty):
                    pieces = []
                    for q in (2 * pair, 2 * pair + 1):
                        v = in_ref[i * pat + k, g * SUB : (g + 1) * SUB, q * LANES : (q + 1) * LANES]
                        pieces += [(v, 0), (v, TILE)]
                    left, right = edge_messages(pieces, lane)
                    vreg = i * per_ty + pair
                    left_ref[row, vreg * LANES : (vreg + 1) * LANES] = left
                    right_ref[row, vreg * LANES : (vreg + 1) * LANES] = right


def coded_rows(k, part, pat):
    first = 2 * k * part
    starts = (first, first + part, first + part // 2, first + part + part // 2, 2 * pat * part + k * part // 2)
    return [slice(r, r + 2 * SUB) for r in starts]


def own_coded(in_ref, source, part, q):
    return decode_four([in_ref[source, r, q * LANES : (q + 1) * LANES] for r in coded_rows(0, part, 1)])


def data_edges_kernel(src_of, in_ref, left_ref, right_ref):
    lane = lane_iota((2 * SUB, LANES))
    ty, pat = src_of
    part = in_ref.shape[1] * 2 // 5
    per_ty = in_ref.shape[2] // LANES // 2
    for k in range(pat):
        rows = coded_rows(k, part, pat)
        for i in range(ty):
            for pair in range(per_ty):
                both = [own_coded(in_ref, i * pat + k, part, q) for q in (2 * pair, 2 * pair + 1)]
                sides = [edge_messages([(v[n], o) for v in both for o in (0, TILE)], lane) for n in range(4)]
                vreg = i * per_ty + pair
                for side, ref in enumerate((left_ref, right_ref)):
                    for r, v in zip(rows, encode_four([found[side] for found in sides])):
                        ref[r, vreg * LANES : (vreg + 1) * LANES] = v


def unpack_data(src_of, in_ref, from_left_ref, from_right_ref, out_ref):
    lane = lane_iota((2 * SUB, LANES))
    ty, pat = src_of
    part = in_ref.shape[1] * 2 // 5
    per_ty = in_ref.shape[2] // LANES // 2
    for k in range(pat):
        rows = coded_rows(k, part, pat)
        for i in range(ty):
            for pair in range(per_ty):
                vreg = i * per_ty + pair
                at = slice(vreg * LANES, (vreg + 1) * LANES)
                from_left = decode_four([from_left_ref[r, at] for r in rows])
                from_right = decode_four([from_right_ref[r, at] for r in rows])
                both = [own_coded(in_ref, i * pat + k, part, q) for q in (2 * pair, 2 * pair + 1)]
                for n in range(4):
                    own = [x for v in both for x in (v[n], roll(v[n], -TILE))]
                    for u in range(4):
                        m = 4 * vreg + u
                        out_ref[m // 2, rows[n], (m % 2) * LANES : (m % 2 + 1) * LANES] = from_fixed(
                            with_halo(own[u], u, from_right[n], from_left[n], lane)
                        )


def unpack_wide(src_of, in_ref, from_left_ref, from_right_ref, out_ref):
    lane = lane_iota((SUB, LANES))
    ty, pat = src_of
    groups = in_ref.shape[1] // SUB
    per_ty = in_ref.shape[2] // LANES // 2
    for k in range(pat):
        for g in range(groups):
            row = slice((k * groups + g) * SUB, (k * groups + g + 1) * SUB)
            for i in range(ty):
                for pair in range(per_ty):
                    vreg = i * per_ty + pair
                    from_left = from_left_ref[row, vreg * LANES : (vreg + 1) * LANES]
                    from_right = from_right_ref[row, vreg * LANES : (vreg + 1) * LANES]
                    own = []
                    for q in (2 * pair, 2 * pair + 1):
                        v = in_ref[i * pat + k, g * SUB : (g + 1) * SUB, q * LANES : (q + 1) * LANES]
                        own += [v, roll(v, -TILE)]
                    for u in range(4):
                        m = 4 * vreg + u
                        out_ref[m // 2, row, (m % 2) * LANES : (m % 2 + 1) * LANES] = with_halo(
                            own[u], u, from_right, from_left, lane
                        )


def with_halo(own, u, from_right, from_left, lane):
    inner = lane % GROUP
    value = jnp.where(inner < TILE, own, roll(from_right, HALO * (2 - u)))
    return jnp.where(inner < TILE + HALO, value, roll(from_left, HALO * (3 - u)))


def tables_kernel(tile_of, k_ref, radius_ref, codes_ref, axial_ref, w_ref, fwd_ref, bwd_ref, light_ref):
    lane = lane_iota((GROUP, LANES))
    row = lax.broadcasted_iota(jnp.int32, (GROUP, LANES), 0)
    tap = column_of(row) - column_of(lane) + RADIUS
    first = lane < GROUP
    hit = [tap == j for j in range(TAPS)]
    nothing = jnp.zeros((GROUP, LANES), BF16)

    def scalar(flip, i, j):
        if i < 0 or i >= TAPS:
            return jnp.float32(0.0)
        if flip:
            i, j = TAPS - 1 - i, TAPS - 1 - j
        return jnp.where(abs(j - RADIUS) <= radius_ref[i], k_ref[i, j], 0.0)

    for flip in range(2):
        for i0 in range(-2, TAPS + 3):
            value = jnp.zeros((GROUP, LANES), F32)
            if 0 <= i0 <= TAPS:
                for j in range(TAPS):
                    both = jnp.where(first, scalar(flip, i0, j), scalar(flip, i0 - 1, j))
                    value = jnp.where(hit[j], both, value)
            value = value.astype(BF16)
            for k in range(3):
                for r in range(ROWS_BLOCK):
                    for q in range(ROWS_BLOCK // 2):
                        if ROWS_BLOCK * (k - 1) + r - 2 * q + RADIUS == i0:
                            w_ref[
                                3 * flip + k,
                                r * GROUP : (r + 1) * GROUP,
                                q * LANES : (q + 1) * LANES,
                            ] = value

    planes, rows = axial_ref.shape[0], fwd_ref.shape[0]
    axial = axial_ref[...].astype(BF16)
    pick = lax.broadcasted_iota(jnp.int32, (planes, rows), 1) % planes
    pick = (pick == lax.broadcasted_iota(jnp.int32, (planes, rows), 0)).astype(F32).astype(BF16)
    plain = jnp.dot(axial, pick, preferred_element_type=F32)
    turned = lax.dot_general(axial, pick, (((0,), (0,)), ((), ())), preferred_element_type=F32)
    column = lax.broadcasted_iota(jnp.int32, (planes, rows), 1)
    for p in range(rows // planes):
        here = column // planes == p
        fwd_ref[p * planes : (p + 1) * planes] = jnp.where(here, plain, 0.0).astype(BF16)
    span = 3 * planes
    for h in range(2):
        here = (column >= h * span) & (column < (h + 1) * span)
        bwd_ref[h * planes : (h + 1) * planes] = jnp.where(here, turned, 0.0).astype(BF16)[:, : 2 * span]

    col = column_of(lane_iota((1, BLOCK)))
    within = lane_iota((1, BLOCK)) // GROUP
    x = tile_of() * TILE + col
    cosines = [0.7 * math.cos(TWO_PI * m / 5.0) for m in range(5)]
    patterns = light_ref.shape[1]
    for p in range(patterns):
        angle, phase = codes_ref[0, p], codes_ref[1, p]
        step_col = jnp.where(angle == 0, 2, -1)
        step_row = jnp.where(angle == 0, 0, jnp.where(angle == 1, 2, -2))
        for b in range(light_ref.shape[0]):
            y = within + b * ROWS_BLOCK
            turn = lax.rem(step_col * x + step_row * y + phase + 5 * OFFSET, 5)
            value = jnp.full((1, BLOCK), cosines[0], F32)
            for m in range(1, 5):
                value = jnp.where(turn == m, cosines[m], value)
            light_ref[b, p : p + 1] = value


def lateral(src_ref, w_ref, flip, b, count):
    total = None
    for k in range(3):
        v = src_ref[b + k : b + k + count]
        part = jnp.dot(v.reshape(-1, BLOCK), w_ref[3 * flip + k], preferred_element_type=F32)
        total = part if total is None else total + part
    return total.reshape(count, -1, BLOCK)


def split3(v):
    high = v.astype(BF16)
    rest = v - high.astype(F32)
    mid = rest.astype(BF16)
    return high, mid, (rest - mid.astype(F32)).astype(BF16)


class Step:
    def __init__(self, nx, tile_of, w_ref, ax_fwd, ax_bwd, light_ref, wave_ref):
        self.w, self.ax_fwd, self.ax_bwd, self.light, self.wave = w_ref, ax_fwd, ax_bwd, light_ref, wave_ref
        self.blocks, self.patterns = light_ref.shape[0], light_ref.shape[1]
        self.planes = wave_ref.shape[0]
        self.col = column_of(lane_iota((1, BLOCK)))
        place = tile_of() * TILE + self.col
        self.inside = (place >= 0) & (place < nx)

    def reach(self, width):
        return self.inside & (self.col >= -width) & (self.col < TILE + width)

    def clear_ends(self, ref):
        ref[0] = jnp.zeros(ref.shape[1:], BF16)
        ref[self.blocks + 1] = jnp.zeros(ref.shape[1:], BF16)

    def normalizer(self, norm_ref):
        depth = self.ax_bwd.shape[1]
        ones = lax.broadcasted_iota(jnp.int32, (depth, BLOCK), 0) < self.planes
        ones = jnp.where(ones, 1.0, 0.0).astype(BF16)
        colsum = jnp.dot(self.ax_bwd[...], ones, preferred_element_type=F32)[: self.planes]
        ones = jnp.broadcast_to(jnp.where(self.inside, 1.0, 0.0), (2 * SUB, BLOCK)).astype(BF16)
        parts = [jnp.dot(ones, self.w[3 + k], preferred_element_type=F32) for k in range(3)]
        for b in range(self.blocks):
            total = sum(parts[k] for k in range(3) if 0 <= b + k - 1 < self.blocks)
            cover = total.astype(BF16).astype(F32)[0:1]
            lat_sum = jnp.sum(self.light[b], axis=0, keepdims=True)
            norm_ref[b] = colsum * cover * (float(self.patterns) + lat_sum * self.wave[...])

    def blur(self, obj_ref, stage_ref):
        for b in range(self.blocks):
            lighting = 1.0 + self.light[b][:, None, :] * self.wave[...][None]
            lit = (lighting * obj_ref[b][None]).astype(BF16).reshape(-1, BLOCK)
            stage_ref[b + 1] = jnp.dot(self.ax_fwd[...], lit, preferred_element_type=F32).astype(BF16)

    def compare(self, stage_ref, data_ref, quot_ref, width, predicted_ref=None):
        ok = self.reach(width)[None]
        acc = jnp.zeros((SUB, BLOCK), F32)
        for b in range(0, self.blocks, CHUNK):
            if predicted_ref is None:
                predicted = lateral(stage_ref, self.w, 0, b, CHUNK)
            else:
                predicted = predicted_ref[b : b + CHUNK]
            data = data_ref[b : b + CHUNK]
            miss = data - predicted
            acc = acc + jnp.sum((miss * miss).reshape(-1, SUB, BLOCK), axis=0)
            quot_ref[b + 1 : b + 1 + CHUNK] = jnp.where(ok, data / predicted, 0.0).astype(BF16)
        row = jnp.sum(jnp.where((self.col >= 0) & (self.col < TILE), acc, 0.0), axis=0, keepdims=True)
        return sum(row[:, h * LANES : (h + 1) * LANES] for h in range(BLOCK // LANES))

    def update(self, quot_ref, obj_ref, norm_ref, width):
        ok = self.reach(width)
        for b0 in range(0, self.blocks, CHUNK):
            back = lateral(quot_ref, self.w, 1, b0, CHUNK).astype(BF16)
            for b in range(b0, b0 + CHUNK):
                part = back[b - b0].astype(F32).reshape(self.patterns, self.planes, BLOCK)
                plain = jnp.sum(part, axis=0)
                waved = jnp.sum(self.light[b][:, None, :] * part, axis=0)
                stack = jnp.concatenate(split3(plain) + split3(waved), axis=0)
                both = jnp.dot(self.ax_bwd[...], stack, preferred_element_type=F32)
                summed = both[: self.planes] + self.wave[...] * both[self.planes :]
                obj_ref[b] = jnp.where(ok, obj_ref[b] * summed / norm_ref[b], 0.0)


def put_halo(own_ref, from_left_ref, from_right_ref, out_ref):
    lane = lane_iota((SUB, LANES))
    for z in range(0, out_ref.shape[1], SUB):
        for vreg in range(out_ref.shape[0] // 2):
            from_left = from_left_ref[z : z + SUB, vreg * LANES : (vreg + 1) * LANES]
            from_right = from_right_ref[z : z + SUB, vreg * LANES : (vreg + 1) * LANES]
            for u in range(4):
                m = 4 * vreg + u
                at = (m // 2, slice(z, z + SUB), slice((m % 2) * LANES, (m % 2 + 1) * LANES))
                out_ref[at] = with_halo(own_ref[at], u, from_right, from_left, lane)


def forward_kernel(nx, tile_of, src_of, w_ref, ax_fwd, ax_bwd, light_ref, wave_ref,
                   est_ref, from_left_ref, from_right_ref, obj_ref, norm_ref, predicted_ref, stage_ref):
    unpack_wide(src_of, est_ref, from_left_ref, from_right_ref, obj_ref)
    step = Step(nx, tile_of, w_ref, ax_fwd, ax_bwd, light_ref, wave_ref)
    step.normalizer(norm_ref)
    step.clear_ends(stage_ref)
    step.blur(obj_ref, stage_ref)
    for b in range(0, step.blocks, CHUNK):
        predicted_ref[b : b + CHUNK] = lateral(stage_ref, w_ref, 0, b, CHUNK)


def first_kernel(nx, tile_of, src_of, w_ref, ax_fwd, ax_bwd, light_ref, wave_ref, norm_ref, obj_in_ref,
                 predicted_ref, in_ref, from_left_ref, from_right_ref, data_ref, obj_ref, left_ref, right_ref,
                 sq_ref, stage_ref, quot_ref):
    unpack_data(src_of, in_ref, from_left_ref, from_right_ref, data_ref)
    step = Step(nx, tile_of, w_ref, ax_fwd, ax_bwd, light_ref, wave_ref)
    step.clear_ends(stage_ref)
    step.clear_ends(quot_ref)
    obj_ref[...] = obj_in_ref[...]
    sq_ref[...] = jnp.zeros(sq_ref.shape, F32)
    sq_ref[0:1] = step.compare(None, data_ref, quot_ref, 12, predicted_ref)
    step.update(quot_ref, obj_ref, norm_ref, 8)
    step.blur(obj_ref, stage_ref)
    sq_ref[1:2] = step.compare(stage_ref, data_ref, quot_ref, 4)
    step.update(quot_ref, obj_ref, norm_ref, 0)

    lane = lane_iota((SUB, LANES))
    for z in range(0, step.planes, SUB):
        for vreg in range(step.blocks // 2):
            pieces = []
            for u in range(4):
                m = 4 * vreg + u
                pieces.append((obj_ref[m // 2, z : z + SUB, (m % 2) * LANES : (m % 2 + 1) * LANES], 0))
            left, right = edge_messages(pieces, lane)
            left_ref[z : z + SUB, vreg * LANES : (vreg + 1) * LANES] = left
            right_ref[z : z + SUB, vreg * LANES : (vreg + 1) * LANES] = right


def second_kernel(nx, tile_of, src_of, w_ref, ax_fwd, ax_bwd, light_ref, wave_ref, norm_ref, data_ref,
                  obj_in_ref, from_left_ref, from_right_ref, sq_in_ref, out_ref, obj_ref, stage_ref, quot_ref):
    put_halo(obj_in_ref, from_left_ref, from_right_ref, obj_ref)
    step = Step(nx, tile_of, w_ref, ax_fwd, ax_bwd, light_ref, wave_ref)
    step.clear_ends(stage_ref)
    step.clear_ends(quot_ref)
    squares = [sq_in_ref[0:1], sq_in_ref[1:2]]
    for quot_width, obj_width in ((12, 8), (4, 0)):
        step.blur(obj_ref, stage_ref)
        squares.append(step.compare(stage_ref, data_ref, quot_ref, quot_width))
        step.update(quot_ref, obj_ref, norm_ref, obj_width)

    ty, pat = src_of
    quads = step.blocks // ty
    planes = step.planes
    lane = lane_iota((2 * SUB, LANES))
    own = (lane // TILE) % 2 == 0
    last = to_log(jnp.concatenate(squares + [jnp.zeros((SUB - len(squares), LANES), F32)], axis=0))
    last = (jnp.concatenate([last >> 8, last & 255]) - BIAS).astype(jnp.int16)
    low_rows, last_rows = quads * planes, quads * planes * 3 // 2
    for i in range(ty):
        for k in range(pat):
            out_ref[i * pat + k, last_rows : last_rows + 2 * SUB] = last
        for q in range(0, quads, 2):
            for z in range(0, planes, 2 * SUB):
                fixed = []
                for b in (i * quads + q, i * quads + q + 1):
                    v0 = obj_ref[b, z : z + 2 * SUB, 0:LANES]
                    v1 = obj_ref[b, z : z + 2 * SUB, LANES : 2 * LANES]
                    fixed.append(to_log(jnp.where(own, v0, roll(v1, TILE))))
                starts = (q * planes + z, (q + 1) * planes + z, low_rows + q // 2 * planes + z)
                for row, v in zip(starts, encode(*fixed)):
                    for k in range(pat):
                        out_ref[i * pat + k, row : row + 2 * SUB] = v


def final_kernel(dest_of_tile, rows, in_ref, out_ref):
    lane = lane_iota((2 * SUB, LANES))
    planes = out_ref.shape[0] // rows
    tiles_half = LANES // TILE
    quads = rows // 4
    low_rows = quads * planes
    for half in range(len(dest_of_tile) // tiles_half):

        @pl.when(pl.program_id(0) == half)
        def _(half=half):
            for z in range(0, planes, 2 * SUB):
                for q in range(0, quads, 2):
                    starts = (q * planes + z, (q + 1) * planes + z, low_rows + q // 2 * planes + z)
                    both = []
                    for t in range(tiles_half):
                        dest = dest_of(dest_of_tile, half * tiles_half + t)
                        coded = decode(*(in_ref[dest, row : row + 2 * SUB] for row in starts))
                        both.append([from_log(v) for v in coded])
                    for p in range(2):
                        for g, piece in enumerate(quad_transpose([v[p] for v in both], lane)):
                            for h in range(2):
                                start = (z + h * SUB) * rows + 4 * (q + p) + QUAD_ROWS[g]
                                out_ref[pl.ds(start, SUB, stride=rows), :] = piece[h * SUB : (h + 1) * SUB]


def masked_kernel(lateral_kernel, psf_radius):
    offsets = jnp.arange(TAPS) - RADIUS
    within = jnp.abs(offsets)[None, :] <= psf_radius[:, None]
    return jnp.where(within, lateral_kernel, jnp.zeros_like(lateral_kernel)).astype(BF16)


def shape(dims, dtype=F32):
    return jax.ShapeDtypeStruct(dims, dtype)


PARAMS = pltpu.CompilerParams(vmem_limit_bytes=24 * 2**20)
PACKED = pltpu.CompilerParams(
    vmem_limit_bytes=24 * 2**20
)
VMEM = pl.BlockSpec(memory_space=pltpu.VMEM)
SMEM = pl.BlockSpec(memory_space=pltpu.SMEM)


def over_tx(value, size):
    if size & (size - 1):
        return lax.psum(value, "tx")
    step = 1
    while step < size:
        value = value + lax.ppermute(value, "tx", [(i, i ^ step) for i in range(size)])
        step *= 2
    return value


def tiled_device(sizes, estimate, data, axial, lateral_kernel, psf_radius, pattern_codes):
    ty, tx, pat = sizes["ty"], sizes["tx"], sizes["pat"]
    planes, rows, cols = estimate.shape
    pat_local = data.shape[0]
    patterns = pat_local * pat
    ny, nx = rows * ty, cols * tx
    members = ty * pat
    blocks = ny // ROWS_BLOCK
    axes = ("ty", "tx", "pat")

    owner = [(i, k if i % 2 == 0 else pat - 1 - k) for i in range(ty) for k in range(pat)]
    dest_of_tile = [i * pat + k for i, k in owner]
    order = [(i * tx + j) * pat + k for j in range(tx) for i, k in (owner if j % 2 == 0 else owner[::-1])]
    to_right = [(a, b) for a, b in zip(order[:-1], order[1:])]
    to_left = [(b, a) for a, b in to_right]
    src_of = (ty, pat)

    ti = lax.axis_index("ty")

    def tile_of():
        i, j, k = (lax.axis_index(a) for a in axes)
        c = i * pat + jnp.where(lax.rem(i, 2) == 0, k, pat - 1 - k)
        return j * members + jnp.where(lax.rem(j, 2) == 0, c, members - 1 - c)

    halves = cols // LANES
    piece_lanes = rows * TILE
    halo_lanes = ny * HALO

    def whole(dims):
        return pl.BlockSpec(dims, lambda h: (0,) * len(dims))

    def half_columns(height):
        return pl.BlockSpec((height, LANES), lambda h: (0, h))

    def edges(pieces, body, name):
        out = shape((pieces.shape[1] * pieces.shape[0] // ty, halo_lanes), pieces.dtype)
        return pl.pallas_call(
            functools.partial(body, (ty, pieces.shape[0] // ty)),
            out_shape=(out, out),
            in_specs=[VMEM],
            out_specs=(VMEM,) * 2,
            compiler_params=PARAMS,
            name=name,
        )(pieces)

    def swap_edges(left, right):
        return lax.ppermute(right, axes, to_right), lax.ppermute(left, axes, to_left)

    message = pl.pallas_call(
        functools.partial(pack_kernel, dest_of_tile, rows),
        out_shape=shape((members, 5 * planes // 2, piece_lanes), jnp.int16),
        grid=(halves,),
        in_specs=[half_columns(data.size // cols)],
        out_specs=whole((members, 5 * planes // 2, piece_lanes)),
        compiler_params=PARAMS,
        name="pack",
    )(data.reshape(-1, cols))
    message, estimate = lax.optimization_barrier((message, estimate))
    mine = lax.all_to_all(message, ("ty", "pat"), 0, 0, tiled=True)

    pieces = pl.pallas_call(
        functools.partial(estimate_kernel, dest_of_tile, rows, pat),
        out_shape=shape((ty, planes, piece_lanes)),
        grid=(halves,),
        in_specs=[half_columns(planes * rows)],
        out_specs=whole((ty, planes, piece_lanes)),
        scratch_shapes=[pltpu.VMEM((members, planes, piece_lanes), F32)],
        compiler_params=PARAMS,
        name="prep_estimate",
    )(estimate.reshape(-1, cols))
    tile_rows = [lax.dynamic_index_in_dim(pieces, ti, 0, keepdims=False)]
    for shift in range(1, ty):
        sent = lax.dynamic_index_in_dim(pieces, (ti + shift) % ty, 0, keepdims=False)
        tile_rows.append(lax.ppermute(sent, "ty", [(i, (i + shift) % ty) for i in range(ty)]))
    tile_rows = jnp.stack(tile_rows)
    tile_rows = jnp.stack(
        [lax.dynamic_index_in_dim(tile_rows, (ti - i) % ty, 0, keepdims=False) for i in range(ty)]
    )
    est_left, est_right = swap_edges(*edges(tile_rows, edges_kernel, "prep_edges"))

    weights, ax_fwd, ax_bwd, light = pl.pallas_call(
        functools.partial(tables_kernel, tile_of),
        out_shape=(
            shape((6, BLOCK, BLOCK), BF16),
            shape((patterns * planes, patterns * planes), BF16),
            shape((2 * planes, 6 * planes), BF16),
            shape((blocks, patterns, BLOCK)),
        ),
        in_specs=[SMEM] * 3 + [VMEM],
        out_specs=(VMEM,) * 4,
        compiler_params=PARAMS,
        name="tables",
    )(lateral_kernel, psf_radius, pattern_codes, axial)
    wave = np.cos(np.arange(planes, dtype=np.float32) * np.float32(TWO_PI * 3.0 / planes))
    wave = jnp.asarray(np.ascontiguousarray(np.broadcast_to(wave[:, None], (planes, BLOCK))))

    object_shape = shape((blocks, planes, BLOCK))
    field_shape = shape((blocks, patterns * planes, BLOCK))
    object_scratch = pltpu.VMEM(object_shape.shape, F32)
    stage = pltpu.VMEM((blocks + 2, patterns * planes, BLOCK), BF16)
    table_specs = [VMEM] * 5
    mine, est_left, est_right, weights = lax.optimization_barrier((mine, est_left, est_right, weights))
    from_left, from_right = swap_edges(*edges(mine, data_edges_kernel, "edges"))
    tables = (weights, ax_fwd, ax_bwd, light, wave)
    current, norm, predicted = pl.pallas_call(
        functools.partial(forward_kernel, nx, tile_of, (ty, 1)),
        out_shape=(object_shape, object_shape, field_shape),
        in_specs=table_specs + [VMEM] * 3,
        out_specs=(VMEM,) * 3,
        scratch_shapes=[stage],
        compiler_params=PARAMS,
        name="forward",
    )(*tables, tile_rows, est_left, est_right)

    edge_shape = shape((planes, halo_lanes))
    data_all, current, left, right, sq_first = pl.pallas_call(
        functools.partial(first_kernel, nx, tile_of, src_of),
        out_shape=(field_shape, object_shape, edge_shape, edge_shape, shape((SUB, LANES))),
        in_specs=table_specs + [VMEM] * 6,
        out_specs=(VMEM,) * 5,
        scratch_shapes=[stage, stage],
        compiler_params=PACKED,
        name="first",
    )(*tables, norm, current, predicted, mine, from_left, from_right)
    from_left, from_right = swap_edges(left, right)
    outgoing = pl.pallas_call(
        functools.partial(second_kernel, nx, tile_of, src_of),
        out_shape=shape((members, rows // 4 * planes * 3 // 2 + 2 * SUB, LANES), jnp.int16),
        in_specs=table_specs + [VMEM] * 6,
        out_specs=VMEM,
        scratch_shapes=[object_scratch, stage, stage],
        compiler_params=PACKED,
        name="second",
    )(*tables, norm, data_all, current, from_left, from_right, sq_first)

    incoming = lax.all_to_all(outgoing, ("ty", "pat"), 0, 0, tiled=True)
    last = incoming[:, rows // 4 * planes * 3 // 2 :].astype(jnp.int32) + BIAS
    squares = jnp.sum(from_log((last[:, :ITERS] << 8) + last[:, SUB : SUB + ITERS]), axis=(0, 2))
    squares = over_tx(squares, tx)
    result = pl.pallas_call(
        functools.partial(final_kernel, dest_of_tile, rows),
        out_shape=shape((planes * rows, cols)),
        grid=(halves,),
        in_specs=[whole(incoming.shape)],
        out_specs=half_columns(planes * rows),
        compiler_params=PARAMS,
        name="unpack",
    )(incoming)
    cell_count = float(patterns * planes * ny * nx)
    return result.reshape(estimate.shape), jnp.sqrt(squares / cell_count)


def extended(block, sides, width):
    for axis, dim in sides:
        count = lax.axis_size(axis)
        forward = [(i, i + 1) for i in range(count - 1)]
        backward = [(target, source) for source, target in forward]
        low = lax.ppermute(
            lax.slice_in_dim(block, block.shape[dim] - width, None, axis=dim), axis, forward
        )
        high = lax.ppermute(lax.slice_in_dim(block, 0, width, axis=dim), axis, backward)
        block = jnp.concatenate([low, block, high], axis=dim)
    return block


def wave_table(angle_code, phase_code, row_coord, col_coord, planes):
    step_col = jnp.where(angle_code == 0, 2, -1).astype(jnp.int32)
    step_row = jnp.where(angle_code == 0, 0, jnp.where(angle_code == 1, 2, -2)).astype(jnp.int32)
    argument = (
        step_col[:, None, None] * col_coord[None, None, :]
        + step_row[:, None, None] * row_coord[None, :, None]
        + phase_code[:, None, None]
    ) % 5
    lateral_wave = jnp.cos(argument.astype(jnp.float32) * (TWO_PI / 5.0))
    plane_index = jnp.arange(planes).astype(jnp.float32)
    axial_wave = jnp.cos(plane_index * (TWO_PI * 3.0 / planes))
    return 1.0 + 0.7 * lateral_wave[:, None, :, :] * axial_wave[None, :, None, None]


def tap_matrices(kernel, width_in, width_out):
    tap_count = 2 * RADIUS + 1
    offset = jnp.arange(width_in)[:, None] - jnp.arange(width_out)[None, :]
    onehot = (offset[None, :, :] == jnp.arange(tap_count)[:, None, None]).astype(jnp.float32)
    return jnp.einsum(
        "ij,jab->iab", kernel.astype(jnp.float32), onehot, precision=lax.Precision.HIGHEST
    ).astype(jnp.bfloat16)


def lateral_pass(padded, matrices, height):
    summed = None
    for tap_row in range(2 * RADIUS + 1):
        window = padded[..., tap_row : tap_row + height, :]
        product = jnp.dot(window, matrices[tap_row], preferred_element_type=jnp.float32)
        summed = product if summed is None else summed + product
    return summed


def general_device(estimate, data, axial, lateral_kernel, psf_radius, pattern_codes):
    planes, height, width = estimate.shape
    pat_local = data.shape[0]
    full_rows = height * lax.axis_size("ty")
    full_cols = width * lax.axis_size("tx")
    depth = 2 * RADIUS
    margin = depth - RADIUS
    row_coord = lax.axis_index("ty") * height - depth + jnp.arange(height + 2 * depth)
    col_coord = lax.axis_index("tx") * width - depth + jnp.arange(width + 2 * depth)
    codes_here = lax.dynamic_slice_in_dim(
        pattern_codes, lax.axis_index("pat") * pat_local, pat_local, 1
    )
    lighting = wave_table(codes_here[0], codes_here[1], row_coord, col_coord, planes)
    lighting_inner = lighting[:, :, depth : depth + height, depth : depth + width]
    kernel = masked_kernel(lateral_kernel, psf_radius)
    forward_taps = tap_matrices(kernel, width + 2 * depth, width + 2 * margin)
    adjoint_taps = tap_matrices(kernel[::-1, ::-1], width + 2 * RADIUS, width)
    axial_b = axial.astype(jnp.bfloat16)
    row_inside = (row_coord >= 0) & (row_coord < full_rows)
    col_inside = (col_coord >= 0) & (col_coord < full_cols)
    inside_all = row_inside[:, None] & col_inside[None, :]
    inside = inside_all[
        margin : margin + height + 2 * RADIUS, margin : margin + width + 2 * RADIUS
    ].astype(jnp.bfloat16)
    inside_mid = inside_all[
        RADIUS : RADIUS + height + 2 * margin, RADIUS : RADIUS + width + 2 * margin
    ]
    coverage = lateral_pass(inside[None], adjoint_taps, height).astype(jnp.bfloat16)
    spread = jnp.einsum(
        "ba,byx->ayx",
        axial_b,
        jnp.broadcast_to(coverage, (planes, height, width)),
        preferred_element_type=jnp.float32,
    )
    normalizer = lax.psum(jnp.sum(lighting_inner * spread[None], axis=0), "pat")
    cell_count = float(pat_local * lax.axis_size("pat") * planes * full_rows * full_cols)
    data_wide = extended(data, (("ty", 2), ("tx", 3)), RADIUS)
    current = estimate
    squares_list = []
    for iteration in range(ITERS):
        padded = extended(current, (("ty", 1), ("tx", 2)), depth)
        lighted = (lighting * padded[None]).astype(jnp.bfloat16)
        blurred = jnp.einsum(
            "ab,pbyx->payx", axial_b, lighted, preferred_element_type=jnp.float32
        ).astype(jnp.bfloat16)
        predicted = lateral_pass(blurred, forward_taps, height + 2 * margin)
        predicted_inner = predicted[:, :, margin : margin + height, margin : margin + width]
        misfit = data - predicted_inner
        local_square = jnp.sum(misfit * misfit)
        safe = jnp.where(inside_mid[None, None], predicted, 1.0)
        quotient_padded = jnp.where(inside_mid[None, None], data_wide / safe, 0.0).astype(
            jnp.bfloat16
        )
        backward = lateral_pass(quotient_padded, adjoint_taps, height).astype(jnp.bfloat16)
        gathered = jnp.einsum(
            "ba,pbyx->payx", axial_b, backward, preferred_element_type=jnp.float32
        )
        contribution = jnp.sum(lighting_inner * gathered, axis=0)
        summed = lax.psum(contribution, "pat")
        current = current * summed / normalizer
        squares_list.append(lax.psum(local_square, ("ty", "tx", "pat")))
    squares = jnp.stack(squares_list)
    return (current, jnp.sqrt(squares / cell_count))


def solution(mesh):
    sizes = dict(mesh.shape)
    in_specs = (P(None, "ty", "tx"), P("pat", None, "ty", "tx"), P(), P(), P(), P())
    out_specs = (P(None, "ty", "tx"), P())

    def per_device(estimate, data, *rest):
        planes, rows, cols = estimate.shape
        members = sizes["ty"] * sizes["pat"]
        fits = (
            cols == members * TILE
            and cols % LANES == 0
            and rows % 8 == 0
            and rows * sizes["ty"] <= 2 * TILE
            and planes == 4 * SUB
            and data.shape[0] == 2
        )
        if fits:
            return tiled_device(sizes, estimate, data, *rest)
        return general_device(estimate, data, *rest)

    return jax.shard_map(
        per_device, mesh=mesh, in_specs=in_specs, out_specs=out_specs, check_vma=False
    )
```
